32 devices in a mesh: dp: 8 (over z, x), tensor: 4 (over y, core).
Axes of the slice: x: 2, y: 2, z: 4, core: 2. Of those that a mesh axis runs over, the one named last changes fastest.
Arguments:
- tokens: bfloat16 [32768, 768], P(('dp', 'tensor')), may hold values from -6 to 6
- lengths: int32 [32], P('dp'), may hold values from 256 to 1024, as said below
- w_query: bfloat16 [768, 768], P('dp', 'tensor'), may hold values from -0.3125 to 0.3125
- w_key: bfloat16 [768, 768], P('dp', 'tensor'), may hold values from -0.3125 to 0.3125
- w_value: bfloat16 [768, 768], P('dp', 'tensor'), may hold values from -0.21875 to 0.21875
- w_out: bfloat16 [768, 768], P('tensor', 'dp'), may hold values from -1 to 1
- w_up: bfloat16 [768, 3072], P('dp', 'tensor'), may hold values from -0.21875 to 0.21875
- w_down: bfloat16 [3072, 768], P('tensor', 'dp'), may hold values from -0.109375 to 0.109375
- query_bias: float32 [768], P(('dp', 'tensor')), may hold values from -1.8 to 1.8
- value_bias: float32 [768], P(('dp', 'tensor')), may hold values from -1.8 to 1.8
- out_bias: float32 [768], P(('dp', 'tensor')), may hold values from -1.2 to 1.2
- attn_gain: float32 [768], P(('dp', 'tensor')), may hold values from 0.25 to 1.75
- attn_shift: float32 [768], P(('dp', 'tensor')), may hold values from -1.2 to 1.2
- up_bias: float32 [3072], P(('dp', 'tensor')), may hold values from -1.8 to 1.8
- down_bias: float32 [768], P(('dp', 'tensor')), may hold values from -1.2 to 1.2
- ffn_gain: float32 [768], P(('dp', 'tensor')), may hold values from 0.25 to 1.75
- ffn_shift: float32 [768], P(('dp', 'tensor')), may hold values from -1.8 to 1.8
- cotangent: bfloat16 [32768, 768], P(('dp', 'tensor')), may hold values from -6 to 6
Outputs:
- output: float32 [32768, 768], P(('dp', 'tensor'))
- grad_tokens: float32 [32768, 768], P(('dp', 'tensor'))
- query_grad: float32 [768, 768], P('dp', 'tensor')
- key_grad: float32 [768, 768], P('dp', 'tensor')
- value_grad: float32 [768, 768], P('dp', 'tensor')
- out_grad: float32 [768, 768], P('tensor', 'dp')
- up_grad: float32 [768, 3072], P('dp', 'tensor')
- down_grad: float32 [3072, 768], P('tensor', 'dp')
- query_bias_grad: float32 [768], P(('dp', 'tensor'))
- value_bias_grad: float32 [768], P(('dp', 'tensor'))
- out_bias_grad: float32 [768], P(('dp', 'tensor'))
- attn_gain_grad: float32 [768], P(('dp', 'tensor'))
- attn_shift_grad: float32 [768], P(('dp', 'tensor'))
- up_bias_grad: float32 [3072], P(('dp', 'tensor'))
- down_bias_grad: float32 [768], P(('dp', 'tensor'))
- ffn_gain_grad: float32 [768], P(('dp', 'tensor'))
- ffn_shift_grad: float32 [768], P(('dp', 'tensor'))
The draws below stay inside these ranges and needn't reach their ends.
Inputs may be any that keep to these rules, and one draw needn't show every extreme that they name: `lengths`: each sequence's count of valid tokens, which come first in it; in every draw some sequence has all 1024 slots valid and some has 256.
All inputs are finite; a program needn't handle non-finite values.
Results may differ from the reference program's by a relative error of at most 0.019.
Values may be sent and summed in bfloat16 or wider, within the bound.
A program may use at most 192 MiB of HBM per device.

```python
import jax
import jax.numpy as jnp
from jax import lax

D = 768
HEADS = 12
HEAD = 64
FF = 3072
SEQ_LEN = 1024
SEQS = 4
NSEQ = 32
TOKENS = 32768
N_DP = 8


def draw_lengths(key, part):
    base_key = jax.random.fold_in(key, 11)
    key_one, key_two, key_three = jax.random.split(base_key, 3)
    drawn = jax.random.randint(key_one, (NSEQ,), SEQ_LEN // 4, SEQ_LEN + 1, dtype=jnp.int32)
    first_seq = jax.random.randint(key_two, (), 0, NSEQ, dtype=jnp.int32)
    second_seq = (first_seq + 1 + jax.random.randint(key_three, (), 0, NSEQ - 1, dtype=jnp.int32)) % NSEQ
    places = jnp.arange(NSEQ, dtype=jnp.int32)
    drawn = jnp.where(places == first_seq, SEQ_LEN, drawn)
    drawn = jnp.where(places == second_seq, SEQ_LEN // 4, drawn)
    return drawn.astype(jnp.int32)


def steps_of(rng, shape, cuts, least, high):
    loudness, own = 1.0, jax.random.fold_in(rng, 6)
    for position, parts in cuts:
        steps = jnp.exp(jax.random.uniform(jax.random.fold_in(own, position), (parts,), jnp.float32, least / len(cuts), high / len(cuts)))
        loudness = loudness * jnp.repeat(steps, shape[position] // parts).reshape([-1 if axis == position else 1 for axis in range(len(shape))])
    return loudness


def gaussian(rng, shape, scale, limit, shards=(), held_as=jnp.bfloat16):
    result = scale * jax.random.normal(rng, shape, jnp.float32)
    if shards:
        result = result * steps_of(rng, shape, shards, -0.22, 0.18)
    return jnp.clip(result, -limit, limit).astype(held_as)


def setup_inputs(seed: int = 0) -> dict:
    keys = jax.random.split(jax.random.key(seed), 19)
    tokens = gaussian(keys[0], (TOKENS, D), 1.0, 6.0, ((0, 32),))
    lengths = draw_lengths(jax.random.fold_in(keys[18], 71), 0)
    w_query = gaussian(keys[2], (D, D), (D // 2) ** -0.5, 0.3125, ((0, 8), (1, 4)))
    w_key = gaussian(keys[3], (D, D), (D // 2) ** -0.5, 0.3125, ((0, 8), (1, 4)))
    w_value = gaussian(keys[4], (D, D), D ** -0.5, 0.21875, ((0, 8), (1, 4)))
    w_out = gaussian(keys[5], (D, D), (HEAD // 2) ** -0.5, 1.0, ((0, 4), (1, 8)))
    w_up = gaussian(keys[6], (D, FF), D ** -0.5, 0.21875, ((0, 8), (1, 4)))
    w_down = gaussian(keys[7], (FF, D), FF ** -0.5, 0.109375, ((0, 4), (1, 8)))
    query_bias = gaussian(keys[8], (D,), 0.3, 1.8, ((0, 32),), jnp.float32)
    value_bias = gaussian(keys[9], (D,), 0.3, 1.8, ((0, 32),), jnp.float32)
    out_bias = gaussian(keys[10], (D,), 0.2, 1.2, ((0, 32),), jnp.float32)
    attn_gain = jnp.clip(1.0 + 0.15 * jax.random.normal(keys[11], (D,), jnp.float32), 0.25, 1.75)
    attn_shift = gaussian(keys[12], (D,), 0.2, 1.2, ((0, 32),), jnp.float32)
    up_bias = gaussian(keys[13], (FF,), 0.3, 1.8, ((0, 32),), jnp.float32)
    down_bias = gaussian(keys[14], (D,), 0.2, 1.2, ((0, 32),), jnp.float32)
    ffn_gain = jnp.clip(1.0 + 0.15 * jax.random.normal(keys[15], (D,), jnp.float32), 0.25, 1.75)
    ffn_shift = gaussian(keys[16], (D,), 0.3, 1.8, ((0, 32),), jnp.float32)
    cotangent = gaussian(keys[17], (TOKENS, D), 1.0, 6.0, ((0, 32),))
    return {"tokens": tokens, "lengths": lengths, "w_query": w_query, "w_key": w_key, "w_value": w_value, "w_out": w_out, "w_up": w_up, "w_down": w_down, "query_bias": query_bias, "value_bias": value_bias, "out_bias": out_bias, "attn_gain": attn_gain, "attn_shift": attn_shift, "up_bias": up_bias, "down_bias": down_bias, "ffn_gain": ffn_gain, "ffn_shift": ffn_shift, "cotangent": cotangent}


@jax.custom_vjp
def low(v):
    return lax.optimization_barrier(v.astype(jnp.bfloat16)).astype(jnp.float32)

@jax.custom_vjp
def low_back(v):
    return v

def low_keep(v):
    return (low(v), None)

def low_pass(kept, grad):
    return (grad,)

def back_keep(v):
    return (v, None)

def back_low(kept, grad):
    return (low(grad),)
low.defvjp(low_keep, low_pass)
low_back.defvjp(back_keep, back_low)
EPSILON = 1e-12
FLOOR_SCORE = -1e+30

def both_round(operand):
    return low_back(low(operand))

def matmul(left_side, right_side):
    return jnp.dot(left_side, right_side, precision=lax.Precision.HIGHEST, preferred_element_type=jnp.float32)

def layer_norm(values, norm_gain, norm_shift):
    center = values - lax.optimization_barrier(jnp.mean(values, axis=-1, keepdims=True))
    spread = lax.optimization_barrier(jnp.mean(center * center, axis=-1, keepdims=True))
    return center * lax.rsqrt(spread + EPSILON) * norm_gain + norm_shift

def attend(seq_items):
    query_seq, key_seq, value_seq, length = seq_items
    scores = jnp.einsum('qhd,khd->hqk', query_seq, key_seq, precision=lax.Precision.HIGHEST) * HEAD ** (-0.5)
    scores = low_back(scores)
    counted = jnp.arange(SEQ_LEN, dtype=jnp.int32) < length
    scores = jnp.where(counted[None, None, :], scores, FLOOR_SCORE)
    row_top = lax.optimization_barrier(jnp.max(scores, axis=-1, keepdims=True))
    exp_terms = jnp.exp(scores - row_top)
    prob_low = low(exp_terms / lax.optimization_barrier(jnp.sum(exp_terms, axis=-1, keepdims=True)))
    return both_round(jnp.einsum('hqk,khd->qhd', prob_low, value_seq, precision=lax.Precision.HIGHEST))

def layer_forward(inputs, weights, group_lengths):
    w_query, w_key, w_value, w_out, w_up, w_down, query_bias, value_bias, out_bias, attn_gain, attn_shift, up_bias, down_bias, ffn_gain, ffn_shift = weights
    head_shape = (SEQS, SEQ_LEN, HEADS, HEAD)
    queries = both_round(matmul(inputs, w_query) + query_bias)
    keys_low = both_round(matmul(inputs, w_key))
    values_low = both_round(matmul(inputs, w_value) + value_bias)
    head_mix = lax.map(jax.checkpoint(attend), (queries.reshape(head_shape), keys_low.reshape(head_shape), values_low.reshape(head_shape), group_lengths))
    head_mix = head_mix.reshape(SEQS * SEQ_LEN, D)
    attention = low_back(matmul(head_mix, w_out) + out_bias)
    hidden = layer_norm(inputs + attention, attn_gain, attn_shift)
    hidden_low = both_round(hidden)
    pre_act = low_back(matmul(hidden_low, w_up) + up_bias)
    act_low = both_round(jax.nn.gelu(pre_act, approximate=False))
    branch = low_back(matmul(act_low, w_down) + down_bias)
    normed = layer_norm(hidden + branch, ffn_gain, ffn_shift)
    positions = jnp.arange(SEQS * SEQ_LEN, dtype=jnp.int32)
    row_length = group_lengths[positions // SEQ_LEN]
    valid = (positions % SEQ_LEN < row_length).astype(normed.dtype)
    return normed * valid[:, None]

def reference(tokens, lengths, w_query, w_key, w_value, w_out, w_up, w_down, query_bias, value_bias, out_bias, attn_gain, attn_shift, up_bias, down_bias, ffn_gain, ffn_shift, cotangent):
    params = (w_query.astype(jnp.float32), w_key.astype(jnp.float32), w_value.astype(jnp.float32), w_out.astype(jnp.float32), w_up.astype(jnp.float32), w_down.astype(jnp.float32), query_bias, value_bias, out_bias, attn_gain, attn_shift, up_bias, down_bias, ffn_gain, ffn_shift)
    token_groups = tokens.astype(jnp.float32).reshape(N_DP, SEQS * SEQ_LEN, D)
    cot_groups = cotangent.astype(jnp.float32).reshape(N_DP, SEQS * SEQ_LEN, D)
    length_groups = lengths.astype(jnp.int32).reshape(N_DP, SEQS)

    def group_step(totals, group_items):
        group_tokens, group_cot, group_lengths = group_items

        def forward_fn(inputs, weights):
            return layer_forward(inputs, weights, group_lengths)
        group_out, pullback = jax.vjp(forward_fn, group_tokens, params)
        grad_inputs, grad_params = pullback(group_cot)
        totals = tuple((running + added for running, added in zip(totals, grad_params)))
        return (totals, (group_out, grad_inputs))
    initial = tuple((jnp.zeros_like(param) for param in params))
    totals, (outputs, grad_inputs) = lax.scan(group_step, initial, (token_groups, cot_groups, length_groups))
    return (outputs.reshape(TOKENS, D), grad_inputs.reshape(TOKENS, D), totals[0], totals[1], totals[2], totals[3], totals[4], totals[5], totals[6], totals[7], totals[8], totals[9], totals[10], totals[11], totals[12], totals[13], totals[14])
```

```python
import functools

import jax
import jax.numpy as jnp
from jax import lax
from jax.experimental import pallas as pl
from jax.experimental.pallas import tpu as pltpu
from jax.sharding import PartitionSpec as P

HEAD = 64
EPSILON = 1e-12
FLOOR_SCORE = -1e30
BLOCK = 256
WIDE = 256
BF16 = jnp.bfloat16
F32 = jnp.float32
VMEM_LIMIT = 60 * 1024 * 1024


def dot_nn(a, b):
    return lax.dot_general(a, b, (((1,), (0,)), ((), ())), preferred_element_type=F32)


def dot_nt(a, b):
    return lax.dot_general(a, b, (((1,), (1,)), ((), ())), preferred_element_type=F32)


def dot_tn(a, b):
    return lax.dot_general(a, b, (((0,), (0,)), ((), ())), preferred_element_type=F32)


def lane_iota(rows, lanes):
    return lax.broadcasted_iota(jnp.int32, (rows, lanes), 1)


def row_iota(rows, lanes):
    return lax.broadcasted_iota(jnp.int32, (rows, lanes), 0)


def head_mask(rows, h, extra):
    lane = lane_iota(rows, WIDE)
    keep = (lane >= h * HEAD) & (lane < (h + 1) * HEAD)
    if extra is not None:
        keep = keep | (lane >= extra)
    return keep


def normalize(v):
    center = v - jnp.mean(v, axis=-1, keepdims=True)
    inv = lax.rsqrt(jnp.mean(center * center, axis=-1, keepdims=True) + EPSILON)
    return center * inv, inv


def norm_back(g, n, inv):
    return inv * (
        g - jnp.mean(g, axis=-1, keepdims=True) - n * jnp.mean(g * n, axis=-1, keepdims=True)
    )


def split_three(v):
    hi = v.astype(BF16)
    rest = v - hi.astype(F32)
    mid = rest.astype(BF16)
    low = (rest - mid.astype(F32)).astype(BF16)
    return hi.astype(F32), mid.astype(F32), low.astype(F32)


def attend_kernel(len_ref, x_ref, w_ref, b_ref, ob_ref, res_ref, q_ref, k_ref, v_ref, mix_ref, lse_ref):
    t = pl.program_id(0)
    rows, width = x_ref.shape
    cols = mix_ref.shape[2]
    heads = cols // HEAD
    length = len_ref[0]
    lane = lane_iota(BLOCK, WIDE)

    @pl.when(t == 0)
    def _():
        @pl.loop(0, rows, step=BLOCK)
        def _(r):
            r = pl.multiple_of(r, BLOCK)
            res_ref[pl.ds(r, BLOCK), :] = x_ref[pl.ds(r, BLOCK), :].astype(F32) + ob_ref[...]

    @pl.loop(0, rows, step=BLOCK)
    def _(r):
        r = pl.multiple_of(r, BLOCK)
        here = pl.ds(r, BLOCK)
        out = dot_nn(x_ref[here, :], w_ref[0, :, : 3 * cols]) + b_ref[0]
        one = jnp.ones((BLOCK, WIDE - cols), F32)
        tail = lane_iota(BLOCK, WIDE - cols)
        position = r + row_iota(BLOCK, WIDE - cols)
        q_ref[0, here, :cols] = (out[:, :cols].astype(BF16).astype(F32) * HEAD**-0.5).astype(BF16)
        q_ref[0, here, cols:] = jnp.where(tail == 3, one, 0.0).astype(BF16)
        k_ref[0, here, :cols] = out[:, cols : 2 * cols].astype(BF16)
        bias = jnp.where(position < length, 0.0, FLOOR_SCORE)
        k_ref[0, here, cols:] = jnp.where(
            tail < 3, one, jnp.where(tail == 3, bias, 0.0)
        ).astype(BF16)
        v_ref[0, here, :cols] = out[:, 2 * cols : 3 * cols].astype(BF16)
        v_ref[0, here, cols:] = one.astype(BF16)

    @pl.loop(0, rows, step=BLOCK)
    def _(r):
        r = pl.multiple_of(r, BLOCK)
        here = pl.ds(r, BLOCK)
        query = q_ref[0, here, :]
        scores = [
            dot_nt(jnp.where(head_mask(BLOCK, h, cols), query, 0), k_ref[0]) for h in range(heads)
        ]
        mixed = jnp.zeros((BLOCK, WIDE), F32)
        total = jnp.zeros((BLOCK, 128), F32)
        for h in range(heads):
            top = jnp.max(scores[h], axis=-1, keepdims=True)
            terms = jnp.exp(scores[h] - top).astype(BF16)
            got = dot_nn(terms, v_ref[0])
            denom = got[:, cols : cols + 1]
            mixed = jnp.where(head_mask(BLOCK, h, None), got * (1.0 / denom), mixed)
            total = jnp.where(lane_iota(BLOCK, 128) == h, -(top + jnp.log(denom)), total)
        low = mixed[:, :cols].astype(BF16)
        mix_ref[0, here, :] = low
        lse_ref[0, here, :] = total
        res_ref[here, :] += dot_nt(low, w_ref[0, :, 3 * cols :])


def ffn_kernel(
    len_ref, res_ref, cot_ref, vec_ref, ub_ref, wu_ref, wd_ref,
    out_ref, gfirst_ref, gattn_ref, small_ref, gup_ref, gdn_ref,
    hid, hlow, acc, gb, act, dact, gpre,
):
    phase, t = pl.program_id(0), pl.program_id(1)
    last = pl.num_programs(1) - 1
    rows, width = res_ref.shape
    length = len_ref[0]
    gain_one, shift_one, down_bias = vec_ref[0:1, :], vec_ref[1:2, :], vec_ref[2:3, :]
    gain_two, shift_two = vec_ref[3:4, :], vec_ref[4:5, :]

    def blocks(body):
        @pl.loop(0, rows, step=BLOCK)
        def _(r):
            r = pl.multiple_of(r, BLOCK)
            body(r, pl.ds(r, BLOCK))

    def put(row, value):
        small_ref[row : row + 1, :] += jnp.sum(value, axis=0, keepdims=True)

    @pl.when((phase == 0) & (t == 0))
    def _():
        small_ref[...] = jnp.zeros_like(small_ref)

        def first(r, here):
            n, _ = normalize(res_ref[here, :])
            hidden = n * gain_one + shift_one
            hid[here, :] = hidden
            hlow[here, :] = hidden.astype(BF16)
            acc[here, :] = hidden + down_bias

        blocks(first)

    @pl.when(phase == 0)
    def _():
        def forward(r, here):
            pre = dot_nn(hlow[here, :], wu_ref[0]) + ub_ref[0]
            phi = 0.5 * (1.0 + lax.erf(pre * (0.5**0.5)))
            low = (pre * phi).astype(BF16)
            act[t, here, :] = low
            dact[t, here, :] = phi + pre * (jnp.exp(-0.5 * pre * pre) * 0.3989422804014327)
            acc[here, :] += dot_nt(low, wd_ref[0])

        blocks(forward)

    @pl.when((phase == 0) & (t == last))
    def _():
        def turn(r, here):
            n, inv = normalize(acc[here, :])
            valid = ((r + row_iota(BLOCK, 1)) < length).astype(F32)
            out_ref[here, :] = (n * gain_two + shift_two) * valid
            cot = cot_ref[here, :].astype(F32) * valid
            put(4, cot * n)
            put(5, cot)
            grad = norm_back(cot * gain_two, n, inv)
            acc[here, :] = grad
            low = grad.astype(BF16)
            gb[here, :] = low
            put(3, low.astype(F32))

        blocks(turn)

    @pl.when(phase == 1)
    def _():
        def backward(r, here):
            grad_act = dot_nn(gb[here, :], wd_ref[0]).astype(BF16).astype(F32)
            low = (grad_act * dact[t, here, :]).astype(BF16)
            gpre[here, :] = low
            part = dot_nt(low, wu_ref[0])

            @pl.when(t == 0)
            def _():
                hid[here, :] = part

            @pl.when(t > 0)
            def _():
                hid[here, :] += part

            small_ref[pl.ds(8 + t, 1), :] += jnp.sum(low.astype(F32), axis=0, keepdims=True)

        blocks(backward)

        @pl.loop(0, width, step=BLOCK)
        def _(c):
            c = pl.multiple_of(c, BLOCK)
            here = pl.ds(c, BLOCK)
            gdn_ref[0, here, :] = dot_tn(gb[:, here], act[t]).astype(BF16)
            gup_ref[0, here, :] = dot_tn(hlow[:, here], gpre[...]).astype(BF16)

    @pl.when((phase == 1) & (t == last))
    def _():
        def finish(r, here):
            grad_hidden = acc[here, :] + hid[here, :].astype(BF16).astype(F32)
            n, inv = normalize(res_ref[here, :])
            put(1, grad_hidden * n)
            put(2, grad_hidden)
            grad = norm_back(grad_hidden * gain_one, n, inv)
            gfirst_ref[here, :] = grad
            low = grad.astype(BF16)
            gattn_ref[here, :] = low
            put(0, low.astype(F32))

        blocks(finish)


def attend_back_kernel(
    x_ref, w_ref, gattn_ref, gfirst_ref, q_ref, k_ref, v_ref, mix_ref, lse_ref,
    gtok_ref, grad_ref, bias_ref,
    qh, gh, dq, kh, ds, dqkv,
):
    t = pl.program_id(0)
    rows, width = x_ref.shape
    cols = mix_ref.shape[2]
    heads = cols // HEAD

    @pl.when(t == 0)
    def _():
        gtok_ref[...] = gfirst_ref[...]

    bias_ref[...] = jnp.zeros_like(bias_ref)

    @pl.loop(0, rows, step=BLOCK)
    def _(r):
        r = pl.multiple_of(r, BLOCK)
        here = pl.ds(r, BLOCK)
        grad_mixed = dot_nn(gattn_ref[here, :], w_ref[0, :, 3 * cols :]).astype(BF16)
        product = grad_mixed.astype(F32) * mix_ref[0, here, :].astype(F32)
        lane = lane_iota(BLOCK, WIDE)
        wide = jnp.concatenate(
            [grad_mixed.astype(F32), jnp.zeros((BLOCK, WIDE - cols), F32)], axis=1
        )
        query = q_ref[0, here, :].astype(F32)
        key = k_ref[0, here, :]
        for h in range(heads):
            inside = (lane_iota(BLOCK, cols) >= h * HEAD) & (lane_iota(BLOCK, cols) < (h + 1) * HEAD)
            delta = jnp.sum(jnp.where(inside, product, 0.0), axis=-1, keepdims=True)
            hi, mid, low = split_three(-delta)
            keep = head_mask(BLOCK, h, None)
            tail = jnp.where(lane == cols, hi, jnp.where(lane == cols + 1, mid, jnp.where(lane == cols + 2, low, 0.0)))
            gh[h, here, :] = jnp.where(keep, wide, tail).astype(BF16)
            hi, mid, low = split_three(lse_ref[0, here, h : h + 1])
            tail = jnp.where(lane == cols, hi, jnp.where(lane == cols + 1, mid, jnp.where(lane == cols + 2, low, 0.0)))
            tail = jnp.where(lane == cols + 3, 1.0, tail)
            qh[h, here, :] = jnp.where(keep, query, tail).astype(BF16)
            kh[h, here, :] = jnp.where(keep, key, 0)

    @pl.loop(0, rows, step=BLOCK)
    def _(r):
        r = pl.multiple_of(r, BLOCK)
        here = pl.ds(r, BLOCK)
        key, value = k_ref[0, here, :], v_ref[0, here, :]
        grad_key = jnp.zeros((BLOCK, WIDE), F32)
        grad_value = jnp.zeros((BLOCK, WIDE), F32)
        logits = [dot_nt(key, qh[h]) for h in range(heads)]
        grads = [dot_nt(value, gh[h]) for h in range(heads)]
        for h in range(heads):
            prob = jnp.exp(logits[h])
            grad_value += dot_nn(prob.astype(BF16), gh[h])
            grad_score = (prob * grads[h]).astype(BF16)
            grad_key += dot_nn(grad_score, qh[h])
            part = dot_tn(grad_score, kh[h, here, :])
            if h == 0:
                total = part
            else:
                total += part

        @pl.when(r == 0)
        def _():
            dq[...] = total

        @pl.when(r > 0)
        def _():
            dq[...] += total

        low = grad_key[:, :cols].astype(BF16)
        dqkv[here, cols : 2 * cols] = low
        low = grad_value[:, :cols].astype(BF16)
        dqkv[here, 2 * cols :] = low
        bias_ref[0, 1:2, :] += jnp.sum(low.astype(F32), axis=0, keepdims=True)

    @pl.loop(0, rows, step=BLOCK)
    def _(r):
        r = pl.multiple_of(r, BLOCK)
        here = pl.ds(r, BLOCK)
        low = (dq[here, :cols] * HEAD**-0.5).astype(BF16)
        dqkv[here, :cols] = low
        bias_ref[0, 0:1, :] += jnp.sum(low.astype(F32), axis=0, keepdims=True)
        gtok_ref[here, :] += dot_nt(dqkv[here, :], w_ref[0, :, : 3 * cols])

    @pl.loop(0, width, step=BLOCK)
    def _(c):
        c = pl.multiple_of(c, BLOCK)
        here = pl.ds(c, BLOCK)
        grad_ref[0, here, : 3 * cols] = dot_tn(x_ref[:, here], dqkv[...]).astype(BF16)
        grad_ref[0, here, 3 * cols :] = dot_tn(gattn_ref[:, here], mix_ref[0]).astype(BF16)


def resident(shape):
    return pl.BlockSpec(shape, lambda *ids: (0,) * len(shape), pipeline_mode=pl.Buffered(1))


def result(shape):
    return pl.BlockSpec(shape, lambda *ids: (0,) * len(shape))


def per_step(shape):
    return pl.BlockSpec((1, *shape[1:]), lambda t: (t, 0, 0))


def struct(shape, dtype):
    return jax.ShapeDtypeStruct(shape, dtype)


def params(steps):
    return pltpu.CompilerParams(
        dimension_semantics=("arbitrary",) * steps, vmem_limit_bytes=VMEM_LIMIT
    )


def run_attend(length, tokens, w_attn, bias, out_bias):
    rows, width = tokens.shape
    groups = w_attn.shape[0]
    cols = width // groups
    wide = (groups, rows, WIDE)
    return pl.pallas_call(
        attend_kernel,
        grid=(groups,),
        in_specs=[
            pl.BlockSpec(memory_space=pltpu.SMEM),
            resident((rows, width)),
            per_step(w_attn.shape),
            per_step(bias.shape),
            resident(out_bias.shape),
        ],
        out_specs=[
            result((rows, width)),
            per_step(wide), per_step(wide), per_step(wide),
            per_step((groups, rows, cols)), per_step((groups, rows, 128)),
        ],
        out_shape=[
            struct((rows, width), F32),
            struct(wide, BF16), struct(wide, BF16), struct(wide, BF16),
            struct((groups, rows, cols), BF16), struct((groups, rows, 128), F32),
        ],
        compiler_params=params(1),
        name="attend",
    )(length, tokens, w_attn, bias, out_bias)


def run_ffn(length, residual, cotangent, vectors, up_bias, w_up, w_down):
    rows, width = residual.shape
    groups = w_up.shape[0]
    units = w_up.shape[2]
    slab = pl.BlockSpec((1, width, units), lambda p, t: (t, 0, 0))
    grad = pl.BlockSpec((1, width, units), lambda p, t: (p * t, 0, 0))
    return pl.pallas_call(
        ffn_kernel,
        grid=(2, groups),
        in_specs=[
            pl.BlockSpec(memory_space=pltpu.SMEM),
            resident((rows, width)),
            resident((rows, width)),
            resident(vectors.shape),
            pl.BlockSpec((1, 1, units), lambda p, t: (t, 0, 0)),
            slab, slab,
        ],
        out_specs=[
            result((rows, width)), result((rows, width)), result((rows, width)), result((16, width)),
            grad, grad,
        ],
        out_shape=[
            struct((rows, width), F32), struct((rows, width), F32), struct((rows, width), BF16),
            struct((16, width), F32),
            struct(w_up.shape, BF16), struct(w_up.shape, BF16),
        ],
        scratch_shapes=[
            pltpu.VMEM((rows, width), F32), pltpu.VMEM((rows, width), BF16),
            pltpu.VMEM((rows, width), F32), pltpu.VMEM((rows, width), BF16),
            pltpu.VMEM((groups, rows, units), BF16), pltpu.VMEM((groups, rows, units), F32),
            pltpu.VMEM((rows, units), BF16),
        ],
        compiler_params=params(2),
        name="ffn",
    )(length, residual, cotangent, vectors, up_bias, w_up, w_down)


def run_attend_back(tokens, w_attn, grad_attn, grad_first, q, k, v, mixed, lse):
    rows, width = tokens.shape
    groups = w_attn.shape[0]
    cols = width // groups
    heads = cols // HEAD
    return pl.pallas_call(
        attend_back_kernel,
        grid=(groups,),
        in_specs=[
            resident((rows, width)), per_step(w_attn.shape),
            resident((rows, width)), resident((rows, width)),
            per_step(q.shape), per_step(k.shape), per_step(v.shape),
            per_step(mixed.shape), per_step(lse.shape),
        ],
        out_specs=[result((rows, width)), per_step(w_attn.shape), per_step((groups, 8, cols))],
        out_shape=[
            struct((rows, width), F32), struct(w_attn.shape, BF16), struct((groups, 8, cols), F32),
        ],
        scratch_shapes=[
            pltpu.VMEM((heads, rows, WIDE), BF16), pltpu.VMEM((heads, rows, WIDE), BF16),
            pltpu.VMEM((rows, WIDE), F32), pltpu.VMEM((heads, rows, WIDE), BF16),
            pltpu.VMEM((8, 128), BF16), pltpu.VMEM((rows, 3 * cols), BF16),
        ],
        compiler_params=params(1),
        name="attend_back",
    )(tokens, w_attn, grad_attn, grad_first, q, k, v, mixed, lse)


def shards(
    tokens, lengths, w_query, w_key, w_value, w_out, w_up, w_down,
    query_bias, value_bias, out_bias, attn_gain, attn_shift, up_bias, down_bias, ffn_gain, ffn_shift,
    cotangent,
):
    rows, width = tokens.shape
    groups = lax.axis_size("tensor")
    spans = lax.axis_size("dp")
    seq_count = lengths.shape[0]
    assert rows * groups == seq_count * rows and seq_count == groups
    rank = lax.axis_index("tensor")
    length = lax.dynamic_slice_in_dim(lengths, rank, 1)
    both = ("dp", "tensor")

    pack = jnp.concatenate([w_query, w_key, w_value, w_out.T, w_up, w_down.T], axis=1)
    whole = lax.all_gather(pack, both, axis=0, tiled=True)
    whole = whole.reshape(spans, groups, *pack.shape).swapaxes(0, 1)
    whole = whole.reshape(groups, width, pack.shape[1])
    cols = width // groups
    units = w_up.shape[1]
    w_attn, w_in, w_back = whole[:, :, : 4 * cols], whole[:, :, 4 * cols : 4 * cols + units], whole[:, :, 4 * cols + units :]

    vectors = (query_bias, value_bias, out_bias, attn_gain, attn_shift, down_bias, ffn_gain, ffn_shift)
    count = query_bias.shape[0]
    flat = jnp.concatenate([jnp.stack(vectors).reshape(-1), up_bias])
    gathered = lax.all_gather(flat, both, axis=0, tiled=True).reshape(spans * groups, -1)
    full = gathered[:, : 8 * count].reshape(-1, 8, count).swapaxes(0, 1).reshape(8, width)
    ub = gathered[:, 8 * count :].reshape(groups, 1, units)
    qb, vb = full[0].reshape(groups, 1, cols), full[1].reshape(groups, 1, cols)
    bias = jnp.concatenate([qb, jnp.zeros_like(qb), vb], axis=2)

    residual, q, k, v, mixed, lse = run_attend(length, tokens, w_attn, bias, full[2:3])
    output, grad_first, grad_attn, small, grad_in, grad_back = run_ffn(
        length, residual, cotangent, full[3:8], ub, w_in, w_back
    )
    grad_tokens, grad_attn_w, bias_grad = run_attend_back(
        tokens, w_attn, grad_attn, grad_first, q, k, v, mixed, lse
    )

    every = jnp.concatenate([grad_attn_w, grad_in, grad_back], axis=2)
    every = every.reshape(groups, spans, width // spans, -1).swapaxes(0, 1)
    every = every.reshape(spans * groups * (width // spans), -1)
    owned = lax.psum_scatter(every, both, scatter_dimension=0, tiled=True).astype(F32)

    rows8 = jnp.concatenate(
        [bias_grad[:, 0].reshape(1, width), bias_grad[:, 1].reshape(1, width), small[:6]]
    )
    parts = jnp.concatenate(
        [
            rows8.reshape(8, spans * groups, count).swapaxes(0, 1).reshape(spans * groups, 8 * count),
            small[8 : 8 + groups].reshape(spans * groups, -1),
        ],
        axis=1,
    )
    tiny = lax.psum_scatter(parts.reshape(-1), both, scatter_dimension=0, tiled=True)
    tiny8 = tiny[: 8 * count].reshape(8, count)
    return (
        output, grad_tokens,
        owned[:, :cols], owned[:, cols : 2 * cols], owned[:, 2 * cols : 3 * cols],
        owned[:, 3 * cols : 4 * cols].T,
        owned[:, 4 * cols : 4 * cols + units], owned[:, 4 * cols + units :].T,
        tiny8[0], tiny8[1], tiny8[2], tiny8[3], tiny8[4], tiny[8 * count :], tiny8[5], tiny8[6], tiny8[7],
    )


def solution(mesh):
    rows, vector, matrix, flipped = (
        P(("dp", "tensor"), None), P(("dp", "tensor")), P("dp", "tensor"), P("tensor", "dp"),
    )
    return jax.shard_map(
        shards,
        mesh=mesh,
        in_specs=(rows, P("dp"), matrix, matrix, matrix, flipped, matrix, flipped, *(vector,) * 9, rows),
        out_specs=(rows, rows, matrix, matrix, matrix, flipped, matrix, flipped, *(vector,) * 9),
        check_vma=False,
    )
```

```python
import functools

import jax
import jax.numpy as jnp
from jax import lax
from jax.experimental import pallas as pl
from jax.experimental.pallas import tpu as pltpu
from jax.sharding import PartitionSpec as P

HEAD = 64
EPSILON = 1e-12
FLOOR_SCORE = -1e30
BLOCK = 256
WIDE = 256
BF16 = jnp.bfloat16
F32 = jnp.float32
VMEM_LIMIT = 60 * 1024 * 1024


def dot_nn(a, b):
    return lax.dot_general(a, b, (((1,), (0,)), ((), ())), preferred_element_type=F32)


def dot_nt(a, b):
    return lax.dot_general(a, b, (((1,), (1,)), ((), ())), preferred_element_type=F32)


def dot_tn(a, b):
    return lax.dot_general(a, b, (((0,), (0,)), ((), ())), preferred_element_type=F32)


def lane_iota(rows, lanes):
    return lax.broadcasted_iota(jnp.int32, (rows, lanes), 1)


def row_iota(rows, lanes):
    return lax.broadcasted_iota(jnp.int32, (rows, lanes), 0)


def head_mask(rows, h, extra):
    lane = lane_iota(rows, WIDE)
    keep = (lane >= h * HEAD) & (lane < (h + 1) * HEAD)
    if extra is not None:
        keep = keep | (lane >= extra)
    return keep


def normalize(v):
    center = v - jnp.mean(v, axis=-1, keepdims=True)
    inv = lax.rsqrt(jnp.mean(center * center, axis=-1, keepdims=True) + EPSILON)
    return center * inv, inv


def norm_back(g, n, inv):
    return inv * (
        g - jnp.mean(g, axis=-1, keepdims=True) - n * jnp.mean(g * n, axis=-1, keepdims=True)
    )


def split_three(v):
    hi = v.astype(BF16)
    rest = v - hi.astype(F32)
    mid = rest.astype(BF16)
    low = (rest - mid.astype(F32)).astype(BF16)
    return hi.astype(F32), mid.astype(F32), low.astype(F32)


MESH = pl.DeviceIdType.MESH
DEPTH = 4
SLOTS = 11


def around(z, k):
    return lax.rem(z + k, DEPTH)


class Place:
    def __init__(self):
        dp, t = lax.axis_index("dp"), lax.axis_index("tensor")
        self.z, self.x = lax.div(dp, 2), lax.rem(dp, 2)
        self.y, self.c = lax.div(t, 2), lax.rem(t, 2)

    def device(self, z=None, x=None, y=None, c=None):
        z, x = self.z if z is None else z, self.x if x is None else x
        y, c = self.y if y is None else y, self.c if c is None else c
        return (z * 2 + x, y * 2 + c)

    def neighbours(self):
        return [self.device(z=around(self.z, k)) for k in range(1, DEPTH)] + [
            self.device(x=1 - self.x), self.device(y=1 - self.y), self.device(c=1 - self.c),
        ]

    def greet(self):
        barrier = pltpu.get_barrier_semaphore()
        peers = self.neighbours()
        for peer in peers:
            pl.semaphore_signal(barrier, inc=1, device_id=peer, device_id_type=MESH)
        pl.semaphore_wait(barrier, len(peers))

    def group(self, step):
        y = lax.rem(self.y + lax.div(step, 2), 2)
        c = lax.rem(self.c + lax.rem(step, 2), 2)
        return y * 2 + c


class Spread:
    def __init__(self, place, own, buf, send, recv, home, first):
        self.p, self.own, self.buf, self.send, self.recv, self.home = place, own, buf, send, recv, home
        self.first = first
        self.to_a = place.device(x=1 - place.x) if first == "x" else place.device(y=1 - place.y)
        self.to_b = place.device(y=1 - place.y) if first == "x" else place.device(x=1 - place.x)
        self.to_c = place.device(c=1 - place.c)

    def at(self, z, a=0, b=0, c=0):
        p = self.p
        dx, dy = (a, b) if self.first == "x" else (b, a)
        y = p.y if dy == 0 else 1 - p.y
        x = p.x if dx == 0 else 1 - p.x
        return self.buf.at[y, p.c if c == 0 else 1 - p.c, z, x]

    def chip(self, dy, c=0):
        p = self.p
        return self.buf.at[p.y if dy == 0 else 1 - p.y, p.c if c == 0 else 1 - p.c]

    def copy(self, src, dst, slot, device):
        return pltpu.make_async_remote_copy(
            src_ref=src, dst_ref=dst, send_sem=self.send.at[slot], recv_sem=self.recv.at[slot],
            device_id=device, device_id_type=MESH,
        )

    def arrive(self, ref, slot, device):
        self.copy(ref, ref, slot, device).wait_recv()

    def local(self):
        return pltpu.make_async_copy(self.own, self.at(self.p.z), self.home)

    def begin(self):
        p = self.p
        self.local().start()
        for k in range(1, DEPTH):
            self.copy(self.own, self.at(p.z), k - 1, p.device(z=around(p.z, k))).start()
        self.copy(self.own, self.at(p.z), 3, self.to_a).start()

    def after_z(self):
        p = self.p
        for k in range(1, DEPTH):
            ref = self.at(around(p.z, DEPTH - k))
            self.arrive(ref, k - 1, p.device(z=around(p.z, k)))
            self.copy(ref, ref, 3 + DEPTH - k, self.to_a).start()
        self.local().wait()
        ref = self.at(slice(None))
        self.copy(ref, ref, 7, self.to_b).start()

    def after_a(self):
        for k in range(DEPTH):
            self.arrive(self.at(around(self.p.z, k), a=1), 3 + k, self.to_a)
        ref = self.at(slice(None), a=1)
        self.copy(ref, ref, 8, self.to_b).start()
        if self.first == "x":
            self.swap(0)

    def swap(self, dy):
        ref = self.chip(dy)
        self.copy(ref, ref, 9 + dy, self.to_c).start()

    def after_b(self):
        self.arrive(self.at(slice(None), b=1), 7, self.to_b)
        if self.first == "y":
            self.swap(0)
        self.arrive(self.at(slice(None), a=1, b=1), 8, self.to_b)
        self.swap(1)

    def after_c(self, dy):
        self.arrive(self.chip(dy, c=1), 9 + dy, self.to_c)

    def finish(self):
        p = self.p
        one, column, chip = self.at(p.z), self.at(slice(None)), self.chip(0)
        sizes = [(one, p.device(z=around(p.z, k))) for k in range(1, DEPTH)] + [(one, self.to_a)] * DEPTH
        sizes += [(column, self.to_b)] * 2 + [(chip, self.to_c)] * 2
        for slot, (ref, device) in enumerate(sizes):
            self.copy(ref, ref, slot, device).wait_send()


def segment_tables():
    lane = jnp.arange(768, dtype=jnp.int32)
    rows = jnp.stack([lane % 24, lane // 24, lane % 96, lane // 96])
    return jnp.concatenate([rows, jnp.zeros_like(rows)])


def one_hot(tab_ref, row, start, rows):
    return (row_iota(rows, tab_ref.shape[1]) == start + tab_ref[row : row + 1, :]).astype(BF16)


def join_vectors(block_ref, tab_ref, vec_ref):
    pieces = jnp.sum(block_ref[...].reshape(32, 8, 384), axis=1)
    parts = jnp.concatenate(split_three(pieces), axis=0).astype(BF16)
    width = vec_ref.shape[1]
    row = row_iota(32, width)
    owner = lax.shift_left(row & 7, 2) + lax.shift_right_logical(row, 3)

    def place(start, table):
        got = dot_nn(parts, one_hot(tab_ref, table, start, 384))
        return got[:32] + got[32:64] + got[64:]

    for j in range(8):
        keep = owner == tab_ref[1:2, :]
        vec_ref[j : j + 1, :] = jnp.sum(jnp.where(keep, place(24 * j, 0), 0.0), axis=0, keepdims=True)
    got = place(192, 2)
    for k in range(4):
        keep = owner == tab_ref[3:4, :] + 8 * k
        vec_ref[8 + k : 9 + k, :] = jnp.sum(jnp.where(keep, got, 0.0), axis=0, keepdims=True)
    vec_ref[12:, :] = jnp.zeros((vec_ref.shape[0] - 12, width), F32)


def attend_steps(
    length, hook, x_ref, w_ref, bias_ref, g, out_bias, res_ref, q_ref, k_ref, v_ref, mix_ref, lse_ref, first
):
    rows, width = x_ref.shape
    cols = mix_ref.shape[2]
    heads = cols // HEAD

    @pl.when(first)
    def _():
        @pl.loop(0, rows, step=BLOCK)
        def _(r):
            r = pl.multiple_of(r, BLOCK)
            res_ref[pl.ds(r, BLOCK), :] = x_ref[pl.ds(r, BLOCK), :].astype(F32) + out_bias[...]

    @pl.loop(0, rows, step=BLOCK)
    def _(r):
        r = pl.multiple_of(r, BLOCK)
        here = pl.ds(r, BLOCK)
        out = dot_nn(x_ref[here, :], w_ref[0, :, : 3 * cols]) + bias_ref[g, 0:1, :]
        one = jnp.ones((BLOCK, WIDE - cols), F32)
        tail = lane_iota(BLOCK, WIDE - cols)
        position = r + row_iota(BLOCK, WIDE - cols)
        q_ref[0, here, :cols] = (out[:, :cols].astype(BF16).astype(F32) * HEAD**-0.5).astype(BF16)
        q_ref[0, here, cols:] = jnp.where(tail == 3, one, 0.0).astype(BF16)
        k_ref[0, here, :cols] = out[:, cols : 2 * cols].astype(BF16)
        bias = jnp.where(position < length, 0.0, FLOOR_SCORE)
        k_ref[0, here, cols:] = jnp.where(
            tail < 3, one, jnp.where(tail == 3, bias, 0.0)
        ).astype(BF16)
        v_ref[0, here, :cols] = out[:, 2 * cols : 3 * cols].astype(BF16)
        v_ref[0, here, cols:] = one.astype(BF16)

    @pl.loop(0, rows, step=BLOCK)
    def _(r):
        r = pl.multiple_of(r, BLOCK)
        hook(r)
        here = pl.ds(r, BLOCK)
        query = q_ref[0, here, :]
        scores = [
            dot_nt(jnp.where(head_mask(BLOCK, h, cols), query, 0), k_ref[0]) for h in range(heads)
        ]
        mixed = jnp.zeros((BLOCK, WIDE), F32)
        total = jnp.zeros((BLOCK, 128), F32)
        for h in range(heads):
            top = jnp.max(scores[h], axis=-1, keepdims=True)
            terms = jnp.exp(scores[h] - top).astype(BF16)
            got = dot_nn(terms, v_ref[0])
            denom = got[:, cols : cols + 1]
            mixed = jnp.where(head_mask(BLOCK, h, None), got * (1.0 / denom), mixed)
            total = jnp.where(lane_iota(BLOCK, 128) == h, -(top + jnp.log(denom)), total)
        low = mixed[:, :cols].astype(BF16)
        mix_ref[0, here, :] = low
        lse_ref[0, here, :] = total
        res_ref[here, :] += dot_nt(low, w_ref[0, :, 3 * cols :])


def attend_kernel(len_ref, x_ref, w_ref, bias_ref, ob_ref, *outs):
    t = pl.program_id(0)
    attend_steps(len_ref[0], lambda r: None, x_ref, w_ref, bias_ref, t, ob_ref, *outs, t == 0)


def attend_spread_kernel(
    len_ref, tab_ref, x_ref, own_vec, own_attn, own_up, own_down,
    res_ref, q_ref, k_ref, v_ref, mix_ref, lse_ref, w_ref, vec_ref, up_ref, down_ref,
    vec_buf, attn_buf, bias_buf, send, recv, home,
):
    t = pl.program_id(0)
    place = Place()
    cols = mix_ref.shape[2]

    def spread(n, own, buf, first):
        return Spread(place, own, buf, send.at[n], recv.at[n], home.at[n], first)

    small = spread(0, own_vec, vec_buf, "x")
    attn = spread(1, own_attn, attn_buf, "x")
    up = spread(2, own_up, up_ref, "y")
    down = spread(3, own_down, down_ref, "x")

    @pl.when(t == 0)
    def _():
        place.greet()
        small.begin()
        attn.begin()
        small.after_z()
        small.after_a()
        small.after_b()
        small.after_c(0)
        small.after_c(1)
        join_vectors(vec_buf, tab_ref, vec_ref)
        for g in range(bias_buf.shape[0]):
            there = slice(g * cols, (g + 1) * cols)
            bias_buf[g, 0:1, :] = jnp.concatenate(
                [vec_ref[0:1, there], jnp.zeros((1, cols), F32), vec_ref[1:2, there]], axis=1
            )
        attn.after_z()
        attn.after_a()
        up.begin()
        down.begin()

    @pl.when(t == 1)
    def _():
        attn.after_c(0)

    @pl.when(t == 3)
    def _():
        attn.after_c(1)

    def hook(r):
        def at(step, block, *events):
            @pl.when((t == step) & (r == block * BLOCK))
            def _():
                for event in events:
                    event()

        at(0, 3, up.after_z)
        at(1, 1, attn.after_b, down.after_z)
        at(1, 3, up.after_a)
        at(2, 2, down.after_a)
        at(3, 1, up.after_b)

    g = place.group(t)
    y, c = lax.div(g, 2), lax.rem(g, 2)
    for z in range(DEPTH):
        for x in range(2):
            n = attn_buf.shape[4]
            start = (z * 2 + x) * n
            w_ref[0, start : start + n, :] = attn_buf[y, c, z, x]
    attend_steps(
        len_ref[lax.axis_index("tensor")], hook, x_ref, w_ref, bias_buf, g, vec_ref.at[2:3],
        res_ref, q_ref, k_ref, v_ref, mix_ref, lse_ref, t == 0,
    )

    @pl.when(t == pl.num_programs(0) - 1)
    def _():
        down.after_b()
        for piece in (up, down):
            piece.after_c(0)
            piece.after_c(1)
        for piece in (small, attn, up, down):
            piece.finish()


def ffn_kernel(
    len_ref, res_ref, cot_ref, vec_ref, wu_ref, wd_ref,
    out_ref, gfirst_ref, gattn_ref, small_ref, gup_ref, gdn_ref,
    hid, hlow, acc, gb, act, dact, gpre,
):
    phase, t = pl.program_id(0), pl.program_id(1)
    last = pl.num_programs(1) - 1
    rows, width = res_ref.shape
    length = len_ref[0]
    gain_one, shift_one, down_bias = vec_ref[3:4, :], vec_ref[4:5, :], vec_ref[5:6, :]
    gain_two, shift_two = vec_ref[6:7, :], vec_ref[7:8, :]

    def blocks(body):
        @pl.loop(0, rows, step=BLOCK)
        def _(r):
            r = pl.multiple_of(r, BLOCK)
            body(r, pl.ds(r, BLOCK))

    def put(row, value):
        small_ref[row : row + 1, :] += jnp.sum(value, axis=0, keepdims=True)

    @pl.when((phase == 0) & (t == 0))
    def _():
        small_ref[...] = jnp.zeros_like(small_ref)

        def first(r, here):
            n, _ = normalize(res_ref[here, :])
            hidden = n * gain_one + shift_one
            hid[here, :] = hidden
            hlow[here, :] = hidden.astype(BF16)
            acc[here, :] = hidden + down_bias

        blocks(first)

    @pl.when(phase == 0)
    def _():
        def forward(r, here):
            pre = dot_nn(hlow[here, :], wu_ref[0]) + vec_ref[pl.ds(8 + t, 1), :]
            phi = 0.5 * (1.0 + lax.erf(pre * (0.5**0.5)))
            low = (pre * phi).astype(BF16)
            act[t, here, :] = low
            dact[t, here, :] = phi + pre * (jnp.exp(-0.5 * pre * pre) * 0.3989422804014327)
            acc[here, :] += dot_nt(low, wd_ref[0])

        blocks(forward)

    @pl.when((phase == 0) & (t == last))
    def _():
        def turn(r, here):
            n, inv = normalize(acc[here, :])
            valid = ((r + row_iota(BLOCK, 1)) < length).astype(F32)
            out_ref[here, :] = (n * gain_two + shift_two) * valid
            cot = cot_ref[here, :].astype(F32) * valid
            put(4, cot * n)
            put(5, cot)
            grad = norm_back(cot * gain_two, n, inv)
            acc[here, :] = grad
            low = grad.astype(BF16)
            gb[here, :] = low
            put(3, low.astype(F32))

        blocks(turn)

    @pl.when(phase == 1)
    def _():
        def backward(r, here):
            grad_act = dot_nn(gb[here, :], wd_ref[0]).astype(BF16).astype(F32)
            low = (grad_act * dact[t, here, :]).astype(BF16)
            gpre[here, :] = low
            part = dot_nt(low, wu_ref[0])

            @pl.when(t == 0)
            def _():
                hid[here, :] = part

            @pl.when(t > 0)
            def _():
                hid[here, :] += part

            small_ref[pl.ds(8 + t, 1), :] += jnp.sum(low.astype(F32), axis=0, keepdims=True)

        blocks(backward)

        @pl.loop(0, width, step=BLOCK)
        def _(c):
            c = pl.multiple_of(c, BLOCK)
            here = pl.ds(c, BLOCK)
            gdn_ref[0, here, :] = dot_tn(gb[:, here], act[t]).astype(BF16)
            gup_ref[0, here, :] = dot_tn(hlow[:, here], gpre[...]).astype(BF16)

    @pl.when((phase == 1) & (t == last))
    def _():
        def finish(r, here):
            grad_hidden = acc[here, :] + hid[here, :].astype(BF16).astype(F32)
            n, inv = normalize(res_ref[here, :])
            put(1, grad_hidden * n)
            put(2, grad_hidden)
            grad = norm_back(grad_hidden * gain_one, n, inv)
            gfirst_ref[here, :] = grad
            low = grad.astype(BF16)
            gattn_ref[here, :] = low
            put(0, low.astype(F32))

        blocks(finish)


def attend_back_kernel(
    x_ref, w_ref, gattn_ref, gfirst_ref, q_ref, k_ref, v_ref, mix_ref, lse_ref,
    gtok_ref, grad_ref, bias_ref,
    qh, gh, dq, kh, ds, dqkv,
):
    t = pl.program_id(0)
    rows, width = x_ref.shape
    cols = mix_ref.shape[2]
    heads = cols // HEAD

    @pl.when(t == 0)
    def _():
        gtok_ref[...] = gfirst_ref[...]

    bias_ref[...] = jnp.zeros_like(bias_ref)

    @pl.loop(0, rows, step=BLOCK)
    def _(r):
        r = pl.multiple_of(r, BLOCK)
        here = pl.ds(r, BLOCK)
        grad_mixed = dot_nn(gattn_ref[here, :], w_ref[0, :, 3 * cols :]).astype(BF16)
        product = grad_mixed.astype(F32) * mix_ref[0, here, :].astype(F32)
        lane = lane_iota(BLOCK, WIDE)
        wide = jnp.concatenate(
            [grad_mixed.astype(F32), jnp.zeros((BLOCK, WIDE - cols), F32)], axis=1
        )
        query = q_ref[0, here, :].astype(F32)
        key = k_ref[0, here, :]
        for h in range(heads):
            inside = (lane_iota(BLOCK, cols) >= h * HEAD) & (lane_iota(BLOCK, cols) < (h + 1) * HEAD)
            delta = jnp.sum(jnp.where(inside, product, 0.0), axis=-1, keepdims=True)
            hi, mid, low = split_three(-delta)
            keep = head_mask(BLOCK, h, None)
            tail = jnp.where(lane == cols, hi, jnp.where(lane == cols + 1, mid, jnp.where(lane == cols + 2, low, 0.0)))
            gh[h, here, :] = jnp.where(keep, wide, tail).astype(BF16)
            hi, mid, low = split_three(lse_ref[0, here, h : h + 1])
            tail = jnp.where(lane == cols, hi, jnp.where(lane == cols + 1, mid, jnp.where(lane == cols + 2, low, 0.0)))
            tail = jnp.where(lane == cols + 3, 1.0, tail)
            qh[h, here, :] = jnp.where(keep, query, tail).astype(BF16)
            kh[h, here, :] = jnp.where(keep, key, 0)

    @pl.loop(0, rows, step=BLOCK)
    def _(r):
        r = pl.multiple_of(r, BLOCK)
        here = pl.ds(r, BLOCK)
        key, value = k_ref[0, here, :], v_ref[0, here, :]
        grad_key = jnp.zeros((BLOCK, WIDE), F32)
        grad_value = jnp.zeros((BLOCK, WIDE), F32)
        logits = [dot_nt(key, qh[h]) for h in range(heads)]
        grads = [dot_nt(value, gh[h]) for h in range(heads)]
        for h in range(heads):
            prob = jnp.exp(logits[h])
            grad_value += dot_nn(prob.astype(BF16), gh[h])
            grad_score = (prob * grads[h]).astype(BF16)
            grad_key += dot_nn(grad_score, qh[h])
            part = dot_tn(grad_score, kh[h, here, :])
            if h == 0:
                total = part
            else:
                total += part

        @pl.when(r == 0)
        def _():
            dq[...] = total

        @pl.when(r > 0)
        def _():
            dq[...] += total

        low = grad_key[:, :cols].astype(BF16)
        dqkv[here, cols : 2 * cols] = low
        low = grad_value[:, :cols].astype(BF16)
        dqkv[here, 2 * cols :] = low
        bias_ref[0, 1:2, :] += jnp.sum(low.astype(F32), axis=0, keepdims=True)

    @pl.loop(0, rows, step=BLOCK)
    def _(r):
        r = pl.multiple_of(r, BLOCK)
        here = pl.ds(r, BLOCK)
        low = (dq[here, :cols] * HEAD**-0.5).astype(BF16)
        dqkv[here, :cols] = low
        bias_ref[0, 0:1, :] += jnp.sum(low.astype(F32), axis=0, keepdims=True)
        gtok_ref[here, :] += dot_nt(dqkv[here, :], w_ref[0, :, : 3 * cols])

    @pl.loop(0, width, step=BLOCK)
    def _(c):
        c = pl.multiple_of(c, BLOCK)
        here = pl.ds(c, BLOCK)
        grad_ref[0, here, : 3 * cols] = dot_tn(x_ref[:, here], dqkv[...]).astype(BF16)
        grad_ref[0, here, 3 * cols :] = dot_tn(gattn_ref[:, here], mix_ref[0]).astype(BF16)


def resident(shape):
    return pl.BlockSpec(shape, lambda *ids: (0,) * len(shape), pipeline_mode=pl.Buffered(1))


def result(shape):
    return pl.BlockSpec(shape, lambda *ids: (0,) * len(shape))


def per_step(shape):
    return pl.BlockSpec((1, *shape[1:]), lambda t: (t, 0, 0))


def struct(shape, dtype):
    return jax.ShapeDtypeStruct(shape, dtype)


def params(steps):
    return pltpu.CompilerParams(
        dimension_semantics=("arbitrary",) * steps, vmem_limit_bytes=VMEM_LIMIT
    )


def attend_outs(groups, rows, width):
    cols = width // groups
    wide = (groups, rows, WIDE)
    specs = [
        result((rows, width)),
        per_step(wide), per_step(wide), per_step(wide),
        per_step((groups, rows, cols)), per_step((groups, rows, 128)),
    ]
    shapes = [
        struct((rows, width), F32),
        struct(wide, BF16), struct(wide, BF16), struct(wide, BF16),
        struct((groups, rows, cols), BF16), struct((groups, rows, 128), F32),
    ]
    return specs, shapes


def run_attend(length, tokens, w_attn, bias, out_bias):
    rows, width = tokens.shape
    groups = w_attn.shape[0]
    specs, shapes = attend_outs(groups, rows, width)
    return pl.pallas_call(
        attend_kernel,
        grid=(groups,),
        in_specs=[
            pl.BlockSpec(memory_space=pltpu.SMEM),
            resident((rows, width)),
            per_step(w_attn.shape),
            resident(bias.shape),
            resident(out_bias.shape),
        ],
        out_specs=specs,
        out_shape=shapes,
        compiler_params=params(1),
        name="attend",
    )(length, tokens, w_attn, bias, out_bias)


def run_attend_spread(lengths, tokens, vec, w_attn, w_up, w_down):
    rows, width = tokens.shape
    groups = 4
    specs, shapes = attend_outs(groups, rows, width)
    whole = (2, 2, DEPTH, 2)
    slab = (groups, width, width)
    table = segment_tables()
    return pl.pallas_call(
        attend_spread_kernel,
        grid=(groups,),
        in_specs=[
            pl.BlockSpec(memory_space=pltpu.SMEM), resident(table.shape), resident((rows, width)),
            resident(vec.shape), resident(w_attn.shape), resident(w_up.shape), resident(w_down.shape),
        ],
        out_specs=specs + [
            per_step(slab), result((16, width)),
            pl.BlockSpec(memory_space=pl.ANY), pl.BlockSpec(memory_space=pl.ANY),
        ],
        out_shape=shapes + [
            struct(slab, BF16), struct((16, width), F32),
            struct((*whole, *w_up.shape), BF16), struct((*whole, *w_down.shape), BF16),
        ],
        scratch_shapes=[
            pltpu.VMEM((*whole, *vec.shape), F32), pltpu.VMEM((*whole, *w_attn.shape), BF16),
            pltpu.VMEM((groups, 8, 3 * width // groups), F32),
            pltpu.SemaphoreType.DMA((4, SLOTS)), pltpu.SemaphoreType.DMA((4, SLOTS)),
            pltpu.SemaphoreType.DMA((4,)),
        ],
        compiler_params=pltpu.CompilerParams(
            dimension_semantics=("arbitrary",), vmem_limit_bytes=VMEM_LIMIT, collective_id=0,
            has_side_effects=True,
        ),
        name="attend",
    )(lengths, table, tokens, vec, w_attn, w_up, w_down)


def run_ffn(length, residual, cotangent, vectors, w_up, w_down):
    rows, width = residual.shape
    groups = w_up.shape[0]
    units = w_up.shape[2]
    slab = pl.BlockSpec((1, width, units), lambda p, t: (t, 0, 0))
    grad = pl.BlockSpec((1, width, units), lambda p, t: (p * t, 0, 0))
    return pl.pallas_call(
        ffn_kernel,
        grid=(2, groups),
        in_specs=[
            pl.BlockSpec(memory_space=pltpu.SMEM),
            resident((rows, width)),
            resident((rows, width)),
            resident(vectors.shape),
            slab, slab,
        ],
        out_specs=[
            result((rows, width)), result((rows, width)), result((rows, width)), result((16, width)),
            grad, grad,
        ],
        out_shape=[
            struct((rows, width), F32), struct((rows, width), F32), struct((rows, width), BF16),
            struct((16, width), F32),
            struct(w_up.shape, BF16), struct(w_up.shape, BF16),
        ],
        scratch_shapes=[
            pltpu.VMEM((rows, width), F32), pltpu.VMEM((rows, width), BF16),
            pltpu.VMEM((rows, width), F32), pltpu.VMEM((rows, width), BF16),
            pltpu.VMEM((groups, rows, units), BF16), pltpu.VMEM((groups, rows, units), F32),
            pltpu.VMEM((rows, units), BF16),
        ],
        compiler_params=params(2),
        name="ffn",
    )(length, residual, cotangent, vectors, w_up, w_down)


def run_attend_back(tokens, w_attn, grad_attn, grad_first, q, k, v, mixed, lse):
    rows, width = tokens.shape
    groups = w_attn.shape[0]
    cols = width // groups
    heads = cols // HEAD
    return pl.pallas_call(
        attend_back_kernel,
        grid=(groups,),
        in_specs=[
            resident((rows, width)), per_step(w_attn.shape),
            resident((rows, width)), resident((rows, width)),
            per_step(q.shape), per_step(k.shape), per_step(v.shape),
            per_step(mixed.shape), per_step(lse.shape),
        ],
        out_specs=[result((rows, width)), per_step(w_attn.shape), per_step((groups, 8, cols))],
        out_shape=[
            struct((rows, width), F32), struct(w_attn.shape, BF16), struct((groups, 8, cols), F32),
        ],
        scratch_shapes=[
            pltpu.VMEM((heads, rows, WIDE), BF16), pltpu.VMEM((heads, rows, WIDE), BF16),
            pltpu.VMEM((rows, WIDE), F32), pltpu.VMEM((heads, rows, WIDE), BF16),
            pltpu.VMEM((8, 128), BF16), pltpu.VMEM((rows, 3 * cols), BF16),
        ],
        compiler_params=params(1),
        name="attend_back",
    )(tokens, w_attn, grad_attn, grad_first, q, k, v, mixed, lse)


def shards(
    tokens, lengths, w_query, w_key, w_value, w_out, w_up, w_down,
    query_bias, value_bias, out_bias, attn_gain, attn_shift, up_bias, down_bias, ffn_gain, ffn_shift,
    cotangent,
):
    rows, width = tokens.shape
    groups = lax.axis_size("tensor")
    spans = lax.axis_size("dp")
    seq_count = lengths.shape[0]
    assert rows * groups == seq_count * rows and seq_count == groups
    rank = lax.axis_index("tensor")
    length = lax.dynamic_slice_in_dim(lengths, rank, 1)
    both = ("dp", "tensor")

    cols = width // groups
    units = w_up.shape[1]
    count = query_bias.shape[0]
    vectors = (query_bias, value_bias, out_bias, attn_gain, attn_shift, down_bias, ffn_gain, ffn_shift)
    flat = jnp.concatenate([*vectors, up_bias])
    own_attn = jnp.concatenate([w_query, w_key, w_value, w_out.T], axis=1)

    near = (spans, groups, width, units) == (8, 4, 768, 768)
    if near:
        vec = jnp.pad(flat[None], ((0, 7), (0, 384 - flat.shape[0])))
        residual, q, k, v, mixed, lse, w_attn, full, w_in, w_back = run_attend_spread(
            lengths, tokens, vec, own_attn, w_up, w_down.T
        )
        w_in, w_back = w_in.reshape(groups, width, units), w_back.reshape(groups, width, units)
    else:
        pack = jnp.concatenate([own_attn, w_up, w_down.T], axis=1)
        whole = lax.all_gather(pack, both, axis=0, tiled=True)
        whole = whole.reshape(spans, groups, *pack.shape).swapaxes(0, 1)
        whole = whole.reshape(groups, width, pack.shape[1])
        w_attn, w_in, w_back = jnp.split(whole, [4 * cols, 4 * cols + units], axis=2)
        gathered = lax.all_gather(flat, both, axis=0, tiled=True).reshape(spans * groups, -1)
        full = gathered[:, : 8 * count].reshape(-1, 8, count).swapaxes(0, 1).reshape(8, width)
        full = jnp.concatenate([full, gathered[:, 8 * count :].reshape(groups, units)])
        full = jnp.pad(full, ((0, 16 - full.shape[0]), (0, 0)))
        qb, vb = full[0].reshape(groups, 1, cols), full[1].reshape(groups, 1, cols)
        bias = jnp.pad(jnp.concatenate([qb, jnp.zeros_like(qb), vb], axis=2), ((0, 0), (0, 7), (0, 0)))
        residual, q, k, v, mixed, lse = run_attend(length, tokens, w_attn, bias, full[2:3])
    output, grad_first, grad_attn, small, grad_in, grad_back = run_ffn(
        length, residual, cotangent, full, w_in, w_back
    )
    grad_tokens, grad_attn_w, bias_grad = run_attend_back(
        tokens, w_attn, grad_attn, grad_first, q, k, v, mixed, lse
    )

    if near:
        mine = jnp.arange(groups) ^ rank
        grad_attn_w, bias_grad = grad_attn_w[mine], bias_grad[mine]
    every = jnp.concatenate([grad_attn_w, grad_in, grad_back], axis=2)
    every = every.reshape(groups, spans, width // spans, -1).swapaxes(0, 1)
    every = every.reshape(spans * groups * (width // spans), -1)
    owned = lax.psum_scatter(every, both, scatter_dimension=0, tiled=True).astype(F32)

    rows8 = jnp.concatenate(
        [bias_grad[:, 0].reshape(1, width), bias_grad[:, 1].reshape(1, width), small[:6]]
    )
    parts = jnp.concatenate(
        [
            rows8.reshape(8, spans * groups, count).swapaxes(0, 1).reshape(spans * groups, 8 * count),
            small[8 : 8 + groups].reshape(spans * groups, -1),
        ],
        axis=1,
    )
    tiny = lax.psum_scatter(parts.reshape(-1), both, scatter_dimension=0, tiled=True)
    tiny8 = tiny[: 8 * count].reshape(8, count)
    return (
        output, grad_tokens,
        owned[:, :cols], owned[:, cols : 2 * cols], owned[:, 2 * cols : 3 * cols],
        owned[:, 3 * cols : 4 * cols].T,
        owned[:, 4 * cols : 4 * cols + units], owned[:, 4 * cols + units :].T,
        tiny8[0], tiny8[1], tiny8[2], tiny8[3], tiny8[4], tiny[8 * count :], tiny8[5], tiny8[6], tiny8[7],
    )


def solution(mesh):
    rows, vector, matrix, flipped = (
        P(("dp", "tensor"), None), P(("dp", "tensor")), P("dp", "tensor"), P("tensor", "dp"),
    )
    return jax.shard_map(
        shards,
        mesh=mesh,
        in_specs=(rows, P("dp"), matrix, matrix, matrix, flipped, matrix, flipped, *(vector,) * 9, rows),
        out_specs=(rows, rows, matrix, matrix, matrix, flipped, matrix, flipped, *(vector,) * 9),
        check_vma=False,
    )
```

```python
import functools

import jax
import jax.numpy as jnp
from jax import lax
from jax.experimental import pallas as pl
from jax.experimental.pallas import tpu as pltpu
from jax.sharding import PartitionSpec as P

HEAD = 64
EPSILON = 1e-12
FLOOR_SCORE = -1e30
BLOCK = 256
WIDE = 256
BF16 = jnp.bfloat16
F32 = jnp.float32
VMEM_LIMIT = 60 * 1024 * 1024


def dot_nn(a, b):
    return lax.dot_general(a, b, (((1,), (0,)), ((), ())), preferred_element_type=F32)


def dot_nt(a, b):
    return lax.dot_general(a, b, (((1,), (1,)), ((), ())), preferred_element_type=F32)


def dot_tn(a, b):
    return lax.dot_general(a, b, (((0,), (0,)), ((), ())), preferred_element_type=F32)


def lane_iota(rows, lanes):
    return lax.broadcasted_iota(jnp.int32, (rows, lanes), 1)


def row_iota(rows, lanes):
    return lax.broadcasted_iota(jnp.int32, (rows, lanes), 0)


def head_mask(rows, h, extra):
    lane = lane_iota(rows, WIDE)
    keep = (lane >= h * HEAD) & (lane < (h + 1) * HEAD)
    if extra is not None:
        keep = keep | (lane >= extra)
    return keep


def normalize(v):
    center = v - jnp.mean(v, axis=-1, keepdims=True)
    inv = lax.rsqrt(jnp.mean(center * center, axis=-1, keepdims=True) + EPSILON)
    return center * inv, inv


def norm_back(g, n, inv):
    return inv * (
        g - jnp.mean(g, axis=-1, keepdims=True) - n * jnp.mean(g * n, axis=-1, keepdims=True)
    )


def split_three(v):
    hi = v.astype(BF16)
    rest = v - hi.astype(F32)
    mid = rest.astype(BF16)
    low = (rest - mid.astype(F32)).astype(BF16)
    return hi.astype(F32), mid.astype(F32), low.astype(F32)


MESH = pl.DeviceIdType.MESH
DEPTH = 4
SLOTS = 11


def around(z, k):
    return lax.rem(z + k, DEPTH)


class Place:
    def __init__(self):
        dp, t = lax.axis_index("dp"), lax.axis_index("tensor")
        self.z, self.x = lax.div(dp, 2), lax.rem(dp, 2)
        self.y, self.c = lax.div(t, 2), lax.rem(t, 2)

    def device(self, z=None, x=None, y=None, c=None):
        z, x = self.z if z is None else z, self.x if x is None else x
        y, c = self.y if y is None else y, self.c if c is None else c
        return (z * 2 + x, y * 2 + c)

    def neighbours(self):
        return [self.device(z=around(self.z, k)) for k in range(1, DEPTH)] + [
            self.device(x=1 - self.x), self.device(y=1 - self.y), self.device(c=1 - self.c),
        ]

    def greet(self):
        barrier = pltpu.get_barrier_semaphore()
        peers = self.neighbours()
        for peer in peers:
            pl.semaphore_signal(barrier, inc=1, device_id=peer, device_id_type=MESH)
        pl.semaphore_wait(barrier, len(peers))

    def group(self, step):
        y = lax.rem(self.y + lax.div(step, 2), 2)
        c = lax.rem(self.c + lax.rem(step, 2), 2)
        return y * 2 + c


class Spread:
    def __init__(self, place, own, buf, send, recv, home, first):
        self.p, self.own, self.buf, self.send, self.recv, self.home = place, own, buf, send, recv, home
        self.first = first
        self.to_a = place.device(x=1 - place.x) if first == "x" else place.device(y=1 - place.y)
        self.to_b = place.device(y=1 - place.y) if first == "x" else place.device(x=1 - place.x)
        self.to_c = place.device(c=1 - place.c)

    def at(self, z, a=0, b=0, c=0):
        p = self.p
        dx, dy = (a, b) if self.first == "x" else (b, a)
        y = p.y if dy == 0 else 1 - p.y
        x = p.x if dx == 0 else 1 - p.x
        return self.buf.at[y, p.c if c == 0 else 1 - p.c, z, x]

    def chip(self, dy, c=0):
        p = self.p
        return self.buf.at[p.y if dy == 0 else 1 - p.y, p.c if c == 0 else 1 - p.c]

    def copy(self, src, dst, slot, device):
        return pltpu.make_async_remote_copy(
            src_ref=src, dst_ref=dst, send_sem=self.send.at[slot], recv_sem=self.recv.at[slot],
            device_id=device, device_id_type=MESH,
        )

    def arrive(self, ref, slot, device):
        self.copy(ref, ref, slot, device).wait_recv()

    def local(self):
        return pltpu.make_async_copy(self.own, self.at(self.p.z), self.home)

    def begin(self):
        p = self.p
        self.local().start()
        for k in range(1, DEPTH):
            self.copy(self.own, self.at(p.z), k - 1, p.device(z=around(p.z, k))).start()
        self.copy(self.own, self.at(p.z), 3, self.to_a).start()

    def after_z(self):
        p = self.p
        for k in range(1, DEPTH):
            ref = self.at(around(p.z, DEPTH - k))
            self.arrive(ref, k - 1, p.device(z=around(p.z, k)))
            self.copy(ref, ref, 3 + DEPTH - k, self.to_a).start()
        self.local().wait()
        ref = self.at(slice(None))
        self.copy(ref, ref, 7, self.to_b).start()

    def after_a(self):
        for k in range(DEPTH):
            self.arrive(self.at(around(self.p.z, k), a=1), 3 + k, self.to_a)
        ref = self.at(slice(None), a=1)
        self.copy(ref, ref, 8, self.to_b).start()
        if self.first == "x":
            self.swap(0)

    def swap(self, dy):
        ref = self.chip(dy)
        self.copy(ref, ref, 9 + dy, self.to_c).start()

    def after_b(self):
        self.arrive(self.at(slice(None), b=1), 7, self.to_b)
        if self.first == "y":
            self.swap(0)
        self.arrive(self.at(slice(None), a=1, b=1), 8, self.to_b)
        self.swap(1)

    def after_c(self, dy):
        self.arrive(self.chip(dy, c=1), 9 + dy, self.to_c)

    def finish(self):
        p = self.p
        one, column, chip = self.at(p.z), self.at(slice(None)), self.chip(0)
        sizes = [(one, p.device(z=around(p.z, k))) for k in range(1, DEPTH)] + [(one, self.to_a)] * DEPTH
        sizes += [(column, self.to_b)] * 2 + [(chip, self.to_c)] * 2
        for slot, (ref, device) in enumerate(sizes):
            self.copy(ref, ref, slot, device).wait_send()


class Collect:
    def __init__(self, place, near, far, rc, rb, ra, rz, send, recv, last):
        self.p, self.near, self.far, self.last = place, near, far, last
        self.rc, self.rb, self.ra, self.rz, self.send, self.recv = rc, rb, ra, rz, send, recv
        to_x, to_y = place.device(x=1 - place.x), place.device(y=1 - place.y)
        self.to_a, self.to_b = (to_x, to_y) if last == "x" else (to_y, to_x)
        self.to_c = place.device(c=1 - place.c)

    def copy(self, src, dst, slot, device):
        return pltpu.make_async_remote_copy(
            src_ref=src, dst_ref=dst, send_sem=self.send.at[slot], recv_sem=self.recv.at[slot],
            device_id=device, device_id_type=MESH,
        )

    def copy_c(self, src, dy):
        return self.copy(src, self.rc.at[dy], dy, self.to_c)

    def copies_b(self):
        if self.last == "x":
            return [self.copy(self.far, self.rb, 2, self.to_b)]
        there = (slice(None), 1 - self.p.x)
        return [
            self.copy(part.at[there], self.rb.at[dy], 2 + 5 * dy, self.to_b)
            for dy, part in enumerate((self.near, self.far))
        ]

    def copy_a(self):
        if self.last == "x":
            return self.copy(self.near.at[:, 1 - self.p.x], self.ra, 3, self.to_a)
        return self.copy(self.far.at[:, self.p.x], self.ra, 3, self.to_a)

    def copies_z(self):
        p = self.p
        return [
            self.copy(
                self.near.at[around(p.z, k), p.x], self.rz.at[k - 1], 3 + k, p.device(z=around(p.z, k))
            )
            for k in range(1, DEPTH)
        ]

    def wait_c(self, dy):
        self.copy_c(self.rc.at[dy], dy).wait_recv()

    def wait_b(self):
        for copy in self.copies_b():
            copy.wait_recv()

    def sum_c(self):
        for dy, part in enumerate((self.near, self.far)):
            self.wait_c(dy)

            @pl.loop(0, DEPTH)
            def _(z):
                part[z] = add(part[z], self.rc[dy, z]).astype(part.dtype)

    def send_b(self):
        for copy in self.copies_b():
            copy.start()

    def sum_b(self):
        self.wait_b()
        x = self.p.x

        @pl.loop(0, DEPTH)
        def _(z):
            if self.last == "x":
                self.near[z] = add(self.near[z], self.rb[z]).astype(self.near.dtype)
            else:
                for dy, part in enumerate((self.near, self.far)):
                    part[z, x] = add(part[z, x], self.rb[dy, z]).astype(part.dtype)

    def send_a(self):
        self.copy_a().start()

    def sum_a(self):
        self.copy_a().wait_recv()
        x = self.p.x

        @pl.loop(0, DEPTH)
        def _(z):
            self.near[z, x] = add(self.near[z, x], self.ra[z]).astype(self.near.dtype)

    def send_z(self):
        for copy in self.copies_z():
            copy.start()

    def sum_z(self, out_ref):
        for copy in self.copies_z():
            copy.wait_recv()
        total = self.near[self.p.z, self.p.x].astype(F32)
        for k in range(DEPTH - 1):
            total = total + self.rz[k].astype(F32)
        out_ref[...] = total

    def finish(self):
        for dy in range(2):
            self.copy_c(self.rc.at[dy], dy).wait_send()
        for copy in [*self.copies_b(), self.copy_a(), *self.copies_z()]:
            copy.wait_send()


def add(a, b):
    return a.astype(F32) + b.astype(F32)


def segment_tables():
    lane = jnp.arange(768, dtype=jnp.int32)
    rows = jnp.stack([lane % 24, lane // 24, lane % 96, lane // 96])
    return jnp.concatenate([rows, jnp.zeros_like(rows)])


def one_hot(tab_ref, row, start, rows):
    return (row_iota(rows, tab_ref.shape[1]) == start + tab_ref[row : row + 1, :]).astype(BF16)


def join_vectors(block_ref, tab_ref, vec_ref):
    pieces = jnp.sum(block_ref[...].reshape(32, 8, 384), axis=1)
    parts = jnp.concatenate(split_three(pieces), axis=0).astype(BF16)
    width = vec_ref.shape[1]
    row = row_iota(32, width)
    owner = lax.shift_left(row & 7, 2) + lax.shift_right_logical(row, 3)

    def place(start, table):
        got = dot_nn(parts, one_hot(tab_ref, table, start, 384))
        return got[:32] + got[32:64] + got[64:]

    for j in range(8):
        keep = owner == tab_ref[1:2, :]
        vec_ref[j : j + 1, :] = jnp.sum(jnp.where(keep, place(24 * j, 0), 0.0), axis=0, keepdims=True)
    got = place(192, 2)
    for k in range(4):
        keep = owner == tab_ref[3:4, :] + 8 * k
        vec_ref[8 + k : 9 + k, :] = jnp.sum(jnp.where(keep, got, 0.0), axis=0, keepdims=True)
    vec_ref[12:, :] = jnp.zeros((vec_ref.shape[0] - 12, width), F32)


def cut_vectors(eight, up_rows, tab_ref, out_ref):
    width = tab_ref.shape[1]

    def owners(shape, dim):
        p = lax.broadcasted_iota(jnp.int32, shape, dim)
        return lax.shift_left(p & 7, 2) + lax.shift_right_logical(p, 3)

    def pick(values, table):
        hot = one_hot(tab_ref, table, 0, 128)
        return sum(dot_nt(part.astype(BF16), hot) for part in split_three(values))

    both = jnp.concatenate([eight, jnp.zeros_like(eight)], axis=0)
    keep = owners((32, 16, width), 0) == tab_ref[1:2, :][None]
    spread = jnp.where(keep, jnp.broadcast_to(both[None], (32, 16, width)), 0.0)
    blocks = pick(spread.reshape(512, width), 0).reshape(32, 16, 128)
    owner = owners((32, width), 0)
    ups = jnp.zeros((32, width), F32)
    for k in range(4):
        ups = jnp.where(owner == tab_ref[3:4, :] + 8 * k, up_rows[k : k + 1, :], ups)
    ups = jnp.broadcast_to(pick(ups, 2)[:, None, :], (32, 16, 128))
    blocks = jnp.where(lax.broadcasted_iota(jnp.int32, (32, 16, 128), 1) == 8, ups, blocks)
    out_ref[...] = blocks.reshape(out_ref.shape)


def attend_steps(
    length, hook, x_ref, w_ref, bias_ref, g, out_bias, res_ref, q_ref, k_ref, v_ref, mix_ref, lse_ref, first
):
    rows, width = x_ref.shape
    cols = mix_ref.shape[2]
    heads = cols // HEAD

    @pl.when(first)
    def _():
        @pl.loop(0, rows, step=BLOCK)
        def _(r):
            r = pl.multiple_of(r, BLOCK)
            res_ref[pl.ds(r, BLOCK), :] = x_ref[pl.ds(r, BLOCK), :].astype(F32) + out_bias[...]

    @pl.loop(0, rows, step=BLOCK)
    def _(r):
        r = pl.multiple_of(r, BLOCK)
        here = pl.ds(r, BLOCK)
        out = dot_nn(x_ref[here, :], w_ref[0, :, : 3 * cols]) + bias_ref[g, 0:1, :]
        one = jnp.ones((BLOCK, WIDE - cols), F32)
        tail = lane_iota(BLOCK, WIDE - cols)
        position = r + row_iota(BLOCK, WIDE - cols)
        q_ref[0, here, :cols] = (out[:, :cols].astype(BF16).astype(F32) * HEAD**-0.5).astype(BF16)
        q_ref[0, here, cols:] = jnp.where(tail == 3, one, 0.0).astype(BF16)
        k_ref[0, here, :cols] = out[:, cols : 2 * cols].astype(BF16)
        bias = jnp.where(position < length, 0.0, FLOOR_SCORE)
        k_ref[0, here, cols:] = jnp.where(
            tail < 3, one, jnp.where(tail == 3, bias, 0.0)
        ).astype(BF16)
        v_ref[0, here, :cols] = out[:, 2 * cols : 3 * cols].astype(BF16)
        v_ref[0, here, cols:] = one.astype(BF16)

    @pl.loop(0, rows, step=BLOCK)
    def _(r):
        r = pl.multiple_of(r, BLOCK)
        hook(r)
        here = pl.ds(r, BLOCK)
        query = q_ref[0, here, :]
        scores = [
            dot_nt(jnp.where(head_mask(BLOCK, h, cols), query, 0), k_ref[0]) for h in range(heads)
        ]
        mixed = jnp.zeros((BLOCK, WIDE), F32)
        total = jnp.zeros((BLOCK, 128), F32)
        for h in range(heads):
            top = jnp.max(scores[h], axis=-1, keepdims=True)
            terms = jnp.exp(scores[h] - top).astype(BF16)
            got = dot_nn(terms, v_ref[0])
            denom = got[:, cols : cols + 1]
            mixed = jnp.where(head_mask(BLOCK, h, None), got * (1.0 / denom), mixed)
            total = jnp.where(lane_iota(BLOCK, 128) == h, -(top + jnp.log(denom)), total)
        low = mixed[:, :cols].astype(BF16)
        mix_ref[0, here, :] = low
        lse_ref[0, here, :] = total
        res_ref[here, :] += dot_nt(low, w_ref[0, :, 3 * cols :])


def attend_kernel(len_ref, x_ref, w_ref, bias_ref, ob_ref, *outs):
    t = pl.program_id(0)
    attend_steps(len_ref[0], lambda r: None, x_ref, w_ref, bias_ref, t, ob_ref, *outs, t == 0)


def attend_spread_kernel(
    len_ref, tab_ref, x_ref, own_vec, own_attn, own_up, own_down,
    res_ref, q_ref, k_ref, v_ref, mix_ref, lse_ref, w_ref, vec_ref, up_ref, down_ref,
    vec_buf, attn_buf, bias_buf, send, recv, home,
):
    t = pl.program_id(0)
    place = Place()
    cols = mix_ref.shape[2]

    def spread(n, own, buf, first):
        return Spread(place, own, buf, send.at[n], recv.at[n], home.at[n], first)

    small = spread(0, own_vec, vec_buf, "x")
    attn = spread(1, own_attn, attn_buf, "x")
    up = spread(2, own_up, up_ref, "y")
    down = spread(3, own_down, down_ref, "x")

    @pl.when(t == 0)
    def _():
        place.greet()
        small.begin()
        attn.begin()
        small.after_z()
        small.after_a()
        small.after_b()
        small.after_c(0)
        small.after_c(1)
        join_vectors(vec_buf, tab_ref, vec_ref)
        for g in range(bias_buf.shape[0]):
            there = slice(g * cols, (g + 1) * cols)
            bias_buf[g, 0:1, :] = jnp.concatenate(
                [vec_ref[0:1, there], jnp.zeros((1, cols), F32), vec_ref[1:2, there]], axis=1
            )
        attn.after_z()
        attn.after_a()
        up.begin()
        down.begin()

    @pl.when(t == 1)
    def _():
        attn.after_c(0)

    @pl.when(t == 3)
    def _():
        attn.after_c(1)

    def hook(r):
        def at(step, block, *events):
            @pl.when((t == step) & (r == block * BLOCK))
            def _():
                for event in events:
                    event()

        at(0, 3, up.after_z)
        at(1, 1, attn.after_b, down.after_z)
        at(1, 3, up.after_a)
        at(2, 2, down.after_a)
        at(3, 1, up.after_b)

    g = place.group(t)
    y, c = lax.div(g, 2), lax.rem(g, 2)
    for z in range(DEPTH):
        for x in range(2):
            n = attn_buf.shape[4]
            start = (z * 2 + x) * n
            w_ref[0, start : start + n, :] = attn_buf[y, c, z, x]
    attend_steps(
        len_ref[lax.axis_index("tensor")], hook, x_ref, w_ref, bias_buf, g, vec_ref.at[2:3],
        res_ref, q_ref, k_ref, v_ref, mix_ref, lse_ref, t == 0,
    )

    @pl.when(t == pl.num_programs(0) - 1)
    def _():
        down.after_b()
        for piece in (up, down):
            piece.after_c(0)
            piece.after_c(1)
        for piece in (small, attn, up, down):
            piece.finish()


def ffn_kernel(
    len_ref, res_ref, cot_ref, vec_ref, wu_ref, wd_ref,
    out_ref, gfirst_ref, gattn_ref, small_ref, gup_ref, gdn_ref,
    hid, hlow, acc, gb, act, dact, gpre,
):
    phase, t = pl.program_id(0), pl.program_id(1)
    last = pl.num_programs(1) - 1
    rows, width = res_ref.shape
    length = len_ref[0]
    gain_one, shift_one, down_bias = vec_ref[3:4, :], vec_ref[4:5, :], vec_ref[5:6, :]
    gain_two, shift_two = vec_ref[6:7, :], vec_ref[7:8, :]

    def blocks(body):
        @pl.loop(0, rows, step=BLOCK)
        def _(r):
            r = pl.multiple_of(r, BLOCK)
            body(r, pl.ds(r, BLOCK))

    def put(row, value):
        small_ref[row : row + 1, :] += jnp.sum(value, axis=0, keepdims=True)

    @pl.when((phase == 0) & (t == 0))
    def _():
        small_ref[...] = jnp.zeros_like(small_ref)

        def first(r, here):
            n, _ = normalize(res_ref[here, :])
            hidden = n * gain_one + shift_one
            hid[here, :] = hidden
            hlow[here, :] = hidden.astype(BF16)
            acc[here, :] = hidden + down_bias

        blocks(first)

    @pl.when(phase == 0)
    def _():
        def forward(r, here):
            pre = dot_nn(hlow[here, :], wu_ref[0]) + vec_ref[pl.ds(8 + t, 1), :]
            phi = 0.5 * (1.0 + lax.erf(pre * (0.5**0.5)))
            low = (pre * phi).astype(BF16)
            act[t, here, :] = low
            dact[t, here, :] = phi + pre * (jnp.exp(-0.5 * pre * pre) * 0.3989422804014327)
            acc[here, :] += dot_nt(low, wd_ref[0])

        blocks(forward)

    @pl.when((phase == 0) & (t == last))
    def _():
        def turn(r, here):
            n, inv = normalize(acc[here, :])
            valid = ((r + row_iota(BLOCK, 1)) < length).astype(F32)
            out_ref[here, :] = (n * gain_two + shift_two) * valid
            cot = cot_ref[here, :].astype(F32) * valid
            put(4, cot * n)
            put(5, cot)
            grad = norm_back(cot * gain_two, n, inv)
            acc[here, :] = grad
            low = grad.astype(BF16)
            gb[here, :] = low
            put(3, low.astype(F32))

        blocks(turn)

    @pl.when(phase == 1)
    def _():
        def backward(r, here):
            grad_act = dot_nn(gb[here, :], wd_ref[0]).astype(BF16).astype(F32)
            low = (grad_act * dact[t, here, :]).astype(BF16)
            gpre[here, :] = low
            part = dot_nt(low, wu_ref[0])

            @pl.when(t == 0)
            def _():
                hid[here, :] = part

            @pl.when(t > 0)
            def _():
                hid[here, :] += part

            small_ref[pl.ds(8 + t, 1), :] += jnp.sum(low.astype(F32), axis=0, keepdims=True)

        blocks(backward)

        @pl.loop(0, width, step=BLOCK)
        def _(c):
            c = pl.multiple_of(c, BLOCK)
            here = pl.ds(c, BLOCK)
            gdn_ref[0, here, :] = dot_tn(gb[:, here], act[t]).astype(BF16)
            gup_ref[0, here, :] = dot_tn(hlow[:, here], gpre[...]).astype(BF16)

    @pl.when((phase == 1) & (t == last))
    def _():
        def finish(r, here):
            grad_hidden = acc[here, :] + hid[here, :].astype(BF16).astype(F32)
            n, inv = normalize(res_ref[here, :])
            put(1, grad_hidden * n)
            put(2, grad_hidden)
            grad = norm_back(grad_hidden * gain_one, n, inv)
            gfirst_ref[here, :] = grad
            low = grad.astype(BF16)
            gattn_ref[here, :] = low
            put(0, low.astype(F32))

        blocks(finish)


def attend_back_steps(
    hook, before_grads, put_grads,
    x_ref, w_ref, gattn_ref, gfirst_ref, q_ref, k_ref, v_ref, mix_ref, lse_ref, gtok_ref, bias_ref,
    qh, gh, dq, kh, dqkv,
):
    t = pl.program_id(0)
    rows, width = x_ref.shape
    cols = mix_ref.shape[2]
    heads = cols // HEAD

    @pl.when(t == 0)
    def _():
        gtok_ref[...] = gfirst_ref[...]

    bias_ref[...] = jnp.zeros_like(bias_ref)

    @pl.loop(0, rows, step=BLOCK)
    def _(r):
        r = pl.multiple_of(r, BLOCK)
        here = pl.ds(r, BLOCK)
        grad_mixed = dot_nn(gattn_ref[here, :], w_ref[0, :, 3 * cols :]).astype(BF16)
        product = grad_mixed.astype(F32) * mix_ref[0, here, :].astype(F32)
        lane = lane_iota(BLOCK, WIDE)
        wide = jnp.concatenate(
            [grad_mixed.astype(F32), jnp.zeros((BLOCK, WIDE - cols), F32)], axis=1
        )
        query = q_ref[0, here, :].astype(F32)
        key = k_ref[0, here, :]
        for h in range(heads):
            inside = (lane_iota(BLOCK, cols) >= h * HEAD) & (lane_iota(BLOCK, cols) < (h + 1) * HEAD)
            delta = jnp.sum(jnp.where(inside, product, 0.0), axis=-1, keepdims=True)
            hi, mid, low = split_three(-delta)
            keep = head_mask(BLOCK, h, None)
            tail = jnp.where(lane == cols, hi, jnp.where(lane == cols + 1, mid, jnp.where(lane == cols + 2, low, 0.0)))
            gh[h, here, :] = jnp.where(keep, wide, tail).astype(BF16)
            hi, mid, low = split_three(lse_ref[0, here, h : h + 1])
            tail = jnp.where(lane == cols, hi, jnp.where(lane == cols + 1, mid, jnp.where(lane == cols + 2, low, 0.0)))
            tail = jnp.where(lane == cols + 3, 1.0, tail)
            qh[h, here, :] = jnp.where(keep, query, tail).astype(BF16)
            kh[h, here, :] = jnp.where(keep, key, 0)

    @pl.loop(0, rows, step=BLOCK)
    def _(r):
        r = pl.multiple_of(r, BLOCK)
        hook(r)
        here = pl.ds(r, BLOCK)
        key, value = k_ref[0, here, :], v_ref[0, here, :]
        grad_key = jnp.zeros((BLOCK, WIDE), F32)
        grad_value = jnp.zeros((BLOCK, WIDE), F32)
        logits = [dot_nt(key, qh[h]) for h in range(heads)]
        grads = [dot_nt(value, gh[h]) for h in range(heads)]
        for h in range(heads):
            prob = jnp.exp(logits[h])
            grad_value += dot_nn(prob.astype(BF16), gh[h])
            grad_score = (prob * grads[h]).astype(BF16)
            grad_key += dot_nn(grad_score, qh[h])
            part = dot_tn(grad_score, kh[h, here, :])
            if h == 0:
                total = part
            else:
                total += part

        @pl.when(r == 0)
        def _():
            dq[...] = total

        @pl.when(r > 0)
        def _():
            dq[...] += total

        low = grad_key[:, :cols].astype(BF16)
        dqkv[here, cols : 2 * cols] = low
        low = grad_value[:, :cols].astype(BF16)
        dqkv[here, 2 * cols :] = low
        bias_ref[0, 1:2, :] += jnp.sum(low.astype(F32), axis=0, keepdims=True)

    @pl.loop(0, rows, step=BLOCK)
    def _(r):
        r = pl.multiple_of(r, BLOCK)
        here = pl.ds(r, BLOCK)
        low = (dq[here, :cols] * HEAD**-0.5).astype(BF16)
        dqkv[here, :cols] = low
        bias_ref[0, 0:1, :] += jnp.sum(low.astype(F32), axis=0, keepdims=True)
        gtok_ref[here, :] += dot_nt(dqkv[here, :], w_ref[0, :, : 3 * cols])

    before_grads()
    half = width // 2

    @pl.loop(0, width, step=half)
    def _(c):
        c = pl.multiple_of(c, half)
        here = pl.ds(c, half)
        put_grads(c, dot_tn(x_ref[:, here], dqkv[...]), dot_tn(gattn_ref[:, here], mix_ref[0]))


def attend_back_kernel(
    x_ref, w_ref, gattn_ref, gfirst_ref, q_ref, k_ref, v_ref, mix_ref, lse_ref,
    gtok_ref, grad_ref, bias_ref,
    *scratch,
):
    wide = 3 * mix_ref.shape[2]

    def put(c, qkv, out):
        here = pl.ds(c, qkv.shape[0])
        grad_ref[0, here, :wide] = qkv.astype(BF16)
        grad_ref[0, here, wide:] = out.astype(BF16)

    attend_back_steps(
        lambda r: None, lambda: None, put,
        x_ref, w_ref, gattn_ref, gfirst_ref, q_ref, k_ref, v_ref, mix_ref, lse_ref, gtok_ref, bias_ref,
        *scratch,
    )


def attend_back_collect_kernel(
    tab_ref, x_ref, w_ref, gattn_ref, gfirst_ref, q_ref, k_ref, v_ref, mix_ref, lse_ref, vec_ref,
    gup_ref, gdn_ref,
    gtok_ref, attn_out, up_out, down_out, small_out,
    qh, gh, dq, kh, dqkv, bias_ref, bias_all,
    gs, attn_rc, attn_rb, attn_ra, attn_rz,
    up_acc, up_rc, up_rb, up_ra, up_rz,
    down_acc, down_rc, down_rb, down_ra, down_rz,
    small_src, small_acc, small_rc, small_rb, small_ra, small_rz,
    send, recv, home,
):
    t = pl.program_id(0)
    last = pl.num_programs(0) - 1
    place = Place()
    cols = mix_ref.shape[2]
    wide = 3 * cols

    def collect(n, near, far, rc, rb, ra, rz, axis):
        return Collect(place, near, far, rc, rb, ra, rz, send.at[n], recv.at[n], axis)

    attn = collect(0, gs.at[3], gs.at[1], attn_rc, attn_rb, attn_ra, attn_rz, "x")
    up = collect(1, up_acc.at[0], up_acc.at[1], up_rc, up_rb, up_ra, up_rz, "x")
    down = collect(2, down_acc.at[0], down_acc.at[1], down_rc, down_rb, down_ra, down_rz, "y")
    small = collect(3, small_acc.at[0], small_acc.at[1], small_rc, small_rb, small_ra, small_rz, "x")
    rows_y = (place.y, 1 - place.y)

    def homes(src, acc, n):
        return [
            pltpu.make_async_copy(src.at[y, place.c], acc.at[dy], home.at[n, dy])
            for dy, y in enumerate(rows_y)
        ]

    def begin(piece, src, acc, n):
        for copy in homes(src, acc, n):
            copy.start()
        for dy, y in enumerate(rows_y):
            piece.copy_c(src.at[y, 1 - place.c], dy).start()

    def settle(src, acc, n):
        for copy in homes(src, acc, n):
            copy.wait()

    @pl.when(t == 0)
    def _():
        place.greet()
        begin(up, gup_ref, up_acc, 0)
        begin(down, gdn_ref, down_acc, 1)
        settle(gup_ref, up_acc, 0)
        settle(gdn_ref, down_acc, 1)

    @pl.when(t == 1)
    def _():
        down.send_b()
        attn.copy_c(gs.at[0], 1).start()

    @pl.when(t == 2)
    def _():
        down.sum_b()

    @pl.when(t == 3)
    def _():
        up.send_z()
        attn.copy_c(gs.at[2], 0).start()

    def hook(r):
        def at(step, block, *events):
            @pl.when((t == step) & (r == block * BLOCK))
            def _():
                for event in events:
                    event()

        at(0, 1, up.sum_c)
        at(0, 2, up.send_b)
        at(0, 3, down.sum_c)
        at(1, 3, up.sum_b)
        at(2, 0, up.send_a, down.send_a, attn.send_b)
        at(2, 3, up.sum_a)
        at(3, 1, down.sum_a)
        at(3, 2, down.send_z)

    g = place.group(last - t)

    def before_grads():
        bias_all[g] = bias_ref[0]

        @pl.when(t == 1)
        def _():
            attn.wait_c(1)

        @pl.when(t == last)
        def _():
            lines = [
                jnp.concatenate([bias_all[n, row : row + 1, :] for n in range(bias_all.shape[0])], axis=1)
                for row in range(2)
            ]
            cut_vectors(jnp.concatenate([*lines, vec_ref[0:6, :]], axis=0), vec_ref[8:12, :], tab_ref, small_src)
            attn.wait_c(0)
            attn.wait_b()
            begin(small, small_src, small_acc, 2)

    def put(c, qkv, out):
        start = lax.div(c, 2 * gs.shape[3])
        some = pl.ds(start, qkv.shape[0] // (2 * gs.shape[3]))
        shape = (qkv.shape[0] // (2 * gs.shape[3]), *gs.shape[2:4])

        def store(*more):
            for lanes, value in ((slice(0, wide), qkv), (slice(wide, None), out)):
                value = value.reshape(*shape, value.shape[1])
                for ref in more:
                    value = value + ref[some, :, :, lanes].astype(F32)
                gs[t, some, :, :, lanes] = value.astype(BF16)

        @pl.when((t == 0) | (t == 2))
        def _():
            store()

        @pl.when(t == 1)
        def _():
            store(attn_rc.at[1])

        @pl.when(t == last)
        def _():
            store(attn_rc.at[0], attn_rb)

    attend_back_steps(
        hook, before_grads, put,
        x_ref, w_ref, gattn_ref, gfirst_ref, q_ref, k_ref, v_ref, mix_ref, lse_ref, gtok_ref, bias_ref,
        qh, gh, dq, kh, dqkv,
    )

    @pl.when(t == last)
    def _():
        settle(small_src, small_acc, 2)
        small.sum_c()
        attn.send_a()
        up.sum_z(up_out)
        small.send_b()
        small.sum_b()
        down.sum_z(down_out)
        small.send_a()
        small.sum_a()
        attn.sum_a()
        small.send_z()
        up.finish()
        down.finish()
        attn.send_z()
        small.sum_z(small_out)
        small.finish()
        attn.sum_z(attn_out)
        attn.finish()


def resident(shape):
    return pl.BlockSpec(shape, lambda *ids: (0,) * len(shape), pipeline_mode=pl.Buffered(1))


def result(shape):
    return pl.BlockSpec(shape, lambda *ids: (0,) * len(shape))


def per_step(shape):
    return pl.BlockSpec((1, *shape[1:]), lambda t: (t, 0, 0))


def struct(shape, dtype):
    return jax.ShapeDtypeStruct(shape, dtype)


def params(steps):
    return pltpu.CompilerParams(
        dimension_semantics=("arbitrary",) * steps, vmem_limit_bytes=VMEM_LIMIT
    )


def attend_outs(groups, rows, width):
    cols = width // groups
    wide = (groups, rows, WIDE)
    specs = [
        result((rows, width)),
        per_step(wide), per_step(wide), per_step(wide),
        per_step((groups, rows, cols)), per_step((groups, rows, 128)),
    ]
    shapes = [
        struct((rows, width), F32),
        struct(wide, BF16), struct(wide, BF16), struct(wide, BF16),
        struct((groups, rows, cols), BF16), struct((groups, rows, 128), F32),
    ]
    return specs, shapes


def run_attend(length, tokens, w_attn, bias, out_bias):
    rows, width = tokens.shape
    groups = w_attn.shape[0]
    specs, shapes = attend_outs(groups, rows, width)
    return pl.pallas_call(
        attend_kernel,
        grid=(groups,),
        in_specs=[
            pl.BlockSpec(memory_space=pltpu.SMEM),
            resident((rows, width)),
            per_step(w_attn.shape),
            resident(bias.shape),
            resident(out_bias.shape),
        ],
        out_specs=specs,
        out_shape=shapes,
        compiler_params=params(1),
        name="attend",
    )(length, tokens, w_attn, bias, out_bias)


def run_attend_spread(lengths, tokens, vec, w_attn, w_up, w_down):
    rows, width = tokens.shape
    groups = 4
    specs, shapes = attend_outs(groups, rows, width)
    whole = (2, 2, DEPTH, 2)
    slab = (groups, width, width)
    table = segment_tables()
    return pl.pallas_call(
        attend_spread_kernel,
        grid=(groups,),
        in_specs=[
            pl.BlockSpec(memory_space=pltpu.SMEM), resident(table.shape), resident((rows, width)),
            resident(vec.shape), resident(w_attn.shape), resident(w_up.shape), resident(w_down.shape),
        ],
        out_specs=specs + [
            per_step(slab), result((16, width)),
            pl.BlockSpec(memory_space=pl.ANY), pl.BlockSpec(memory_space=pl.ANY),
        ],
        out_shape=shapes + [
            struct(slab, BF16), struct((16, width), F32),
            struct((*whole, *w_up.shape), BF16), struct((*whole, *w_down.shape), BF16),
        ],
        scratch_shapes=[
            pltpu.VMEM((*whole, *vec.shape), F32), pltpu.VMEM((*whole, *w_attn.shape), BF16),
            pltpu.VMEM((groups, 8, 3 * width // groups), F32),
            pltpu.SemaphoreType.DMA((4, SLOTS)), pltpu.SemaphoreType.DMA((4, SLOTS)),
            pltpu.SemaphoreType.DMA((4,)),
        ],
        compiler_params=pltpu.CompilerParams(
            dimension_semantics=("arbitrary",), vmem_limit_bytes=VMEM_LIMIT, collective_id=0,
            has_side_effects=True,
        ),
        name="attend",
    )(lengths, table, tokens, vec, w_attn, w_up, w_down)


def run_ffn(length, residual, cotangent, vectors, w_up, w_down):
    rows, width = residual.shape
    groups = w_up.shape[0]
    units = w_up.shape[2]
    slab = pl.BlockSpec((1, width, units), lambda p, t: (t, 0, 0))
    grad = pl.BlockSpec((1, width, units), lambda p, t: (p * t, 0, 0))
    return pl.pallas_call(
        ffn_kernel,
        grid=(2, groups),
        in_specs=[
            pl.BlockSpec(memory_space=pltpu.SMEM),
            resident((rows, width)),
            resident((rows, width)),
            resident(vectors.shape),
            slab, slab,
        ],
        out_specs=[
            result((rows, width)), result((rows, width)), result((rows, width)), result((16, width)),
            grad, grad,
        ],
        out_shape=[
            struct((rows, width), F32), struct((rows, width), F32), struct((rows, width), BF16),
            struct((16, width), F32),
            struct(w_up.shape, BF16), struct(w_up.shape, BF16),
        ],
        scratch_shapes=[
            pltpu.VMEM((rows, width), F32), pltpu.VMEM((rows, width), BF16),
            pltpu.VMEM((rows, width), F32), pltpu.VMEM((rows, width), BF16),
            pltpu.VMEM((groups, rows, units), BF16), pltpu.VMEM((groups, rows, units), F32),
            pltpu.VMEM((rows, units), BF16),
        ],
        compiler_params=params(2),
        name="ffn",
    )(length, residual, cotangent, vectors, w_up, w_down)


def back_scratch(rows, width, cols):
    heads = cols // HEAD
    return [
        pltpu.VMEM((heads, rows, WIDE), BF16), pltpu.VMEM((heads, rows, WIDE), BF16),
        pltpu.VMEM((rows, WIDE), F32), pltpu.VMEM((heads, rows, WIDE), BF16),
        pltpu.VMEM((rows, 3 * cols), BF16),
    ]


def run_attend_back(tokens, w_attn, grad_attn, grad_first, q, k, v, mixed, lse):
    rows, width = tokens.shape
    groups = w_attn.shape[0]
    cols = width // groups
    return pl.pallas_call(
        attend_back_kernel,
        grid=(groups,),
        in_specs=[
            resident((rows, width)), per_step(w_attn.shape),
            resident((rows, width)), resident((rows, width)),
            per_step(q.shape), per_step(k.shape), per_step(v.shape),
            per_step(mixed.shape), per_step(lse.shape),
        ],
        out_specs=[result((rows, width)), per_step(w_attn.shape), per_step((groups, 8, cols))],
        out_shape=[
            struct((rows, width), F32), struct(w_attn.shape, BF16), struct((groups, 8, cols), F32),
        ],
        scratch_shapes=back_scratch(rows, width, cols),
        compiler_params=params(1),
        name="attend_back",
    )(tokens, w_attn, grad_attn, grad_first, q, k, v, mixed, lse)


def run_attend_back_collect(
    tokens, w_attn, grad_attn, grad_first, q, k, v, mixed, lse, small, grad_up, grad_down
):
    rows, width = tokens.shape
    groups = w_attn.shape[0]
    cols = width // groups
    table = segment_tables()

    def back(shape):
        return pl.BlockSpec((1, *shape[1:]), lambda t: (groups - 1 - t, 0, 0))

    def buffers(block, dtype, last):
        chip = (DEPTH, 2, *block)
        return [
            pltpu.VMEM((2, *chip), dtype),
            pltpu.VMEM(chip if last == "x" else (2, DEPTH, *block), dtype),
            pltpu.VMEM((DEPTH, *block), dtype), pltpu.VMEM((DEPTH - 1, *block), dtype),
        ]

    part = (width // (2 * DEPTH), width)
    pair = (2, DEPTH, 2)
    dots = (16, 128)
    return pl.pallas_call(
        attend_back_collect_kernel,
        grid=(groups,),
        in_specs=[
            resident(table.shape), resident((rows, width)), back(w_attn.shape),
            resident((rows, width)), resident((rows, width)),
            back(q.shape), back(k.shape), back(v.shape), back(mixed.shape), back(lse.shape),
            resident(small.shape),
            pl.BlockSpec(memory_space=pl.ANY), pl.BlockSpec(memory_space=pl.ANY),
        ],
        out_specs=[result((rows, width)), result(part), result(part), result(part), result(dots)],
        out_shape=[
            struct((rows, width), F32), struct(part, F32), struct(part, F32), struct(part, F32),
            struct(dots, F32),
        ],
        scratch_shapes=[
            *back_scratch(rows, width, cols),
            pltpu.VMEM((1, 8, cols), F32), pltpu.VMEM((groups, 8, cols), F32),
            pltpu.VMEM((groups, DEPTH, 2, *part), BF16), *buffers(part, BF16, "x"),
            pltpu.VMEM((*pair, *part), BF16), *buffers(part, BF16, "x"),
            pltpu.VMEM((*pair, *part), BF16), *buffers(part, BF16, "y"),
            pltpu.VMEM((2, *pair, *dots), F32), pltpu.VMEM((*pair, *dots), F32), *buffers(dots, F32, "x"),
            pltpu.SemaphoreType.DMA((4, 8)), pltpu.SemaphoreType.DMA((4, 8)),
            pltpu.SemaphoreType.DMA((3, 2)),
        ],
        compiler_params=pltpu.CompilerParams(
            dimension_semantics=("arbitrary",), vmem_limit_bytes=VMEM_LIMIT, collective_id=1,
            has_side_effects=True,
        ),
        name="attend_back",
    )(table, tokens, w_attn, grad_attn, grad_first, q, k, v, mixed, lse, small, grad_up, grad_down)


def shards(
    tokens, lengths, w_query, w_key, w_value, w_out, w_up, w_down,
    query_bias, value_bias, out_bias, attn_gain, attn_shift, up_bias, down_bias, ffn_gain, ffn_shift,
    cotangent,
):
    rows, width = tokens.shape
    groups = lax.axis_size("tensor")
    spans = lax.axis_size("dp")
    seq_count = lengths.shape[0]
    assert rows * groups == seq_count * rows and seq_count == groups
    rank = lax.axis_index("tensor")
    length = lax.dynamic_slice_in_dim(lengths, rank, 1)
    both = ("dp", "tensor")

    cols = width // groups
    units = w_up.shape[1]
    count = query_bias.shape[0]
    vectors = (query_bias, value_bias, out_bias, attn_gain, attn_shift, down_bias, ffn_gain, ffn_shift)
    flat = jnp.concatenate([*vectors, up_bias])
    own_attn = jnp.concatenate([w_query, w_key, w_value, w_out.T], axis=1)

    near = (spans, groups, width, units) == (8, 4, 768, 768)
    if near:
        vec = jnp.pad(flat[None], ((0, 7), (0, 384 - flat.shape[0])))
        residual, q, k, v, mixed, lse, w_attn, full, w_in, w_back = run_attend_spread(
            lengths, tokens, vec, own_attn, w_up, w_down.T
        )
        w_in, w_back = w_in.reshape(groups, width, units), w_back.reshape(groups, width, units)
    else:
        pack = jnp.concatenate([own_attn, w_up, w_down.T], axis=1)
        whole = lax.all_gather(pack, both, axis=0, tiled=True)
        whole = whole.reshape(spans, groups, *pack.shape).swapaxes(0, 1)
        whole = whole.reshape(groups, width, pack.shape[1])
        w_attn, w_in, w_back = jnp.split(whole, [4 * cols, 4 * cols + units], axis=2)
        gathered = lax.all_gather(flat, both, axis=0, tiled=True).reshape(spans * groups, -1)
        full = gathered[:, : 8 * count].reshape(-1, 8, count).swapaxes(0, 1).reshape(8, width)
        full = jnp.concatenate([full, gathered[:, 8 * count :].reshape(groups, units)])
        full = jnp.pad(full, ((0, 16 - full.shape[0]), (0, 0)))
        qb, vb = full[0].reshape(groups, 1, cols), full[1].reshape(groups, 1, cols)
        bias = jnp.pad(jnp.concatenate([qb, jnp.zeros_like(qb), vb], axis=2), ((0, 0), (0, 7), (0, 0)))
        residual, q, k, v, mixed, lse = run_attend(length, tokens, w_attn, bias, full[2:3])
    output, grad_first, grad_attn, small, grad_in, grad_back = run_ffn(
        length, residual, cotangent, full, w_in, w_back
    )
    if near:
        split = (2, 2, DEPTH, 2, width // (2 * DEPTH), units)
        grad_tokens, own_a, own_u, own_d, dots = run_attend_back_collect(
            tokens, w_attn, grad_attn, grad_first, q, k, v, mixed, lse, small,
            grad_in.reshape(split), grad_back.reshape(split),
        )
        tiny8 = dots[:8, :count]
        return (
            output, grad_tokens,
            own_a[:, :cols], own_a[:, cols : 2 * cols], own_a[:, 2 * cols : 3 * cols], own_a[:, 3 * cols :].T,
            own_u, own_d.T,
            tiny8[0], tiny8[1], tiny8[2], tiny8[3], tiny8[4], dots[8, : up_bias.shape[0]],
            tiny8[5], tiny8[6], tiny8[7],
        )
    grad_tokens, grad_attn_w, bias_grad = run_attend_back(
        tokens, w_attn, grad_attn, grad_first, q, k, v, mixed, lse
    )

    every = jnp.concatenate([grad_attn_w, grad_in, grad_back], axis=2)
    every = every.reshape(groups, spans, width // spans, -1).swapaxes(0, 1)
    every = every.reshape(spans * groups * (width // spans), -1)
    owned = lax.psum_scatter(every, both, scatter_dimension=0, tiled=True).astype(F32)

    rows8 = jnp.concatenate(
        [bias_grad[:, 0].reshape(1, width), bias_grad[:, 1].reshape(1, width), small[:6]]
    )
    parts = jnp.concatenate(
        [
            rows8.reshape(8, spans * groups, count).swapaxes(0, 1).reshape(spans * groups, 8 * count),
            small[8 : 8 + groups].reshape(spans * groups, -1),
        ],
        axis=1,
    )
    tiny = lax.psum_scatter(parts.reshape(-1), both, scatter_dimension=0, tiled=True)
    tiny8 = tiny[: 8 * count].reshape(8, count)
    return (
        output, grad_tokens,
        owned[:, :cols], owned[:, cols : 2 * cols], owned[:, 2 * cols : 3 * cols],
        owned[:, 3 * cols : 4 * cols].T,
        owned[:, 4 * cols : 4 * cols + units], owned[:, 4 * cols + units :].T,
        tiny8[0], tiny8[1], tiny8[2], tiny8[3], tiny8[4], tiny[8 * count :], tiny8[5], tiny8[6], tiny8[7],
    )


def solution(mesh):
    rows, vector, matrix, flipped = (
        P(("dp", "tensor"), None), P(("dp", "tensor")), P("dp", "tensor"), P("tensor", "dp"),
    )
    return jax.shard_map(
        shards,
        mesh=mesh,
        in_specs=(rows, P("dp"), matrix, matrix, matrix, flipped, matrix, flipped, *(vector,) * 9, rows),
        out_specs=(rows, rows, matrix, matrix, matrix, flipped, matrix, flipped, *(vector,) * 9),
        check_vma=False,
    )
```

```python
import functools

import jax
import jax.numpy as jnp
from jax import lax
from jax.experimental import pallas as pl
from jax.experimental.pallas import tpu as pltpu
from jax.sharding import PartitionSpec as P

HEAD = 64
EPSILON = 1e-12
FLOOR_SCORE = -1e30
BLOCK = 256
WIDE = 256
BF16 = jnp.bfloat16
F32 = jnp.float32
VMEM_LIMIT = 60 * 1024 * 1024


def dot_nn(a, b):
    return lax.dot_general(a, b, (((1,), (0,)), ((), ())), preferred_element_type=F32)


def dot_nt(a, b):
    return lax.dot_general(a, b, (((1,), (1,)), ((), ())), preferred_element_type=F32)


def dot_tn(a, b):
    return lax.dot_general(a, b, (((0,), (0,)), ((), ())), preferred_element_type=F32)


def lane_iota(rows, lanes):
    return lax.broadcasted_iota(jnp.int32, (rows, lanes), 1)


def row_iota(rows, lanes):
    return lax.broadcasted_iota(jnp.int32, (rows, lanes), 0)


def head_mask(rows, h, extra):
    lane = lane_iota(rows, WIDE)
    keep = (lane >= h * HEAD) & (lane < (h + 1) * HEAD)
    if extra is not None:
        keep = keep | (lane >= extra)
    return keep


def normalize(v):
    center = v - jnp.mean(v, axis=-1, keepdims=True)
    inv = lax.rsqrt(jnp.mean(center * center, axis=-1, keepdims=True) + EPSILON)
    return center * inv, inv


def norm_back(g, n, inv):
    return inv * (
        g - jnp.mean(g, axis=-1, keepdims=True) - n * jnp.mean(g * n, axis=-1, keepdims=True)
    )


def split_three(v):
    hi = v.astype(BF16)
    rest = v - hi.astype(F32)
    mid = rest.astype(BF16)
    low = (rest - mid.astype(F32)).astype(BF16)
    return hi.astype(F32), mid.astype(F32), low.astype(F32)


MESH = pl.DeviceIdType.MESH
DEPTH = 4
SLOTS = 14


def around(z, k):
    return (z, z + 1 - 2 * lax.rem(z, 2), DEPTH - 1 - z, lax.rem(z + 2, DEPTH))[k]


class Place:
    def __init__(self):
        dp, t = lax.axis_index("dp"), lax.axis_index("tensor")
        self.z, self.x = lax.div(dp, 2), lax.rem(dp, 2)
        self.y, self.c = lax.div(t, 2), lax.rem(t, 2)

    def device(self, z=None, x=None, y=None, c=None):
        z, x = self.z if z is None else z, self.x if x is None else x
        y, c = self.y if y is None else y, self.c if c is None else c
        return (z * 2 + x, y * 2 + c)

    def neighbours(self):
        return [self.device(z=around(self.z, k)) for k in range(1, DEPTH)] + [
            self.device(x=1 - self.x), self.device(y=1 - self.y), self.device(c=1 - self.c),
        ]

    def greet(self):
        barrier = pltpu.get_barrier_semaphore()
        peers = self.neighbours()
        for peer in peers:
            pl.semaphore_signal(barrier, inc=1, device_id=peer, device_id_type=MESH)
        pl.semaphore_wait(barrier, len(peers))

    def group(self, step):
        y = lax.rem(self.y + lax.div(step, 2), 2)
        c = lax.rem(self.c + lax.rem(step, 2), 2)
        return y * 2 + c


def remote(src, dst, send, recv, device):
    return pltpu.make_async_remote_copy(
        src_ref=src, dst_ref=dst, send_sem=send, recv_sem=recv, device_id=device, device_id_type=MESH
    )


class Moves:
    def __init__(self, place, send, recv):
        self.p, self.send, self.recv = place, send, recv
        self.to_x, self.to_y = place.device(x=1 - place.x), place.device(y=1 - place.y)
        self.to_c = place.device(c=1 - place.c)

    def to_z(self, k):
        return self.p.device(z=around(self.p.z, k))

    def copy(self, src, dst, slot, device):
        return remote(src, dst, self.send.at[slot], self.recv.at[slot], device)

    def arrive(self, ref, slot, device):
        self.copy(ref, ref, slot, device).wait_recv()

    def gone(self, ref, slot, device):
        self.copy(ref, ref, slot, device).wait_send()


class Spread(Moves):
    def __init__(self, place, own, buf, send, recv, home, first, rows=slice(None)):
        super().__init__(place, send, recv)
        self.own, self.buf, self.home, self.first, self.rows = own.at[rows], buf, home, first, rows
        self.to_a, self.to_b = (self.to_x, self.to_y) if first == "x" else (self.to_y, self.to_x)

    def at(self, z, a=0, b=0):
        p = self.p
        dx, dy = (a, b) if self.first == "x" else (b, a)
        return self.buf.at[p.y if dy == 0 else 1 - p.y, p.c, z, p.x if dx == 0 else 1 - p.x, self.rows]

    def chip(self, dy, c=0):
        p = self.p
        y = p.y if dy == 0 else 1 - p.y
        return self.buf.at[y, p.c if c == 0 else 1 - p.c, :, :, self.rows]

    def local(self):
        return pltpu.make_async_copy(self.own, self.at(self.p.z), self.home)

    def begin_z(self):
        for k in range(1, DEPTH):
            self.copy(self.own, self.at(self.p.z), k - 1, self.to_z(k)).start()

    def begin_ab(self):
        self.local().start()
        self.copy(self.own, self.at(self.p.z), 3, self.to_a).start()
        self.copy(self.own, self.at(self.p.z), 7, self.to_b).start()

    def after_z(self):
        for k in range(1, DEPTH):
            ref = self.at(around(self.p.z, k))
            self.arrive(ref, k - 1, self.to_z(k))
            self.copy(ref, ref, 3 + k, self.to_a).start()
            self.copy(ref, ref, 7 + k, self.to_b).start()
        self.local().wait()

    def after_a(self):
        for k in range(DEPTH):
            self.arrive(self.at(around(self.p.z, k), a=1), 3 + k, self.to_a)
        ref = self.at(slice(None), a=1)
        self.copy(ref, ref, 11, self.to_b).start()
        if self.first == "x":
            self.swap(0)

    def swap(self, dy):
        ref = self.chip(dy)
        self.copy(ref, ref, 12 + dy, self.to_c).start()

    def after_b(self):
        for k in range(DEPTH):
            self.arrive(self.at(around(self.p.z, k), b=1), 7 + k, self.to_b)
        if self.first == "y":
            self.swap(0)
        self.arrive(self.at(slice(None), a=1, b=1), 11, self.to_b)
        self.swap(1)

    def after_c(self, dy):
        self.arrive(self.chip(dy, c=1), 12 + dy, self.to_c)

    def finish(self):
        one, column, chip = self.at(self.p.z), self.at(slice(None)), self.chip(0)
        for k in range(1, DEPTH):
            self.gone(one, k - 1, self.to_z(k))
        for k in range(DEPTH):
            self.gone(one, 3 + k, self.to_a)
            self.gone(one, 7 + k, self.to_b)
        self.gone(column, 11, self.to_b)
        for dy in range(2):
            self.gone(chip, 12 + dy, self.to_c)


class SpreadFlat(Moves):
    def __init__(self, place, own, buf, send, recv, home, rows=slice(None)):
        super().__init__(place, send, recv)
        self.own, self.buf, self.home, self.rows = own.at[rows], buf, home, rows

    def at(self, y=slice(None), z=slice(None), x=slice(None), c=0):
        return self.buf.at[y, self.p.c if c == 0 else 1 - self.p.c, z, x, self.rows]

    def local(self):
        p = self.p
        return pltpu.make_async_copy(self.own, self.at(p.y, p.z, p.x), self.home)

    def begin(self):
        p = self.p
        self.local().start()
        self.copy(self.own, self.at(p.y, p.z, p.x), 0, self.to_y).start()

    def after_y(self):
        p = self.p
        self.local().wait()
        self.arrive(self.at(1 - p.y, p.z, p.x), 0, self.to_y)
        ref = self.at(z=p.z, x=p.x)
        self.copy(ref, ref, 1, self.to_x).start()

    def after_x(self):
        p = self.p
        self.arrive(self.at(z=p.z, x=1 - p.x), 1, self.to_x)
        ref = self.at(z=p.z)
        for k in range(1, DEPTH):
            self.copy(ref, ref, 1 + k, self.to_z(k)).start()

    def after_z(self):
        for k in range(1, DEPTH):
            self.arrive(self.at(z=around(self.p.z, k)), 1 + k, self.to_z(k))
        ref = self.at()
        self.copy(ref, ref, 5, self.to_c).start()

    def after_c(self):
        self.arrive(self.at(c=1), 5, self.to_c)

    def finish(self):
        p = self.p
        self.gone(self.at(p.y, p.z, p.x), 0, self.to_y)
        self.gone(self.at(z=p.z, x=p.x), 1, self.to_x)
        for k in range(1, DEPTH):
            self.gone(self.at(z=p.z), 1 + k, self.to_z(k))
        self.gone(self.at(), 5, self.to_c)


class Collect:
    def __init__(self, place, near, far, rc, rb, ra, rz, send, recv, last):
        self.p, self.near, self.far, self.last = place, near, far, last
        self.rc, self.rb, self.ra, self.rz, self.send, self.recv = rc, rb, ra, rz, send, recv
        to_x, to_y = place.device(x=1 - place.x), place.device(y=1 - place.y)
        self.to_a, self.to_b = (to_x, to_y) if last == "x" else (to_y, to_x)
        self.to_c = place.device(c=1 - place.c)

    def copy(self, src, dst, slot, device):
        return pltpu.make_async_remote_copy(
            src_ref=src, dst_ref=dst, send_sem=self.send.at[slot], recv_sem=self.recv.at[slot],
            device_id=device, device_id_type=MESH,
        )

    def copy_c(self, src, dy):
        return self.copy(src, self.rc.at[dy], dy, self.to_c)

    def copies_b(self):
        if self.last == "x":
            return [self.copy(self.far, self.rb, 2, self.to_b)]
        there = (slice(None), 1 - self.p.x)
        return [
            self.copy(part.at[there], self.rb.at[dy], 2 + 5 * dy, self.to_b)
            for dy, part in enumerate((self.near, self.far))
        ]

    def copy_a(self):
        if self.last == "x":
            return self.copy(self.near.at[:, 1 - self.p.x], self.ra, 3, self.to_a)
        return self.copy(self.far.at[:, self.p.x], self.ra, 3, self.to_a)

    def copies_z(self):
        p = self.p
        return [
            self.copy(
                self.near.at[around(p.z, k), p.x], self.rz.at[k - 1], 3 + k, p.device(z=around(p.z, k))
            )
            for k in range(1, DEPTH)
        ]

    def wait_c(self, dy):
        self.copy_c(self.rc.at[dy], dy).wait_recv()

    def wait_b(self):
        for copy in self.copies_b():
            copy.wait_recv()

    def sum_c(self):
        for dy, part in enumerate((self.near, self.far)):
            self.wait_c(dy)

            @pl.loop(0, DEPTH)
            def _(z):
                part[z] = add(part[z], self.rc[dy, z]).astype(part.dtype)

    def send_b(self):
        for copy in self.copies_b():
            copy.start()

    def sum_b(self):
        self.wait_b()
        x = self.p.x

        @pl.loop(0, DEPTH)
        def _(z):
            if self.last == "x":
                self.near[z] = add(self.near[z], self.rb[z]).astype(self.near.dtype)
            else:
                for dy, part in enumerate((self.near, self.far)):
                    part[z, x] = add(part[z, x], self.rb[dy, z]).astype(part.dtype)

    def send_a(self):
        self.copy_a().start()

    def sum_a(self):
        self.copy_a().wait_recv()
        x = self.p.x

        @pl.loop(0, DEPTH)
        def _(z):
            self.near[z, x] = add(self.near[z, x], self.ra[z]).astype(self.near.dtype)

    def send_z(self):
        for copy in self.copies_z():
            copy.start()

    def sum_z(self, out_ref):
        for copy in self.copies_z():
            copy.wait_recv()
        total = self.near[self.p.z, self.p.x].astype(F32)
        for k in range(DEPTH - 1):
            total = total + self.rz[k].astype(F32)
        out_ref[...] = total

    def finish(self):
        for dy in range(2):
            self.copy_c(self.rc.at[dy], dy).wait_send()
        for copy in [*self.copies_b(), self.copy_a(), *self.copies_z()]:
            copy.wait_send()


class CollectFlat(Moves):
    def __init__(self, place, acc, rc, rz, rx, ry, send, recv):
        super().__init__(place, send, recv)
        self.acc, self.rc, self.rz, self.rx, self.ry = acc, rc, rz, rx, ry

    def copy_c(self, src, dy):
        return self.copy(src, self.rc.at[dy], dy, self.to_c)

    def copies_z(self):
        return [
            self.copy(self.acc.at[:, around(self.p.z, k)], self.rz.at[k - 1], 1 + k, self.to_z(k))
            for k in range(1, DEPTH)
        ]

    def copy_x(self):
        return self.copy(self.acc.at[:, self.p.z, 1 - self.p.x], self.rx, 5, self.to_x)

    def copy_y(self):
        return self.copy(self.acc.at[1, self.p.z, self.p.x], self.ry, 6, self.to_y)

    def sum_c(self):
        for dy in range(2):
            self.copy_c(self.rc.at[dy], dy).wait_recv()

            @pl.loop(0, DEPTH)
            def _(z):
                self.acc[dy, z] = add(self.acc[dy, z], self.rc[dy, z]).astype(BF16)

    def send_z(self):
        for copy in self.copies_z():
            copy.start()

    def sum_z(self):
        for copy in self.copies_z():
            copy.wait_recv()
        z = self.p.z
        for dy in range(2):
            total = add(self.acc[dy, z], self.rz[0, dy])
            total = total + add(self.rz[1, dy], self.rz[2, dy])
            self.acc[dy, z] = total.astype(BF16)

    def send_x(self):
        self.copy_x().start()

    def sum_x(self):
        self.copy_x().wait_recv()
        z, x = self.p.z, self.p.x
        for dy in range(2):
            self.acc[dy, z, x] = add(self.acc[dy, z, x], self.rx[dy]).astype(BF16)

    def send_y(self):
        self.copy_y().start()

    def sum_y(self, out_ref):
        self.copy_y().wait_recv()
        out_ref[...] = add(self.acc[0, self.p.z, self.p.x], self.ry[...])

    def finish(self):
        for dy in range(2):
            self.copy_c(self.rc.at[dy], dy).wait_send()
        for copy in [*self.copies_z(), self.copy_x(), self.copy_y()]:
            copy.wait_send()


class Tail(Moves):
    def __init__(self, place, near, rx, rz, sz, sx, send, recv):
        super().__init__(place, send, recv)
        self.near, self.rx, self.rz, self.sz, self.sx = near, rx, rz, sz, sx
        cut = rx.shape[1]
        self.most, self.others = slice(0, cut), slice(cut, cut + sx.shape[0])

    def first(self):
        p = self.p
        copies = [self.copy(self.near.at[:, 1 - p.x, self.most], self.rx, 0, self.to_x)]
        return copies + [
            self.copy(self.near.at[around(p.z, k), :, self.others], self.sz.at[k - 1], k, self.to_z(k))
            for k in range(1, DEPTH)
        ]

    def second(self):
        p = self.p
        copies = [
            self.copy(self.near.at[around(p.z, k), p.x, self.most], self.rz.at[k - 1], 3 + k, self.to_z(k))
            for k in range(1, DEPTH)
        ]
        return copies + [self.copy(self.near.at[p.z, 1 - p.x, self.others], self.sx, 7, self.to_x)]

    def sum_first(self):
        for copy in self.first():
            copy.wait_recv()
        p = self.p

        @pl.loop(0, DEPTH)
        def _(z):
            self.near[z, p.x, self.most] = add(self.near[z, p.x, self.most], self.rx[z]).astype(BF16)

        total = add(self.near[p.z, :, self.others], self.sz[0])
        total = total + add(self.sz[1], self.sz[2])
        self.near[p.z, :, self.others] = total.astype(BF16)

    def sum_second(self, out_ref):
        for copy in self.second():
            copy.wait_recv()
        p = self.p
        total = add(self.near[p.z, p.x, self.most], self.rz[0])
        out_ref[self.most, :] = total + add(self.rz[1], self.rz[2])
        out_ref[self.others, :] = add(self.near[p.z, p.x, self.others], self.sx[...])

    def finish(self):
        for copy in [*self.first(), *self.second()]:
            copy.wait_send()


def add(a, b):
    return a.astype(F32) + b.astype(F32)


def segment_tables():
    lane = jnp.arange(768, dtype=jnp.int32)
    rows = jnp.stack([lane % 24, lane // 24, lane % 96, lane // 96])
    return jnp.concatenate([rows, jnp.zeros_like(rows)])


def one_hot(tab_ref, row, start, rows):
    return (row_iota(rows, tab_ref.shape[1]) == start + tab_ref[row : row + 1, :]).astype(BF16)


def owners(shape, dim):
    p = lax.broadcasted_iota(jnp.int32, shape, dim)
    return lax.shift_left(p & 7, 2) + lax.shift_right_logical(p, 3)


def join_vectors(block_ref, tab_ref, vec_ref):
    blocks = block_ref[...].reshape(32, 16, 128)
    width = vec_ref.shape[1]

    def place(values, table):
        hot = one_hot(tab_ref, table, 0, 128)
        hi, mid, low = (dot_nn(part.astype(BF16), hot) for part in split_three(values))
        return hi + mid + low

    keep = owners((32, 16, width), 0) == tab_ref[1:2, :][None]
    got = place(blocks.reshape(512, 128), 0).reshape(32, 16, width)
    vec_ref[...] = jnp.sum(jnp.where(keep, got, 0.0), axis=0)
    row = lax.broadcasted_iota(jnp.int32, (32, 16, 128), 1)
    got = place(jnp.sum(jnp.where(row == 8, blocks, 0.0), axis=1), 2)
    for k in range(4):
        keep = owners((32, width), 0) == tab_ref[3:4, :] + 8 * k
        vec_ref[8 + k : 9 + k, :] = jnp.sum(jnp.where(keep, got, 0.0), axis=0, keepdims=True)


def cut_vectors(eight, up_rows, tab_ref, out_ref):
    width = tab_ref.shape[1]

    def pick(values, table):
        hot = one_hot(tab_ref, table, 0, 128)
        return sum(dot_nt(part.astype(BF16), hot) for part in split_three(values))

    both = jnp.concatenate([eight, jnp.zeros_like(eight)], axis=0)
    keep = owners((32, 16, width), 0) == tab_ref[1:2, :][None]
    spread = jnp.where(keep, jnp.broadcast_to(both[None], (32, 16, width)), 0.0)
    blocks = pick(spread.reshape(512, width), 0).reshape(32, 16, 128)
    owner = owners((32, width), 0)
    ups = jnp.zeros((32, width), F32)
    for k in range(4):
        ups = jnp.where(owner == tab_ref[3:4, :] + 8 * k, up_rows[k : k + 1, :], ups)
    ups = jnp.broadcast_to(pick(ups, 2)[:, None, :], (32, 16, 128))
    blocks = jnp.where(lax.broadcasted_iota(jnp.int32, (32, 16, 128), 1) == 8, ups, blocks)
    out_ref[...] = blocks.reshape(out_ref.shape)


def attend_steps(
    length, hook, x_ref, w_ref, bias_ref, g, out_bias, res_ref, q_ref, k_ref, v_ref, mix_ref, lse_ref, first
):
    rows, width = x_ref.shape
    cols = mix_ref.shape[2]
    heads = cols // HEAD

    @pl.when(first)
    def _():
        @pl.loop(0, rows, step=BLOCK)
        def _(r):
            r = pl.multiple_of(r, BLOCK)
            res_ref[pl.ds(r, BLOCK), :] = x_ref[pl.ds(r, BLOCK), :].astype(F32) + out_bias[...]

    @pl.loop(0, rows, step=BLOCK)
    def _(r):
        r = pl.multiple_of(r, BLOCK)
        here = pl.ds(r, BLOCK)
        out = dot_nn(x_ref[here, :], w_ref[0, :, : 3 * cols]) + bias_ref[g, 0:1, :]
        one = jnp.ones((BLOCK, WIDE - cols), F32)
        tail = lane_iota(BLOCK, WIDE - cols)
        position = r + row_iota(BLOCK, WIDE - cols)
        q_ref[0, here, :cols] = (out[:, :cols].astype(BF16).astype(F32) * HEAD**-0.5).astype(BF16)
        q_ref[0, here, cols:] = jnp.where(tail == 3, one, 0.0).astype(BF16)
        k_ref[0, here, :cols] = out[:, cols : 2 * cols].astype(BF16)
        bias = jnp.where(position < length, 0.0, FLOOR_SCORE)
        k_ref[0, here, cols:] = jnp.where(
            tail < 3, one, jnp.where(tail == 3, bias, 0.0)
        ).astype(BF16)
        v_ref[0, here, :cols] = out[:, 2 * cols : 3 * cols].astype(BF16)
        v_ref[0, here, cols:] = one.astype(BF16)

    @pl.loop(0, rows, step=BLOCK)
    def _(r):
        r = pl.multiple_of(r, BLOCK)
        hook(r)
        here = pl.ds(r, BLOCK)
        query = q_ref[0, here, :]
        scores = [
            dot_nt(jnp.where(head_mask(BLOCK, h, cols), query, 0), k_ref[0]) for h in range(heads)
        ]
        mixed = jnp.zeros((BLOCK, WIDE), F32)
        total = jnp.zeros((BLOCK, 128), F32)
        for h in range(heads):
            top = jnp.max(scores[h], axis=-1, keepdims=True)
            terms = jnp.exp(scores[h] - top).astype(BF16)
            got = dot_nn(terms, v_ref[0])
            denom = got[:, cols : cols + 1]
            mixed = jnp.where(head_mask(BLOCK, h, None), got * (1.0 / denom), mixed)
            total = jnp.where(lane_iota(BLOCK, 128) == h, -(top + jnp.log(denom)), total)
        low = mixed[:, :cols].astype(BF16)
        mix_ref[0, here, :] = low
        lse_ref[0, here, :] = total
        res_ref[here, :] += dot_nt(low, w_ref[0, :, 3 * cols :])


def attend_kernel(len_ref, x_ref, w_ref, bias_ref, ob_ref, *outs):
    t = pl.program_id(0)
    attend_steps(len_ref[0], lambda r: None, x_ref, w_ref, bias_ref, t, ob_ref, *outs, t == 0)


def attend_spread_kernel(
    len_ref, tab_ref, x_ref, own_vec, own_attn, own_up, own_down,
    res_ref, q_ref, k_ref, v_ref, mix_ref, lse_ref, w_ref, vec_ref, up_ref, down_ref,
    vec_buf, attn_buf, bias_buf, send, recv, home,
):
    t = pl.program_id(0)
    place = Place()
    cols = mix_ref.shape[2]

    def spread(n, own, buf, first, rows=slice(None)):
        return Spread(place, own, buf, send.at[n], recv.at[n], home.at[n], first, rows)

    def flat(n, own, buf, rows=slice(None)):
        return SpreadFlat(place, own, buf, send.at[n], recv.at[n], home.at[n], rows)

    cut = own_down.shape[0] * 2 // 3
    small = flat(0, own_vec, vec_buf)
    attn = spread(1, own_attn, attn_buf, "x")
    up = spread(2, own_up, up_ref, "y")
    down = spread(3, own_down, down_ref, "x", slice(0, cut))
    rest = flat(4, own_down, down_ref, slice(cut, None))

    @pl.when(t == 0)
    def _():
        place.greet()
        small.begin()
        attn.begin_z()
        small.after_y()
        small.after_x()
        attn.begin_ab()
        rest.begin()
        down.begin_ab()
        up.begin_ab()
        attn.after_z()
        up.begin_z()
        down.begin_z()
        rest.after_y()
        small.after_z()
        small.after_c()
        join_vectors(vec_buf, tab_ref, vec_ref)
        for g in range(bias_buf.shape[0]):
            there = slice(g * cols, (g + 1) * cols)
            bias_buf[g, 0:1, :] = jnp.concatenate(
                [vec_ref[0:1, there], jnp.zeros((1, cols), F32), vec_ref[1:2, there]], axis=1
            )
        attn.after_a()

    @pl.when(t == 1)
    def _():
        attn.after_c(0)

    @pl.when(t == 3)
    def _():
        attn.after_c(1)

    def hook(r):
        def at(step, block, *events):
            @pl.when((t == step) & (r == block * BLOCK))
            def _():
                for event in events:
                    event()

        at(0, 0, rest.after_x)
        at(0, 1, up.after_z)
        at(1, 1, down.after_z)
        at(1, 2, attn.after_b)
        at(2, 0, down.after_a)
        at(2, 1, up.after_a)
        at(3, 1, rest.after_z)

    g = place.group(t)
    y, c = lax.div(g, 2), lax.rem(g, 2)
    for z in range(DEPTH):
        for x in range(2):
            n = attn_buf.shape[4]
            start = (z * 2 + x) * n
            w_ref[0, start : start + n, :] = attn_buf[y, c, z, x]
    attend_steps(
        len_ref[lax.axis_index("tensor")], hook, x_ref, w_ref, bias_buf, g, vec_ref.at[2:3],
        res_ref, q_ref, k_ref, v_ref, mix_ref, lse_ref, t == 0,
    )

    @pl.when(t == pl.num_programs(0) - 1)
    def _():
        down.after_b()
        up.after_b()
        rest.after_c()
        for piece in (down, up):
            piece.after_c(0)
            piece.after_c(1)
        for piece in (small, attn, up, down, rest):
            piece.finish()


def ffn_kernel(
    len_ref, res_ref, cot_ref, vec_ref, wu_ref, wd_ref,
    out_ref, gfirst_ref, gattn_ref, small_ref, gup_ref, gdn_ref,
    hid, hlow, acc, gb, act, dact, gpre,
):
    phase, t = pl.program_id(0), pl.program_id(1)
    last = pl.num_programs(1) - 1
    rows, width = res_ref.shape
    length = len_ref[0]
    gain_one, shift_one, down_bias = vec_ref[3:4, :], vec_ref[4:5, :], vec_ref[5:6, :]
    gain_two, shift_two = vec_ref[6:7, :], vec_ref[7:8, :]

    def blocks(body):
        @pl.loop(0, rows, step=BLOCK)
        def _(r):
            r = pl.multiple_of(r, BLOCK)
            body(r, pl.ds(r, BLOCK))

    def put(row, value):
        small_ref[row : row + 1, :] += jnp.sum(value, axis=0, keepdims=True)

    @pl.when((phase == 0) & (t == 0))
    def _():
        small_ref[...] = jnp.zeros_like(small_ref)

        def first(r, here):
            n, _ = normalize(res_ref[here, :])
            hidden = n * gain_one + shift_one
            hid[here, :] = hidden
            hlow[here, :] = hidden.astype(BF16)
            acc[here, :] = hidden + down_bias

        blocks(first)

    @pl.when(phase == 0)
    def _():
        def forward(r, here):
            pre = dot_nn(hlow[here, :], wu_ref[0]) + vec_ref[pl.ds(8 + t, 1), :]
            phi = 0.5 * (1.0 + lax.erf(pre * (0.5**0.5)))
            low = (pre * phi).astype(BF16)
            act[t, here, :] = low
            dact[t, here, :] = phi + pre * (jnp.exp(-0.5 * pre * pre) * 0.3989422804014327)
            acc[here, :] += dot_nt(low, wd_ref[0])

        blocks(forward)

    @pl.when((phase == 0) & (t == last))
    def _():
        def turn(r, here):
            n, inv = normalize(acc[here, :])
            valid = ((r + row_iota(BLOCK, 1)) < length).astype(F32)
            out_ref[here, :] = (n * gain_two + shift_two) * valid
            cot = cot_ref[here, :].astype(F32) * valid
            put(4, cot * n)
            put(5, cot)
            grad = norm_back(cot * gain_two, n, inv)
            acc[here, :] = grad
            low = grad.astype(BF16)
            gb[here, :] = low
            put(3, low.astype(F32))

        blocks(turn)

    @pl.when(phase == 1)
    def _():
        def backward(r, here):
            grad_act = dot_nn(gb[here, :], wd_ref[0]).astype(BF16).astype(F32)
            low = (grad_act * dact[t, here, :]).astype(BF16)
            gpre[here, :] = low
            part = dot_nt(low, wu_ref[0])

            @pl.when(t == 0)
            def _():
                hid[here, :] = part

            @pl.when(t > 0)
            def _():
                hid[here, :] += part

            small_ref[pl.ds(8 + t, 1), :] += jnp.sum(low.astype(F32), axis=0, keepdims=True)

        blocks(backward)

        @pl.loop(0, width, step=BLOCK)
        def _(c):
            c = pl.multiple_of(c, BLOCK)
            here = pl.ds(c, BLOCK)
            gdn_ref[0, here, :] = dot_tn(gb[:, here], act[t]).astype(BF16)
            gup_ref[0, here, :] = dot_tn(hlow[:, here], gpre[...]).astype(BF16)

    @pl.when((phase == 1) & (t == last))
    def _():
        def finish(r, here):
            grad_hidden = acc[here, :] + hid[here, :].astype(BF16).astype(F32)
            n, inv = normalize(res_ref[here, :])
            put(1, grad_hidden * n)
            put(2, grad_hidden)
            grad = norm_back(grad_hidden * gain_one, n, inv)
            gfirst_ref[here, :] = grad
            low = grad.astype(BF16)
            gattn_ref[here, :] = low
            put(0, low.astype(F32))

        blocks(finish)


def attend_back_steps(
    hook, before_grads, put_grads,
    x_ref, w_ref, gattn_ref, gfirst_ref, q_ref, k_ref, v_ref, mix_ref, lse_ref, gtok_ref, bias_ref,
    qh, gh, dq, kh, dqkv,
):
    t = pl.program_id(0)
    rows, width = x_ref.shape
    cols = mix_ref.shape[2]
    heads = cols // HEAD

    @pl.when(t == 0)
    def _():
        gtok_ref[...] = gfirst_ref[...]

    bias_ref[...] = jnp.zeros_like(bias_ref)

    @pl.loop(0, rows, step=BLOCK)
    def _(r):
        r = pl.multiple_of(r, BLOCK)
        here = pl.ds(r, BLOCK)
        grad_mixed = dot_nn(gattn_ref[here, :], w_ref[0, :, 3 * cols :]).astype(BF16)
        product = grad_mixed.astype(F32) * mix_ref[0, here, :].astype(F32)
        lane = lane_iota(BLOCK, WIDE)
        wide = jnp.concatenate(
            [grad_mixed.astype(F32), jnp.zeros((BLOCK, WIDE - cols), F32)], axis=1
        )
        query = q_ref[0, here, :].astype(F32)
        key = k_ref[0, here, :]
        for h in range(heads):
            inside = (lane_iota(BLOCK, cols) >= h * HEAD) & (lane_iota(BLOCK, cols) < (h + 1) * HEAD)
            delta = jnp.sum(jnp.where(inside, product, 0.0), axis=-1, keepdims=True)
            hi, mid, low = split_three(-delta)
            keep = head_mask(BLOCK, h, None)
            tail = jnp.where(lane == cols, hi, jnp.where(lane == cols + 1, mid, jnp.where(lane == cols + 2, low, 0.0)))
            gh[h, here, :] = jnp.where(keep, wide, tail).astype(BF16)
            hi, mid, low = split_three(lse_ref[0, here, h : h + 1])
            tail = jnp.where(lane == cols, hi, jnp.where(lane == cols + 1, mid, jnp.where(lane == cols + 2, low, 0.0)))
            tail = jnp.where(lane == cols + 3, 1.0, tail)
            qh[h, here, :] = jnp.where(keep, query, tail).astype(BF16)
            kh[h, here, :] = jnp.where(keep, key, 0)

    @pl.loop(0, rows, step=BLOCK)
    def _(r):
        r = pl.multiple_of(r, BLOCK)
        hook(r)
        here = pl.ds(r, BLOCK)
        key, value = k_ref[0, here, :], v_ref[0, here, :]
        grad_key = jnp.zeros((BLOCK, WIDE), F32)
        grad_value = jnp.zeros((BLOCK, WIDE), F32)
        logits = [dot_nt(key, qh[h]) for h in range(heads)]
        grads = [dot_nt(value, gh[h]) for h in range(heads)]
        for h in range(heads):
            prob = jnp.exp(logits[h])
            grad_value += dot_nn(prob.astype(BF16), gh[h])
            grad_score = (prob * grads[h]).astype(BF16)
            grad_key += dot_nn(grad_score, qh[h])
            part = dot_tn(grad_score, kh[h, here, :])
            if h == 0:
                total = part
            else:
                total += part

        @pl.when(r == 0)
        def _():
            dq[...] = total

        @pl.when(r > 0)
        def _():
            dq[...] += total

        low = grad_key[:, :cols].astype(BF16)
        dqkv[here, cols : 2 * cols] = low
        low = grad_value[:, :cols].astype(BF16)
        dqkv[here, 2 * cols :] = low
        bias_ref[0, 1:2, :] += jnp.sum(low.astype(F32), axis=0, keepdims=True)

    @pl.loop(0, rows, step=BLOCK)
    def _(r):
        r = pl.multiple_of(r, BLOCK)
        here = pl.ds(r, BLOCK)
        low = (dq[here, :cols] * HEAD**-0.5).astype(BF16)
        dqkv[here, :cols] = low
        bias_ref[0, 0:1, :] += jnp.sum(low.astype(F32), axis=0, keepdims=True)
        gtok_ref[here, :] += dot_nt(dqkv[here, :], w_ref[0, :, : 3 * cols])

    before_grads()
    half = width // 2

    @pl.loop(0, width, step=half)
    def _(c):
        c = pl.multiple_of(c, half)
        here = pl.ds(c, half)
        put_grads(c, dot_tn(x_ref[:, here], dqkv[...]), dot_tn(gattn_ref[:, here], mix_ref[0]))


def attend_back_kernel(
    x_ref, w_ref, gattn_ref, gfirst_ref, q_ref, k_ref, v_ref, mix_ref, lse_ref,
    gtok_ref, grad_ref, bias_ref,
    *scratch,
):
    wide = 3 * mix_ref.shape[2]

    def put(c, qkv, out):
        here = pl.ds(c, qkv.shape[0])
        grad_ref[0, here, :wide] = qkv.astype(BF16)
        grad_ref[0, here, wide:] = out.astype(BF16)

    attend_back_steps(
        lambda r: None, lambda: None, put,
        x_ref, w_ref, gattn_ref, gfirst_ref, q_ref, k_ref, v_ref, mix_ref, lse_ref, gtok_ref, bias_ref,
        *scratch,
    )


def attend_back_collect_kernel(
    tab_ref, x_ref, w_ref, gattn_ref, gfirst_ref, q_ref, k_ref, v_ref, mix_ref, lse_ref, vec_ref,
    gup_ref, gdn_ref,
    gtok_ref, attn_out, up_out, down_out, small_out,
    qh, gh, dq, kh, dqkv, bias_ref, bias_all,
    gs, attn_rc, attn_rb, tail_rx, tail_rz, tail_sz, tail_sx,
    up_acc, up_rc, up_rb, up_ra, up_rz,
    down_acc, down_rc, down_rb, down_ra, down_rz,
    rest_acc, rest_rc, rest_rz, rest_rx, rest_ry,
    small_src, small_acc, small_rc, small_rb, small_ra, small_rz,
    send, recv, home,
):
    t = pl.program_id(0)
    last = pl.num_programs(0) - 1
    place = Place()
    cols = mix_ref.shape[2]
    wide = 3 * cols

    def collect(n, near, far, rc, rb, ra, rz, axis):
        return Collect(place, near, far, rc, rb, ra, rz, send.at[n], recv.at[n], axis)

    attn = collect(0, gs.at[3], gs.at[1], attn_rc, attn_rb, None, None, "x")
    up = collect(1, up_acc.at[0], up_acc.at[1], up_rc, up_rb, up_ra, up_rz, "x")
    down = collect(2, down_acc.at[0], down_acc.at[1], down_rc, down_rb, down_ra, down_rz, "y")
    small = collect(3, small_acc.at[0], small_acc.at[1], small_rc, small_rb, small_ra, small_rz, "x")
    rest = CollectFlat(place, rest_acc, rest_rc, rest_rz, rest_rx, rest_ry, send.at[4], recv.at[4])
    tail = Tail(place, gs.at[3], tail_rx, tail_rz, tail_sz, tail_sx, send.at[5], recv.at[5])
    rows_y = (place.y, 1 - place.y)
    cut = down_acc.shape[3]
    head, foot = slice(0, cut), slice(cut, cut + rest_acc.shape[3])

    def homes(src, acc, n, rows=slice(None)):
        return [
            pltpu.make_async_copy(src.at[y, place.c, :, :, rows], acc.at[dy], home.at[n, dy])
            for dy, y in enumerate(rows_y)
        ]

    def begin(piece, src, acc, n, rows=slice(None)):
        for dy, y in enumerate(rows_y):
            piece.copy_c(src.at[y, 1 - place.c, :, :, rows], dy).start()
        for copy in homes(src, acc, n, rows):
            copy.start()

    def settle(src, acc, n, rows=slice(None)):
        for copy in homes(src, acc, n, rows):
            copy.wait()

    @pl.when(t == 0)
    def _():
        place.greet()
        begin(up, gup_ref, up_acc, 0)
        begin(down, gdn_ref, down_acc, 1, head)
        begin(rest, gdn_ref, rest_acc, 3, foot)

    @pl.when(t == 1)
    def _():
        attn.copy_c(gs.at[0], 1).start()

    @pl.when(t == 2)
    def _():
        up.sum_b()

    @pl.when(t == 3)
    def _():
        attn.copy_c(gs.at[2], 0).start()
        up.sum_a()

    def hook(r):
        def at(step, block, *events):
            @pl.when((t == step) & (r == block * BLOCK))
            def _():
                for event in events:
                    event()

        def up_first():
            settle(gup_ref, up_acc, 0)
            up.sum_c()

        def down_first():
            settle(gdn_ref, down_acc, 1, head)
            settle(gdn_ref, rest_acc, 3, foot)
            down.sum_c()
            rest.sum_c()

        at(0, 1, up_first)
        at(0, 2, up.send_b)
        at(0, 3, down_first)
        at(1, 3, down.sum_b)
        at(2, 0, up.send_a, attn.send_b)
        at(2, 1, rest.sum_z)
        at(2, 2, rest.send_x, down.sum_a)
        at(2, 3, down.send_z, rest.sum_x)
        at(3, 0, up.send_z)
        at(3, 1, lambda: down.sum_z(down_out.at[head]))
        at(3, 2, lambda: rest.sum_y(down_out.at[foot]))

    g = place.group(last - t)

    def before_grads():
        bias_all[g] = bias_ref[0]

        @pl.when(t == 0)
        def _():
            down.send_b()
            rest.send_z()

        @pl.when(t == 1)
        def _():
            down.send_a()
            attn.wait_c(1)

        @pl.when(t == 2)
        def _():
            rest.send_y()

        @pl.when(t == last)
        def _():
            attn.wait_c(0)
            attn.wait_b()

    def put(c, qkv, out):
        start = lax.div(c, 2 * gs.shape[3])
        some = pl.ds(start, qkv.shape[0] // (2 * gs.shape[3]))
        shape = (qkv.shape[0] // (2 * gs.shape[3]), *gs.shape[2:4])

        def store(*more):
            for lanes, value in ((slice(0, wide), qkv), (slice(wide, None), out)):
                value = value.reshape(*shape, value.shape[1])
                for ref in more:
                    value = value + ref[some, :, :, lanes].astype(F32)
                gs[t, some, :, :, lanes] = value.astype(BF16)

        @pl.when((t == 0) | (t == 2))
        def _():
            store()

        @pl.when(t == 1)
        def _():
            store(attn_rc.at[1])

        @pl.when(t == last)
        def _():
            store(attn_rc.at[0], attn_rb)

    attend_back_steps(
        hook, before_grads, put,
        x_ref, w_ref, gattn_ref, gfirst_ref, q_ref, k_ref, v_ref, mix_ref, lse_ref, gtok_ref, bias_ref,
        qh, gh, dq, kh, dqkv,
    )

    @pl.when(t == last)
    def _():
        up.sum_z(up_out)
        for copy in tail.first():
            copy.start()
        lines = [
            jnp.concatenate([bias_all[n, row : row + 1, :] for n in range(bias_all.shape[0])], axis=1)
            for row in range(2)
        ]
        cut_vectors(jnp.concatenate([*lines, vec_ref[0:6, :]], axis=0), vec_ref[8:12, :], tab_ref, small_src)
        begin(small, small_src, small_acc, 2)
        settle(small_src, small_acc, 2)
        small.sum_c()
        small.send_b()
        small.sum_b()
        small.send_a()
        up.finish()
        down.finish()
        rest.finish()
        tail.sum_first()
        small.sum_a()
        small.send_z()
        for copy in tail.second():
            copy.start()
        small.sum_z(small_out)
        small.finish()
        for dy in range(2):
            attn.copy_c(attn_rc.at[dy], dy).wait_send()
        for copy in attn.copies_b():
            copy.wait_send()
        tail.sum_second(attn_out)
        tail.finish()


def resident(shape):
    return pl.BlockSpec(shape, lambda *ids: (0,) * len(shape), pipeline_mode=pl.Buffered(1))


def result(shape):
    return pl.BlockSpec(shape, lambda *ids: (0,) * len(shape))


def per_step(shape):
    return pl.BlockSpec((1, *shape[1:]), lambda t: (t, 0, 0))


def struct(shape, dtype):
    return jax.ShapeDtypeStruct(shape, dtype)


def params(steps):
    return pltpu.CompilerParams(
        dimension_semantics=("arbitrary",) * steps, vmem_limit_bytes=VMEM_LIMIT
    )


def attend_outs(groups, rows, width):
    cols = width // groups
    wide = (groups, rows, WIDE)
    specs = [
        result((rows, width)),
        per_step(wide), per_step(wide), per_step(wide),
        per_step((groups, rows, cols)), per_step((groups, rows, 128)),
    ]
    shapes = [
        struct((rows, width), F32),
        struct(wide, BF16), struct(wide, BF16), struct(wide, BF16),
        struct((groups, rows, cols), BF16), struct((groups, rows, 128), F32),
    ]
    return specs, shapes


def run_attend(length, tokens, w_attn, bias, out_bias):
    rows, width = tokens.shape
    groups = w_attn.shape[0]
    specs, shapes = attend_outs(groups, rows, width)
    return pl.pallas_call(
        attend_kernel,
        grid=(groups,),
        in_specs=[
            pl.BlockSpec(memory_space=pltpu.SMEM),
            resident((rows, width)),
            per_step(w_attn.shape),
            resident(bias.shape),
            resident(out_bias.shape),
        ],
        out_specs=specs,
        out_shape=shapes,
        compiler_params=params(1),
        name="attend",
    )(length, tokens, w_attn, bias, out_bias)


def run_attend_spread(lengths, tokens, vec, w_attn, w_up, w_down):
    rows, width = tokens.shape
    groups = 4
    specs, shapes = attend_outs(groups, rows, width)
    whole = (2, 2, DEPTH, 2)
    slab = (groups, width, width)
    table = segment_tables()
    return pl.pallas_call(
        attend_spread_kernel,
        grid=(groups,),
        in_specs=[
            pl.BlockSpec(memory_space=pltpu.SMEM), resident(table.shape), resident((rows, width)),
            resident(vec.shape), resident(w_attn.shape), resident(w_up.shape), resident(w_down.shape),
        ],
        out_specs=specs + [
            per_step(slab), result((16, width)),
            pl.BlockSpec(memory_space=pl.ANY), pl.BlockSpec(memory_space=pl.ANY),
        ],
        out_shape=shapes + [
            struct(slab, BF16), struct((16, width), F32),
            struct((*whole, *w_up.shape), BF16), struct((*whole, *w_down.shape), BF16),
        ],
        scratch_shapes=[
            pltpu.VMEM((*whole, *vec.shape), F32), pltpu.VMEM((*whole, *w_attn.shape), BF16),
            pltpu.VMEM((groups, 8, 3 * width // groups), F32),
            pltpu.SemaphoreType.DMA((5, SLOTS)), pltpu.SemaphoreType.DMA((5, SLOTS)),
            pltpu.SemaphoreType.DMA((5,)),
        ],
        compiler_params=pltpu.CompilerParams(
            dimension_semantics=("arbitrary",), vmem_limit_bytes=VMEM_LIMIT, collective_id=0,
            has_side_effects=True,
        ),
        name="attend",
    )(lengths, table, tokens, vec, w_attn, w_up, w_down)


def run_ffn(length, residual, cotangent, vectors, w_up, w_down):
    rows, width = residual.shape
    groups = w_up.shape[0]
    units = w_up.shape[2]
    slab = pl.BlockSpec((1, width, units), lambda p, t: (t, 0, 0))
    grad = pl.BlockSpec((1, width, units), lambda p, t: (p * t, 0, 0))
    return pl.pallas_call(
        ffn_kernel,
        grid=(2, groups),
        in_specs=[
            pl.BlockSpec(memory_space=pltpu.SMEM),
            resident((rows, width)),
            resident((rows, width)),
            resident(vectors.shape),
            slab, slab,
        ],
        out_specs=[
            result((rows, width)), result((rows, width)), result((rows, width)), result((16, width)),
            grad, grad,
        ],
        out_shape=[
            struct((rows, width), F32), struct((rows, width), F32), struct((rows, width), BF16),
            struct((16, width), F32),
            struct(w_up.shape, BF16), struct(w_up.shape, BF16),
        ],
        scratch_shapes=[
            pltpu.VMEM((rows, width), F32), pltpu.VMEM((rows, width), BF16),
            pltpu.VMEM((rows, width), F32), pltpu.VMEM((rows, width), BF16),
            pltpu.VMEM((groups, rows, units), BF16), pltpu.VMEM((groups, rows, units), F32),
            pltpu.VMEM((rows, units), BF16),
        ],
        compiler_params=params(2),
        name="ffn",
    )(length, residual, cotangent, vectors, w_up, w_down)


def back_scratch(rows, width, cols):
    heads = cols // HEAD
    return [
        pltpu.VMEM((heads, rows, WIDE), BF16), pltpu.VMEM((heads, rows, WIDE), BF16),
        pltpu.VMEM((rows, WIDE), F32), pltpu.VMEM((heads, rows, WIDE), BF16),
        pltpu.VMEM((rows, 3 * cols), BF16),
    ]


def run_attend_back(tokens, w_attn, grad_attn, grad_first, q, k, v, mixed, lse):
    rows, width = tokens.shape
    groups = w_attn.shape[0]
    cols = width // groups
    return pl.pallas_call(
        attend_back_kernel,
        grid=(groups,),
        in_specs=[
            resident((rows, width)), per_step(w_attn.shape),
            resident((rows, width)), resident((rows, width)),
            per_step(q.shape), per_step(k.shape), per_step(v.shape),
            per_step(mixed.shape), per_step(lse.shape),
        ],
        out_specs=[result((rows, width)), per_step(w_attn.shape), per_step((groups, 8, cols))],
        out_shape=[
            struct((rows, width), F32), struct(w_attn.shape, BF16), struct((groups, 8, cols), F32),
        ],
        scratch_shapes=back_scratch(rows, width, cols),
        compiler_params=params(1),
        name="attend_back",
    )(tokens, w_attn, grad_attn, grad_first, q, k, v, mixed, lse)


def run_attend_back_collect(
    tokens, w_attn, grad_attn, grad_first, q, k, v, mixed, lse, small, grad_up, grad_down
):
    rows, width = tokens.shape
    groups = w_attn.shape[0]
    cols = width // groups
    table = segment_tables()

    def back(shape):
        return pl.BlockSpec((1, *shape[1:]), lambda t: (groups - 1 - t, 0, 0))

    def buffers(block, dtype, last):
        chip = (DEPTH, 2, *block)
        return [
            pltpu.VMEM((2, *chip), dtype),
            pltpu.VMEM(chip if last == "x" else (2, DEPTH, *block), dtype),
            pltpu.VMEM((DEPTH, *block), dtype), pltpu.VMEM((DEPTH - 1, *block), dtype),
        ]

    part = (width // (2 * DEPTH), width)
    half, third = (part[0] // 2, width), part[0] // 3
    pair = (2, DEPTH, 2)
    dots = (16, 128)
    return pl.pallas_call(
        attend_back_collect_kernel,
        grid=(groups,),
        in_specs=[
            resident(table.shape), resident((rows, width)), back(w_attn.shape),
            resident((rows, width)), resident((rows, width)),
            back(q.shape), back(k.shape), back(v.shape), back(mixed.shape), back(lse.shape),
            resident(small.shape),
            pl.BlockSpec(memory_space=pl.ANY), pl.BlockSpec(memory_space=pl.ANY),
        ],
        out_specs=[result((rows, width)), result(part), result(part), result(part), result(dots)],
        out_shape=[
            struct((rows, width), F32), struct(part, F32), struct(part, F32), struct(part, F32),
            struct(dots, F32),
        ],
        scratch_shapes=[
            *back_scratch(rows, width, cols),
            pltpu.VMEM((1, 8, cols), F32), pltpu.VMEM((groups, 8, cols), F32),
            pltpu.VMEM((groups, DEPTH, 2, *part), BF16), *buffers(part, BF16, "x")[:2],
            pltpu.VMEM((DEPTH, 2 * third, width), BF16), pltpu.VMEM((DEPTH - 1, 2 * third, width), BF16),
            pltpu.VMEM((DEPTH - 1, 2, third, width), BF16), pltpu.VMEM((third, width), BF16),
            pltpu.VMEM((*pair, *part), BF16), *buffers(part, BF16, "x"),
            pltpu.VMEM((*pair, *half), BF16), *buffers(half, BF16, "y"),
            pltpu.VMEM((*pair, *half), BF16), pltpu.VMEM((*pair, *half), BF16),
            pltpu.VMEM((DEPTH - 1, 2, 2, *half), BF16), pltpu.VMEM((2, *half), BF16), pltpu.VMEM(half, BF16),
            pltpu.VMEM((2, *pair, *dots), F32), pltpu.VMEM((*pair, *dots), F32), *buffers(dots, F32, "x"),
            pltpu.SemaphoreType.DMA((6, 8)), pltpu.SemaphoreType.DMA((6, 8)),
            pltpu.SemaphoreType.DMA((4, 2)),
        ],
        compiler_params=pltpu.CompilerParams(
            dimension_semantics=("arbitrary",), vmem_limit_bytes=VMEM_LIMIT, collective_id=1,
            has_side_effects=True,
        ),
        name="attend_back",
    )(table, tokens, w_attn, grad_attn, grad_first, q, k, v, mixed, lse, small, grad_up, grad_down)


def shards(
    tokens, lengths, w_query, w_key, w_value, w_out, w_up, w_down,
    query_bias, value_bias, out_bias, attn_gain, attn_shift, up_bias, down_bias, ffn_gain, ffn_shift,
    cotangent,
):
    rows, width = tokens.shape
    groups = lax.axis_size("tensor")
    spans = lax.axis_size("dp")
    seq_count = lengths.shape[0]
    assert rows * groups == seq_count * rows and seq_count == groups
    rank = lax.axis_index("tensor")
    length = lax.dynamic_slice_in_dim(lengths, rank, 1)
    both = ("dp", "tensor")

    cols = width // groups
    units = w_up.shape[1]
    count = query_bias.shape[0]
    vectors = (query_bias, value_bias, out_bias, attn_gain, attn_shift, down_bias, ffn_gain, ffn_shift)
    flat = jnp.concatenate([*vectors, up_bias])
    own_attn = jnp.concatenate([w_query, w_key, w_value, w_out.T], axis=1)

    near = (spans, groups, width, units) == (8, 4, 768, 768)
    if near:
        vec = jnp.pad(jnp.stack(vectors), ((0, 8), (0, 128 - count)))
        vec = vec.at[8, : up_bias.shape[0]].set(up_bias)
        residual, q, k, v, mixed, lse, w_attn, full, w_in, w_back = run_attend_spread(
            lengths, tokens, vec, own_attn, w_up, w_down.T
        )
        w_in, w_back = w_in.reshape(groups, width, units), w_back.reshape(groups, width, units)
    else:
        pack = jnp.concatenate([own_attn, w_up, w_down.T], axis=1)
        whole = lax.all_gather(pack, both, axis=0, tiled=True)
        whole = whole.reshape(spans, groups, *pack.shape).swapaxes(0, 1)
        whole = whole.reshape(groups, width, pack.shape[1])
        w_attn, w_in, w_back = jnp.split(whole, [4 * cols, 4 * cols + units], axis=2)
        gathered = lax.all_gather(flat, both, axis=0, tiled=True).reshape(spans * groups, -1)
        full = gathered[:, : 8 * count].reshape(-1, 8, count).swapaxes(0, 1).reshape(8, width)
        full = jnp.concatenate([full, gathered[:, 8 * count :].reshape(groups, units)])
        full = jnp.pad(full, ((0, 16 - full.shape[0]), (0, 0)))
        qb, vb = full[0].reshape(groups, 1, cols), full[1].reshape(groups, 1, cols)
        bias = jnp.pad(jnp.concatenate([qb, jnp.zeros_like(qb), vb], axis=2), ((0, 0), (0, 7), (0, 0)))
        residual, q, k, v, mixed, lse = run_attend(length, tokens, w_attn, bias, full[2:3])
    output, grad_first, grad_attn, small, grad_in, grad_back = run_ffn(
        length, residual, cotangent, full, w_in, w_back
    )
    if near:
        split = (2, 2, DEPTH, 2, width // (2 * DEPTH), units)
        grad_tokens, own_a, own_u, own_d, dots = run_attend_back_collect(
            tokens, w_attn, grad_attn, grad_first, q, k, v, mixed, lse, small,
            grad_in.reshape(split), grad_back.reshape(split),
        )
        tiny8 = dots[:8, :count]
        return (
            output, grad_tokens,
            own_a[:, :cols], own_a[:, cols : 2 * cols], own_a[:, 2 * cols : 3 * cols], own_a[:, 3 * cols :].T,
            own_u, own_d.T,
            tiny8[0], tiny8[1], tiny8[2], tiny8[3], tiny8[4], dots[8, : up_bias.shape[0]],
            tiny8[5], tiny8[6], tiny8[7],
        )
    grad_tokens, grad_attn_w, bias_grad = run_attend_back(
        tokens, w_attn, grad_attn, grad_first, q, k, v, mixed, lse
    )

    every = jnp.concatenate([grad_attn_w, grad_in, grad_back], axis=2)
    every = every.reshape(groups, spans, width // spans, -1).swapaxes(0, 1)
    every = every.reshape(spans * groups * (width // spans), -1)
    owned = lax.psum_scatter(every, both, scatter_dimension=0, tiled=True).astype(F32)

    rows8 = jnp.concatenate(
        [bias_grad[:, 0].reshape(1, width), bias_grad[:, 1].reshape(1, width), small[:6]]
    )
    parts = jnp.concatenate(
        [
            rows8.reshape(8, spans * groups, count).swapaxes(0, 1).reshape(spans * groups, 8 * count),
            small[8 : 8 + groups].reshape(spans * groups, -1),
        ],
        axis=1,
    )
    tiny = lax.psum_scatter(parts.reshape(-1), both, scatter_dimension=0, tiled=True)
    tiny8 = tiny[: 8 * count].reshape(8, count)
    return (
        output, grad_tokens,
        owned[:, :cols], owned[:, cols : 2 * cols], owned[:, 2 * cols : 3 * cols],
        owned[:, 3 * cols : 4 * cols].T,
        owned[:, 4 * cols : 4 * cols + units], owned[:, 4 * cols + units :].T,
        tiny8[0], tiny8[1], tiny8[2], tiny8[3], tiny8[4], tiny[8 * count :], tiny8[5], tiny8[6], tiny8[7],
    )


def solution(mesh):
    rows, vector, matrix, flipped = (
        P(("dp", "tensor"), None), P(("dp", "tensor")), P("dp", "tensor"), P("tensor", "dp"),
    )
    return jax.shard_map(
        shards,
        mesh=mesh,
        in_specs=(rows, P("dp"), matrix, matrix, matrix, flipped, matrix, flipped, *(vector,) * 9, rows),
        out_specs=(rows, rows, matrix, matrix, matrix, flipped, matrix, flipped, *(vector,) * 9),
        check_vma=False,
    )
```

```python
import jax
import jax.numpy as jnp
import numpy as np
from jax import lax
from jax.experimental import pallas as pl
from jax.experimental.pallas import tpu as pltpu
from jax.sharding import PartitionSpec as P

HEAD = 64
EPSILON = 1e-12
FLOOR_SCORE = -1e30
BLOCK = 256
WIDE = 256
BF16 = jnp.bfloat16
F32 = jnp.float32
VMEM_LIMIT = 60 * 1024 * 1024


def dot_nn(a, b):
    return lax.dot_general(a, b, (((1,), (0,)), ((), ())), preferred_element_type=F32)


def dot_nt(a, b):
    return lax.dot_general(a, b, (((1,), (1,)), ((), ())), preferred_element_type=F32)


def dot_tn(a, b):
    return lax.dot_general(a, b, (((0,), (0,)), ((), ())), preferred_element_type=F32)


def lane_iota(rows, lanes):
    return lax.broadcasted_iota(jnp.int32, (rows, lanes), 1)


def row_iota(rows, lanes):
    return lax.broadcasted_iota(jnp.int32, (rows, lanes), 0)


def head_mask(rows, h, extra):
    lane = lane_iota(rows, WIDE)
    keep = (lane >= h * HEAD) & (lane < (h + 1) * HEAD)
    if extra is not None:
        keep = keep | (lane >= extra)
    return keep


def normalize(v):
    center = v - jnp.mean(v, axis=-1, keepdims=True)
    inv = lax.rsqrt(jnp.mean(center * center, axis=-1, keepdims=True) + EPSILON)
    return center * inv, inv


def norm_back(g, n, inv):
    return inv * (
        g - jnp.mean(g, axis=-1, keepdims=True) - n * jnp.mean(g * n, axis=-1, keepdims=True)
    )


def split_three(v):
    hi = v.astype(BF16)
    rest = v - hi.astype(F32)
    mid = rest.astype(BF16)
    low = (rest - mid.astype(F32)).astype(BF16)
    return hi.astype(F32), mid.astype(F32), low.astype(F32)


MESH = pl.DeviceIdType.MESH
DEPTH = 4
SLOTS = 14


def around(z, k):
    return (z, z + 1 - 2 * lax.rem(z, 2), DEPTH - 1 - z, lax.rem(z + 2, DEPTH))[k]


class Place:
    def __init__(self):
        dp, t = lax.axis_index("dp"), lax.axis_index("tensor")
        self.z, self.x = lax.div(dp, 2), lax.rem(dp, 2)
        self.y, self.c = lax.div(t, 2), lax.rem(t, 2)

    def device(self, z=None, x=None, y=None, c=None):
        z, x = self.z if z is None else z, self.x if x is None else x
        y, c = self.y if y is None else y, self.c if c is None else c
        return (z * 2 + x, y * 2 + c)

    def neighbours(self):
        return [self.device(z=around(self.z, k)) for k in range(1, DEPTH)] + [
            self.device(x=1 - self.x), self.device(y=1 - self.y), self.device(c=1 - self.c),
        ]

    def greet(self):
        barrier = pltpu.get_barrier_semaphore()
        peers = self.neighbours()
        for peer in peers:
            pl.semaphore_signal(barrier, inc=1, device_id=peer, device_id_type=MESH)
        pl.semaphore_wait(barrier, len(peers))

    def group(self, step):
        y = lax.rem(self.y + lax.div(step, 2), 2)
        c = lax.rem(self.c + lax.rem(step, 2), 2)
        return y * 2 + c


def remote(src, dst, send, recv, device):
    return pltpu.make_async_remote_copy(
        src_ref=src, dst_ref=dst, send_sem=send, recv_sem=recv, device_id=device, device_id_type=MESH
    )


class Moves:
    def __init__(self, place, send, recv):
        self.p, self.send, self.recv = place, send, recv
        self.to_x, self.to_y = place.device(x=1 - place.x), place.device(y=1 - place.y)
        self.to_c = place.device(c=1 - place.c)

    def to_z(self, k):
        return self.p.device(z=around(self.p.z, k))

    def copy(self, src, dst, slot, device):
        return remote(src, dst, self.send.at[slot], self.recv.at[slot], device)

    def arrive(self, ref, slot, device):
        self.copy(ref, ref, slot, device).wait_recv()

    def gone(self, ref, slot, device):
        self.copy(ref, ref, slot, device).wait_send()


class Spread(Moves):
    def __init__(self, place, own, buf, send, recv, home, first, rows=slice(None)):
        super().__init__(place, send, recv)
        self.own, self.buf, self.home, self.first, self.rows = own.at[rows], buf, home, first, rows
        self.to_a, self.to_b = (self.to_x, self.to_y) if first == "x" else (self.to_y, self.to_x)

    def at(self, z, a=0, b=0):
        p = self.p
        dx, dy = (a, b) if self.first == "x" else (b, a)
        return self.buf.at[p.y if dy == 0 else 1 - p.y, p.c, z, p.x if dx == 0 else 1 - p.x, self.rows]

    def chip(self, dy, c=0):
        p = self.p
        y = p.y if dy == 0 else 1 - p.y
        return self.buf.at[y, p.c if c == 0 else 1 - p.c, :, :, self.rows]

    def local(self):
        return pltpu.make_async_copy(self.own, self.at(self.p.z), self.home)

    def begin_z(self):
        for k in range(1, DEPTH):
            self.copy(self.own, self.at(self.p.z), k - 1, self.to_z(k)).start()

    def begin_ab(self):
        self.local().start()
        self.copy(self.own, self.at(self.p.z), 3, self.to_a).start()
        self.copy(self.own, self.at(self.p.z), 7, self.to_b).start()

    def after_z(self):
        for k in range(1, DEPTH):
            ref = self.at(around(self.p.z, k))
            self.arrive(ref, k - 1, self.to_z(k))
            self.copy(ref, ref, 3 + k, self.to_a).start()
            self.copy(ref, ref, 7 + k, self.to_b).start()
        self.local().wait()

    def after_a(self):
        for k in range(DEPTH):
            self.arrive(self.at(around(self.p.z, k), a=1), 3 + k, self.to_a)
        ref = self.at(slice(None), a=1)
        self.copy(ref, ref, 11, self.to_b).start()
        if self.first == "x":
            self.swap(0)

    def swap(self, dy):
        ref = self.chip(dy)
        self.copy(ref, ref, 12 + dy, self.to_c).start()

    def after_b(self):
        for k in range(DEPTH):
            self.arrive(self.at(around(self.p.z, k), b=1), 7 + k, self.to_b)
        if self.first == "y":
            self.swap(0)
        self.arrive(self.at(slice(None), a=1, b=1), 11, self.to_b)
        self.swap(1)

    def after_c(self, dy):
        self.arrive(self.chip(dy, c=1), 12 + dy, self.to_c)

    def finish(self):
        one, column, chip = self.at(self.p.z), self.at(slice(None)), self.chip(0)
        for k in range(1, DEPTH):
            self.gone(one, k - 1, self.to_z(k))
        for k in range(DEPTH):
            self.gone(one, 3 + k, self.to_a)
            self.gone(one, 7 + k, self.to_b)
        self.gone(column, 11, self.to_b)
        for dy in range(2):
            self.gone(chip, 12 + dy, self.to_c)


class SpreadFlat(Moves):
    def __init__(self, place, own, buf, send, recv, home, rows=slice(None)):
        super().__init__(place, send, recv)
        self.own, self.buf, self.home, self.rows = own.at[rows], buf, home, rows

    def at(self, y=slice(None), z=slice(None), x=slice(None), c=0):
        return self.buf.at[y, self.p.c if c == 0 else 1 - self.p.c, z, x, self.rows]

    def local(self):
        p = self.p
        return pltpu.make_async_copy(self.own, self.at(p.y, p.z, p.x), self.home)

    def begin(self):
        p = self.p
        self.local().start()
        self.copy(self.own, self.at(p.y, p.z, p.x), 0, self.to_y).start()

    def after_y(self):
        p = self.p
        self.local().wait()
        self.arrive(self.at(1 - p.y, p.z, p.x), 0, self.to_y)
        ref = self.at(z=p.z, x=p.x)
        self.copy(ref, ref, 1, self.to_x).start()

    def after_x(self):
        p = self.p
        self.arrive(self.at(z=p.z, x=1 - p.x), 1, self.to_x)
        ref = self.at(z=p.z)
        for k in range(1, DEPTH):
            self.copy(ref, ref, 1 + k, self.to_z(k)).start()

    def after_z(self):
        for k in range(1, DEPTH):
            self.arrive(self.at(z=around(self.p.z, k)), 1 + k, self.to_z(k))
        ref = self.at()
        self.copy(ref, ref, 5, self.to_c).start()

    def after_c(self):
        self.arrive(self.at(c=1), 5, self.to_c)

    def finish(self):
        p = self.p
        self.gone(self.at(p.y, p.z, p.x), 0, self.to_y)
        self.gone(self.at(z=p.z, x=p.x), 1, self.to_x)
        for k in range(1, DEPTH):
            self.gone(self.at(z=p.z), 1 + k, self.to_z(k))
        self.gone(self.at(), 5, self.to_c)


class Collect:
    def __init__(self, place, near, far, rc, rb, ra, rz, send, recv, last):
        self.p, self.near, self.far, self.last = place, near, far, last
        self.rc, self.rb, self.ra, self.rz, self.send, self.recv = rc, rb, ra, rz, send, recv
        to_x, to_y = place.device(x=1 - place.x), place.device(y=1 - place.y)
        self.to_a, self.to_b = (to_x, to_y) if last == "x" else (to_y, to_x)
        self.to_c = place.device(c=1 - place.c)

    def copy(self, src, dst, slot, device):
        return pltpu.make_async_remote_copy(
            src_ref=src, dst_ref=dst, send_sem=self.send.at[slot], recv_sem=self.recv.at[slot],
            device_id=device, device_id_type=MESH,
        )

    def copy_c(self, src, dy):
        return self.copy(src, self.rc.at[dy], dy, self.to_c)

    def copies_b(self):
        if self.last == "x":
            return [self.copy(self.far, self.rb, 2, self.to_b)]
        there = (slice(None), 1 - self.p.x)
        return [
            self.copy(part.at[there], self.rb.at[dy], 2 + 5 * dy, self.to_b)
            for dy, part in enumerate((self.near, self.far))
        ]

    def copy_a(self):
        if self.last == "x":
            return self.copy(self.near.at[:, 1 - self.p.x], self.ra, 3, self.to_a)
        return self.copy(self.far.at[:, self.p.x], self.ra, 3, self.to_a)

    def copies_z(self):
        p = self.p
        return [
            self.copy(
                self.near.at[around(p.z, k), p.x], self.rz.at[k - 1], 3 + k, p.device(z=around(p.z, k))
            )
            for k in range(1, DEPTH)
        ]

    def wait_c(self, dy):
        self.copy_c(self.rc.at[dy], dy).wait_recv()

    def wait_b(self):
        for copy in self.copies_b():
            copy.wait_recv()

    def sum_c(self):
        for dy, part in enumerate((self.near, self.far)):
            self.wait_c(dy)

            @pl.loop(0, DEPTH)
            def _(z):
                part[z] = add(part[z], self.rc[dy, z]).astype(part.dtype)

    def send_b(self):
        for copy in self.copies_b():
            copy.start()

    def sum_b(self):
        self.wait_b()
        x = self.p.x

        @pl.loop(0, DEPTH)
        def _(z):
            if self.last == "x":
                self.near[z] = add(self.near[z], self.rb[z]).astype(self.near.dtype)
            else:
                for dy, part in enumerate((self.near, self.far)):
                    part[z, x] = add(part[z, x], self.rb[dy, z]).astype(part.dtype)

    def send_a(self):
        self.copy_a().start()

    def sum_a(self):
        self.copy_a().wait_recv()
        x = self.p.x

        @pl.loop(0, DEPTH)
        def _(z):
            self.near[z, x] = add(self.near[z, x], self.ra[z]).astype(self.near.dtype)

    def send_z(self):
        for copy in self.copies_z():
            copy.start()

    def sum_z(self, out_ref):
        for copy in self.copies_z():
            copy.wait_recv()
        total = self.near[self.p.z, self.p.x].astype(F32)
        for k in range(DEPTH - 1):
            total = total + self.rz[k].astype(F32)
        out_ref[...] = total

    def finish(self):
        for dy in range(2):
            self.copy_c(self.rc.at[dy], dy).wait_send()
        for copy in [*self.copies_b(), self.copy_a(), *self.copies_z()]:
            copy.wait_send()


class CollectFlat(Moves):
    def __init__(self, place, acc, rc, rz, rx, ry, send, recv):
        super().__init__(place, send, recv)
        self.acc, self.rc, self.rz, self.rx, self.ry = acc, rc, rz, rx, ry

    def copy_c(self, src, dy):
        return self.copy(src, self.rc.at[dy], dy, self.to_c)

    def copies_z(self):
        return [
            self.copy(self.acc.at[:, around(self.p.z, k)], self.rz.at[k - 1], 1 + k, self.to_z(k))
            for k in range(1, DEPTH)
        ]

    def copy_x(self):
        return self.copy(self.acc.at[:, self.p.z, 1 - self.p.x], self.rx, 5, self.to_x)

    def copy_y(self):
        return self.copy(self.acc.at[1, self.p.z, self.p.x], self.ry, 6, self.to_y)

    def sum_c(self):
        for dy in range(2):
            self.copy_c(self.rc.at[dy], dy).wait_recv()

            @pl.loop(0, DEPTH)
            def _(z):
                self.acc[dy, z] = add(self.acc[dy, z], self.rc[dy, z]).astype(BF16)

    def send_z(self):
        for copy in self.copies_z():
            copy.start()

    def sum_z(self):
        for copy in self.copies_z():
            copy.wait_recv()
        z = self.p.z
        for dy in range(2):
            total = add(self.acc[dy, z], self.rz[0, dy])
            total = total + add(self.rz[1, dy], self.rz[2, dy])
            self.acc[dy, z] = total.astype(BF16)

    def send_x(self):
        self.copy_x().start()

    def sum_x(self):
        self.copy_x().wait_recv()
        z, x = self.p.z, self.p.x
        for dy in range(2):
            self.acc[dy, z, x] = add(self.acc[dy, z, x], self.rx[dy]).astype(BF16)

    def send_y(self):
        self.copy_y().start()

    def sum_y(self, out_ref):
        self.copy_y().wait_recv()
        out_ref[...] = add(self.acc[0, self.p.z, self.p.x], self.ry[...])

    def finish(self):
        for dy in range(2):
            self.copy_c(self.rc.at[dy], dy).wait_send()
        for copy in [*self.copies_z(), self.copy_x(), self.copy_y()]:
            copy.wait_send()


class Tail(Moves):
    def __init__(self, place, near, rx, rz, sz, sx, send, recv):
        super().__init__(place, send, recv)
        self.near, self.rx, self.rz, self.sz, self.sx = near, rx, rz, sz, sx
        cut = rx.shape[1]
        self.most, self.others = slice(0, cut), slice(cut, cut + sx.shape[0])

    def first(self):
        p = self.p
        copies = [self.copy(self.near.at[:, 1 - p.x, self.most], self.rx, 0, self.to_x)]
        return copies + [
            self.copy(self.near.at[around(p.z, k), :, self.others], self.sz.at[k - 1], k, self.to_z(k))
            for k in range(1, DEPTH)
        ]

    def second(self):
        p = self.p
        copies = [
            self.copy(self.near.at[around(p.z, k), p.x, self.most], self.rz.at[k - 1], 3 + k, self.to_z(k))
            for k in range(1, DEPTH)
        ]
        return copies + [self.copy(self.near.at[p.z, 1 - p.x, self.others], self.sx, 7, self.to_x)]

    def sum_first(self):
        for copy in self.first():
            copy.wait_recv()
        p = self.p

        @pl.loop(0, DEPTH)
        def _(z):
            self.near[z, p.x, self.most] = add(self.near[z, p.x, self.most], self.rx[z]).astype(BF16)

        total = add(self.near[p.z, :, self.others], self.sz[0])
        total = total + add(self.sz[1], self.sz[2])
        self.near[p.z, :, self.others] = total.astype(BF16)

    def sum_second(self, out_ref):
        for copy in self.second():
            copy.wait_recv()
        p = self.p
        total = add(self.near[p.z, p.x, self.most], self.rz[0])
        out_ref[self.most, :] = total + add(self.rz[1], self.rz[2])
        out_ref[self.others, :] = add(self.near[p.z, p.x, self.others], self.sx[...])

    def finish(self):
        for copy in [*self.first(), *self.second()]:
            copy.wait_send()


def add(a, b):
    return a.astype(F32) + b.astype(F32)


def segment_tables():
    lane = np.arange(768, dtype=np.int32)
    rows = np.stack([lane % 24, lane // 24, lane % 96, lane // 96])
    return jnp.asarray(np.concatenate([rows, np.zeros_like(rows)]))


def one_hot(tab_ref, row, start, rows):
    return (row_iota(rows, tab_ref.shape[1]) == start + tab_ref[row : row + 1, :]).astype(BF16)


def owners(shape, dim):
    p = lax.broadcasted_iota(jnp.int32, shape, dim)
    return lax.shift_left(p & 7, 2) + lax.shift_right_logical(p, 3)


def join_vectors(block_ref, tab_ref, vec_ref):
    blocks = block_ref[...].reshape(32, 16, 128)
    width = vec_ref.shape[1]

    def place(values, table):
        hot = one_hot(tab_ref, table, 0, 128)
        hi, mid, low = (dot_nn(part.astype(BF16), hot) for part in split_three(values))
        return hi + mid + low

    keep = owners((32, 16, width), 0) == tab_ref[1:2, :][None]
    got = place(blocks.reshape(512, 128), 0).reshape(32, 16, width)
    vec_ref[...] = jnp.sum(jnp.where(keep, got, 0.0), axis=0)
    row = lax.broadcasted_iota(jnp.int32, (32, 16, 128), 1)
    got = place(jnp.sum(jnp.where(row == 8, blocks, 0.0), axis=1), 2)
    for k in range(4):
        keep = owners((32, width), 0) == tab_ref[3:4, :] + 8 * k
        vec_ref[8 + k : 9 + k, :] = jnp.sum(jnp.where(keep, got, 0.0), axis=0, keepdims=True)


def cut_vectors(eight, up_rows, tab_ref, out_ref):
    width = tab_ref.shape[1]

    def pick(values, table):
        hot = one_hot(tab_ref, table, 0, 128)
        return sum(dot_nt(part.astype(BF16), hot) for part in split_three(values))

    both = jnp.concatenate([eight, jnp.zeros_like(eight)], axis=0)
    keep = owners((32, 16, width), 0) == tab_ref[1:2, :][None]
    spread = jnp.where(keep, jnp.broadcast_to(both[None], (32, 16, width)), 0.0)
    blocks = pick(spread.reshape(512, width), 0).reshape(32, 16, 128)
    owner = owners((32, width), 0)
    ups = jnp.zeros((32, width), F32)
    for k in range(4):
        ups = jnp.where(owner == tab_ref[3:4, :] + 8 * k, up_rows[k : k + 1, :], ups)
    ups = jnp.broadcast_to(pick(ups, 2)[:, None, :], (32, 16, 128))
    blocks = jnp.where(lax.broadcasted_iota(jnp.int32, (32, 16, 128), 1) == 8, ups, blocks)
    out_ref[...] = blocks.reshape(out_ref.shape)


def attend_steps(
    length, hook, x_ref, w_ref, bias_ref, g, out_bias, res_ref, q_ref, k_ref, v_ref, mix_ref, lse_ref, first
):
    rows, width = x_ref.shape
    cols = mix_ref.shape[2]
    heads = cols // HEAD

    @pl.when(first)
    def _():
        @pl.loop(0, rows, step=BLOCK)
        def _(r):
            r = pl.multiple_of(r, BLOCK)
            res_ref[pl.ds(r, BLOCK), :] = x_ref[pl.ds(r, BLOCK), :].astype(F32) + out_bias[...]

    @pl.loop(0, rows, step=BLOCK, unroll=2)
    def _(r):
        r = pl.multiple_of(r, BLOCK)
        here = pl.ds(r, BLOCK)
        out = dot_nn(x_ref[here, :], w_ref[0, :, : 3 * cols]) + bias_ref[g, 0:1, :]
        one = jnp.ones((BLOCK, WIDE - cols), F32)
        tail = lane_iota(BLOCK, WIDE - cols)
        position = r + row_iota(BLOCK, WIDE - cols)
        q_ref[0, here, :cols] = (out[:, :cols].astype(BF16).astype(F32) * HEAD**-0.5).astype(BF16)
        q_ref[0, here, cols:] = jnp.where(tail == 3, one, 0.0).astype(BF16)
        k_ref[0, here, :cols] = out[:, cols : 2 * cols].astype(BF16)
        bias = jnp.where(position < length, 0.0, FLOOR_SCORE)
        k_ref[0, here, cols:] = jnp.where(
            tail < 3, one, jnp.where(tail == 3, bias, 0.0)
        ).astype(BF16)
        v_ref[0, here, :cols] = out[:, 2 * cols : 3 * cols].astype(BF16)
        v_ref[0, here, cols:] = one.astype(BF16)

    @pl.loop(0, rows, step=BLOCK)
    def _(r):
        r = pl.multiple_of(r, BLOCK)
        hook(r)
        here = pl.ds(r, BLOCK)
        query = q_ref[0, here, :]
        scores = [
            dot_nt(jnp.where(head_mask(BLOCK, h, cols), query, 0), k_ref[0]) for h in range(heads)
        ]
        mixed = jnp.zeros((BLOCK, WIDE), F32)
        total = jnp.zeros((BLOCK, 128), F32)
        for h in range(heads):
            top = jnp.max(scores[h], axis=-1, keepdims=True)
            terms = jnp.exp(scores[h] - top).astype(BF16)
            got = dot_nn(terms, v_ref[0])
            denom = got[:, cols : cols + 1]
            mixed = jnp.where(head_mask(BLOCK, h, None), got * (1.0 / denom), mixed)
            total = jnp.where(lane_iota(BLOCK, 128) == h, -(top + jnp.log(denom)), total)
        low = mixed[:, :cols].astype(BF16)
        mix_ref[0, here, :] = low
        lse_ref[0, here, :] = total
        res_ref[here, :] += dot_nt(low, w_ref[0, :, 3 * cols :])


def attend_kernel(len_ref, x_ref, w_ref, bias_ref, ob_ref, *outs):
    t = pl.program_id(0)
    attend_steps(len_ref[0], lambda r: None, x_ref, w_ref, bias_ref, t, ob_ref, *outs, t == 0)


def attend_spread_kernel(
    len_ref, tab_ref, x_ref, own_vec, own_attn, own_up, own_down,
    res_ref, q_ref, k_ref, v_ref, mix_ref, lse_ref, w_ref, vec_ref, up_ref, down_ref,
    vec_buf, attn_buf, bias_buf, send, recv, home,
):
    t = pl.program_id(0)
    place = Place()
    cols = mix_ref.shape[2]

    def spread(n, own, buf, first, rows=slice(None)):
        return Spread(place, own, buf, send.at[n], recv.at[n], home.at[n], first, rows)

    def flat(n, own, buf, rows=slice(None)):
        return SpreadFlat(place, own, buf, send.at[n], recv.at[n], home.at[n], rows)

    cut = own_down.shape[0] * 2 // 3
    small = flat(0, own_vec, vec_buf)
    attn = spread(1, own_attn, attn_buf, "x")
    up = spread(2, own_up, up_ref, "y")
    down = spread(3, own_down, down_ref, "x", slice(0, cut))
    rest = flat(4, own_down, down_ref, slice(cut, None))

    @pl.when(t == 0)
    def _():
        place.greet()
        small.begin()
        attn.begin_z()
        small.after_y()
        small.after_x()
        attn.begin_ab()
        rest.begin()
        down.begin_ab()
        up.begin_ab()
        attn.after_z()
        up.begin_z()
        down.begin_z()
        rest.after_y()
        small.after_z()
        small.after_c()
        join_vectors(vec_buf, tab_ref, vec_ref)
        for g in range(bias_buf.shape[0]):
            there = slice(g * cols, (g + 1) * cols)
            bias_buf[g, 0:1, :] = jnp.concatenate(
                [vec_ref[0:1, there], jnp.zeros((1, cols), F32), vec_ref[1:2, there]], axis=1
            )
        attn.after_a()

    @pl.when(t == 1)
    def _():
        attn.after_c(0)

    @pl.when(t == 3)
    def _():
        attn.after_c(1)

    def hook(r):
        def at(step, block, *events):
            @pl.when((t == step) & (r == block * BLOCK))
            def _():
                for event in events:
                    event()

        at(0, 2, up.after_z)
        at(1, 1, down.after_z, rest.after_x)
        at(1, 2, attn.after_b)
        at(2, 0, down.after_a)
        at(2, 1, up.after_a)
        at(3, 1, rest.after_z)
        at(3, 2, down.after_b)
        at(3, 3, up.after_b)

    g = place.group(t)
    y, c = lax.div(g, 2), lax.rem(g, 2)
    for z in range(DEPTH):
        for x in range(2):
            n = attn_buf.shape[4]
            start = (z * 2 + x) * n
            w_ref[0, start : start + n, :] = attn_buf[y, c, z, x]
    attend_steps(
        len_ref[lax.axis_index("tensor")], hook, x_ref, w_ref, bias_buf, g, vec_ref.at[2:3],
        res_ref, q_ref, k_ref, v_ref, mix_ref, lse_ref, t == 0,
    )

    @pl.when(t == pl.num_programs(0) - 1)
    def _():
        rest.after_c()
        for piece in (down, up):
            piece.after_c(0)
            piece.after_c(1)
        for piece in (small, attn, up, down, rest):
            piece.finish()


def ffn_kernel(
    len_ref, res_ref, cot_ref, vec_ref, wu_ref, wd_ref,
    out_ref, gfirst_ref, gattn_ref, small_ref, gup_ref, gdn_ref,
    hid, hlow, acc, gb, act, dact, gpre,
):
    phase, t = pl.program_id(0), pl.program_id(1)
    last = pl.num_programs(1) - 1
    rows, width = res_ref.shape
    length = len_ref[lax.axis_index("tensor")]
    gain_one, shift_one, down_bias = vec_ref[3:4, :], vec_ref[4:5, :], vec_ref[5:6, :]
    gain_two, shift_two = vec_ref[6:7, :], vec_ref[7:8, :]

    def blocks(body):
        @pl.loop(0, rows, step=BLOCK, unroll=2)
        def _(r):
            r = pl.multiple_of(r, BLOCK)
            body(r, pl.ds(r, BLOCK))

    def put(row, value):
        small_ref[row : row + 1, :] += jnp.sum(value, axis=0, keepdims=True)

    @pl.when((phase == 0) & (t == 0))
    def _():
        small_ref[...] = jnp.zeros_like(small_ref)

        def first(r, here):
            n, _ = normalize(res_ref[here, :])
            hidden = n * gain_one + shift_one
            hid[here, :] = hidden
            hlow[here, :] = hidden.astype(BF16)
            acc[here, :] = hidden + down_bias

        blocks(first)

    @pl.when(phase == 0)
    def _():
        def forward(r, here):
            pre = dot_nn(hlow[here, :], wu_ref[0]) + vec_ref[pl.ds(8 + t, 1), :]
            phi = 0.5 * (1.0 + lax.erf(pre * (0.5**0.5)))
            low = (pre * phi).astype(BF16)
            act[t, here, :] = low
            dact[t, here, :] = phi + pre * (jnp.exp(-0.5 * pre * pre) * 0.3989422804014327)
            acc[here, :] += dot_nt(low, wd_ref[0])

        blocks(forward)

    @pl.when((phase == 0) & (t == last))
    def _():
        def turn(r, here):
            n, inv = normalize(acc[here, :])
            valid = ((r + row_iota(BLOCK, 1)) < length).astype(F32)
            out_ref[here, :] = (n * gain_two + shift_two) * valid
            cot = cot_ref[here, :].astype(F32) * valid
            put(4, cot * n)
            put(5, cot)
            grad = norm_back(cot * gain_two, n, inv)
            acc[here, :] = grad
            low = grad.astype(BF16)
            gb[here, :] = low
            put(3, low.astype(F32))

        blocks(turn)

    @pl.when(phase == 1)
    def _():
        def backward(r, here):
            grad_act = dot_nn(gb[here, :], wd_ref[0]).astype(BF16).astype(F32)
            low = (grad_act * dact[t, here, :]).astype(BF16)
            gpre[here, :] = low
            part = dot_nt(low, wu_ref[0])

            @pl.when(t == 0)
            def _():
                hid[here, :] = part

            @pl.when(t > 0)
            def _():
                hid[here, :] += part

            small_ref[pl.ds(8 + t, 1), :] += jnp.sum(low.astype(F32), axis=0, keepdims=True)

        blocks(backward)

        @pl.loop(0, width, step=BLOCK)
        def _(c):
            c = pl.multiple_of(c, BLOCK)
            here = pl.ds(c, BLOCK)
            gdn_ref[0, here, :] = dot_tn(gb[:, here], act[t]).astype(BF16)
            gup_ref[0, here, :] = dot_tn(hlow[:, here], gpre[...]).astype(BF16)

    @pl.when((phase == 1) & (t == last))
    def _():
        def finish(r, here):
            grad_hidden = acc[here, :] + hid[here, :].astype(BF16).astype(F32)
            n, inv = normalize(res_ref[here, :])
            put(1, grad_hidden * n)
            put(2, grad_hidden)
            grad = norm_back(grad_hidden * gain_one, n, inv)
            gfirst_ref[here, :] = grad
            low = grad.astype(BF16)
            gattn_ref[here, :] = low
            put(0, low.astype(F32))

        blocks(finish)


def attend_back_steps(
    hook, before_grads, put_grads,
    x_ref, w_ref, gattn_ref, gfirst_ref, q_ref, k_ref, v_ref, mix_ref, lse_ref, gtok_ref, bias_ref,
    qh, gh, dq, kh, dqkv,
):
    t = pl.program_id(0)
    rows, width = x_ref.shape
    cols = mix_ref.shape[2]
    heads = cols // HEAD

    if gfirst_ref is not None:
        @pl.when(t == 0)
        def _():
            gtok_ref[...] = gfirst_ref[...]

    bias_ref[...] = jnp.zeros_like(bias_ref)

    @pl.loop(0, rows, step=BLOCK, unroll=2)
    def _(r):
        r = pl.multiple_of(r, BLOCK)
        here = pl.ds(r, BLOCK)
        grad_mixed = dot_nn(gattn_ref[here, :], w_ref[0, :, 3 * cols :]).astype(BF16)
        product = grad_mixed.astype(F32) * mix_ref[0, here, :].astype(F32)
        lane = lane_iota(BLOCK, WIDE)
        wide = jnp.concatenate(
            [grad_mixed.astype(F32), jnp.zeros((BLOCK, WIDE - cols), F32)], axis=1
        )
        query = q_ref[0, here, :].astype(F32)
        key = k_ref[0, here, :]
        for h in range(heads):
            inside = (lane_iota(BLOCK, cols) >= h * HEAD) & (lane_iota(BLOCK, cols) < (h + 1) * HEAD)
            delta = jnp.sum(jnp.where(inside, product, 0.0), axis=-1, keepdims=True)
            hi, mid, low = split_three(-delta)
            keep = head_mask(BLOCK, h, None)
            tail = jnp.where(lane == cols, hi, jnp.where(lane == cols + 1, mid, jnp.where(lane == cols + 2, low, 0.0)))
            gh[h, here, :] = jnp.where(keep, wide, tail).astype(BF16)
            hi, mid, low = split_three(lse_ref[0, here, h : h + 1])
            tail = jnp.where(lane == cols, hi, jnp.where(lane == cols + 1, mid, jnp.where(lane == cols + 2, low, 0.0)))
            tail = jnp.where(lane == cols + 3, 1.0, tail)
            qh[h, here, :] = jnp.where(keep, query, tail).astype(BF16)
            kh[h, here, :] = jnp.where(keep, key, 0)

    @pl.loop(0, rows, step=BLOCK)
    def _(r):
        r = pl.multiple_of(r, BLOCK)
        hook(r)
        here = pl.ds(r, BLOCK)
        key, value = k_ref[0, here, :], v_ref[0, here, :]
        grad_key = jnp.zeros((BLOCK, WIDE), F32)
        grad_value = jnp.zeros((BLOCK, WIDE), F32)
        logits = [dot_nt(key, qh[h]) for h in range(heads)]
        grads = [dot_nt(value, gh[h]) for h in range(heads)]
        for h in range(heads):
            prob = jnp.exp(logits[h])
            grad_value += dot_nn(prob.astype(BF16), gh[h])
            grad_score = (prob * grads[h]).astype(BF16)
            grad_key += dot_nn(grad_score, qh[h])
            part = dot_tn(grad_score, kh[h, here, :])
            if h == 0:
                total = part
            else:
                total += part

        @pl.when(r == 0)
        def _():
            dq[...] = total

        @pl.when(r > 0)
        def _():
            dq[...] += total

        low = grad_key[:, :cols].astype(BF16)
        dqkv[here, cols : 2 * cols] = low
        low = grad_value[:, :cols].astype(BF16)
        dqkv[here, 2 * cols :] = low
        bias_ref[0, 1:2, :] += jnp.sum(low.astype(F32), axis=0, keepdims=True)

    @pl.loop(0, rows, step=BLOCK, unroll=2)
    def _(r):
        r = pl.multiple_of(r, BLOCK)
        here = pl.ds(r, BLOCK)
        low = (dq[here, :cols] * HEAD**-0.5).astype(BF16)
        dqkv[here, :cols] = low
        bias_ref[0, 0:1, :] += jnp.sum(low.astype(F32), axis=0, keepdims=True)
        gtok_ref[here, :] += dot_nt(dqkv[here, :], w_ref[0, :, : 3 * cols])

    before_grads()
    half = width // 2

    @pl.loop(0, width, step=half)
    def _(c):
        c = pl.multiple_of(c, half)
        here = pl.ds(c, half)
        put_grads(c, dot_tn(x_ref[:, here], dqkv[...]), dot_tn(gattn_ref[:, here], mix_ref[0]))


def attend_back_kernel(
    x_ref, w_ref, gattn_ref, gfirst_ref, q_ref, k_ref, v_ref, mix_ref, lse_ref,
    gtok_ref, grad_ref, bias_ref,
    *scratch,
):
    wide = 3 * mix_ref.shape[2]

    def put(c, qkv, out):
        here = pl.ds(c, qkv.shape[0])
        grad_ref[0, here, :wide] = qkv.astype(BF16)
        grad_ref[0, here, wide:] = out.astype(BF16)

    attend_back_steps(
        lambda r: None, lambda: None, put,
        x_ref, w_ref, gattn_ref, gfirst_ref, q_ref, k_ref, v_ref, mix_ref, lse_ref, gtok_ref, bias_ref,
        *scratch,
    )


def attend_back_collect_kernel(
    tab_ref, x_ref, w_ref, gattn_ref, gfirst_ref, q_ref, k_ref, v_ref, mix_ref, lse_ref, vec_ref,
    gup_ref, gdn_ref,
    gtok_ref, attn_out, up_out, down_out, small_out,
    qh, gh, dq, kh, dqkv, bias_ref, bias_all,
    gs, attn_rc, attn_rb, tail_rx, tail_rz, tail_sz, tail_sx,
    up_acc, up_rc, up_rb, up_ra, up_rz,
    down_acc, down_rc, down_rb, down_ra, down_rz,
    rest_acc, rest_rc, rest_rz, rest_rx, rest_ry,
    small_src, small_acc, small_rc, small_rb, small_ra, small_rz,
    send, recv, home,
):
    t = pl.program_id(0)
    last = pl.num_programs(0) - 1
    place = Place()
    cols = mix_ref.shape[2]
    wide = 3 * cols

    def collect(n, near, far, rc, rb, ra, rz, axis):
        return Collect(place, near, far, rc, rb, ra, rz, send.at[n], recv.at[n], axis)

    attn = collect(0, gs.at[3], gs.at[1], attn_rc, attn_rb, None, None, "x")
    up = collect(1, up_acc.at[0], up_acc.at[1], up_rc, up_rb, up_ra, up_rz, "x")
    down = collect(2, down_acc.at[0], down_acc.at[1], down_rc, down_rb, down_ra, down_rz, "y")
    small = collect(3, small_acc.at[0], small_acc.at[1], small_rc, small_rb, small_ra, small_rz, "x")
    rest = CollectFlat(place, rest_acc, rest_rc, rest_rz, rest_rx, rest_ry, send.at[4], recv.at[4])
    tail = Tail(place, gs.at[3], tail_rx, tail_rz, tail_sz, tail_sx, send.at[5], recv.at[5])
    begun = pltpu.make_async_copy(gfirst_ref, gtok_ref, home.at[4, 0])
    rows_y = (place.y, 1 - place.y)
    cut = down_acc.shape[3]
    head, foot = slice(0, cut), slice(cut, cut + rest_acc.shape[3])

    def homes(src, acc, n, rows=slice(None)):
        return [
            pltpu.make_async_copy(src.at[y, place.c, :, :, rows], acc.at[dy], home.at[n, dy])
            for dy, y in enumerate(rows_y)
        ]

    def begin(piece, src, acc, n, rows=slice(None)):
        for dy, y in enumerate(rows_y):
            piece.copy_c(src.at[y, 1 - place.c, :, :, rows], dy).start()
        for copy in homes(src, acc, n, rows):
            copy.start()

    def settle(src, acc, n, rows=slice(None)):
        for copy in homes(src, acc, n, rows):
            copy.wait()

    @pl.when(t == 0)
    def _():
        place.greet()
        begun.start()
        begin(up, gup_ref, up_acc, 0)
        begin(down, gdn_ref, down_acc, 1, head)
        begin(rest, gdn_ref, rest_acc, 3, foot)

    @pl.when(t == 1)
    def _():
        attn.copy_c(gs.at[0], 1).start()

    @pl.when(t == 2)
    def _():
        down.send_a()
        up.sum_b()

    @pl.when(t == 3)
    def _():
        attn.copy_c(gs.at[2], 0).start()
        up.sum_a()

    def hook(r):
        def at(step, block, *events):
            @pl.when((t == step) & (r == block * BLOCK))
            def _():
                for event in events:
                    event()

        def up_first():
            settle(gup_ref, up_acc, 0)
            up.sum_c()

        def down_first():
            settle(gdn_ref, down_acc, 1, head)
            settle(gdn_ref, rest_acc, 3, foot)
            down.sum_c()
            rest.sum_c()

        at(0, 1, up_first)
        at(0, 2, up.send_b)
        at(0, 3, down_first)
        at(2, 0, up.send_a, attn.send_b)
        at(2, 1, rest.sum_z)
        at(2, 2, rest.send_x, down.sum_a)
        at(2, 3, down.send_z)
        at(0, 3, begun.wait)
        at(3, 0, up.send_z)
        at(3, 1, rest.sum_x, lambda: down.sum_z(down_out.at[head]))
        at(3, 2, rest.send_y)

    g = place.group(last - t)

    def before_grads():
        bias_all[g] = bias_ref[0]

        @pl.when(t == 0)
        def _():
            down.send_b()
            rest.send_z()

        @pl.when(t == 1)
        def _():
            down.sum_b()
            attn.wait_c(1)

        @pl.when(t == last)
        def _():
            attn.wait_c(0)
            attn.wait_b()

    def put(c, qkv, out):
        start = lax.div(c, 2 * gs.shape[3])
        some = pl.ds(start, qkv.shape[0] // (2 * gs.shape[3]))
        shape = (qkv.shape[0] // (2 * gs.shape[3]), *gs.shape[2:4])

        def store(*more):
            for lanes, value in ((slice(0, wide), qkv), (slice(wide, None), out)):
                value = value.reshape(*shape, value.shape[1])
                for ref in more:
                    value = value + ref[some, :, :, lanes].astype(F32)
                gs[t, some, :, :, lanes] = value.astype(BF16)

        @pl.when((t == 0) | (t == 2))
        def _():
            store()

        @pl.when(t == 1)
        def _():
            store(attn_rc.at[1])

        @pl.when(t == last)
        def _():
            store(attn_rc.at[0], attn_rb)

    attend_back_steps(
        hook, before_grads, put,
        x_ref, w_ref, gattn_ref, None, q_ref, k_ref, v_ref, mix_ref, lse_ref, gtok_ref, bias_ref,
        qh, gh, dq, kh, dqkv,
    )

    @pl.when(t == last)
    def _():
        up.sum_z(up_out)
        for copy in tail.first():
            copy.start()
        lines = [
            jnp.concatenate([bias_all[n, row : row + 1, :] for n in range(bias_all.shape[0])], axis=1)
            for row in range(2)
        ]
        cut_vectors(jnp.concatenate([*lines, vec_ref[0:6, :]], axis=0), vec_ref[8:12, :], tab_ref, small_src)
        begin(small, small_src, small_acc, 2)
        settle(small_src, small_acc, 2)
        small.sum_c()
        small.send_b()
        small.sum_b()
        small.send_a()
        rest.sum_y(down_out.at[foot])
        up.finish()
        down.finish()
        rest.finish()
        tail.sum_first()
        small.sum_a()
        small.send_z()
        for copy in tail.second():
            copy.start()
        small.sum_z(small_out)
        small.finish()
        for dy in range(2):
            attn.copy_c(attn_rc.at[dy], dy).wait_send()
        for copy in attn.copies_b():
            copy.wait_send()
        tail.sum_second(attn_out)
        tail.finish()


def resident(shape):
    return pl.BlockSpec(shape, lambda *ids: (0,) * len(shape), pipeline_mode=pl.Buffered(1))


def result(shape):
    return pl.BlockSpec(shape, lambda *ids: (0,) * len(shape))


def per_step(shape):
    return pl.BlockSpec((1, *shape[1:]), lambda t: (t, 0, 0))


def struct(shape, dtype):
    return jax.ShapeDtypeStruct(shape, dtype)


def params(steps):
    return pltpu.CompilerParams(
        dimension_semantics=("arbitrary",) * steps, vmem_limit_bytes=VMEM_LIMIT
    )


def attend_outs(groups, rows, width):
    cols = width // groups
    wide = (groups, rows, WIDE)
    specs = [
        result((rows, width)),
        per_step(wide), per_step(wide), per_step(wide),
        per_step((groups, rows, cols)), per_step((groups, rows, 128)),
    ]
    shapes = [
        struct((rows, width), F32),
        struct(wide, BF16), struct(wide, BF16), struct(wide, BF16),
        struct((groups, rows, cols), BF16), struct((groups, rows, 128), F32),
    ]
    return specs, shapes


def run_attend(length, tokens, w_attn, bias, out_bias):
    rows, width = tokens.shape
    groups = w_attn.shape[0]
    specs, shapes = attend_outs(groups, rows, width)
    return pl.pallas_call(
        attend_kernel,
        grid=(groups,),
        in_specs=[
            pl.BlockSpec(memory_space=pltpu.SMEM),
            resident((rows, width)),
            per_step(w_attn.shape),
            resident(bias.shape),
            resident(out_bias.shape),
        ],
        out_specs=specs,
        out_shape=shapes,
        compiler_params=params(1),
        name="attend",
    )(length, tokens, w_attn, bias, out_bias)


def run_attend_spread(lengths, tokens, vec, w_attn, w_up, w_down):
    rows, width = tokens.shape
    groups = 4
    specs, shapes = attend_outs(groups, rows, width)
    whole = (2, 2, DEPTH, 2)
    slab = (groups, width, width)
    table = segment_tables()
    return pl.pallas_call(
        attend_spread_kernel,
        grid=(groups,),
        in_specs=[
            pl.BlockSpec(memory_space=pltpu.SMEM), resident(table.shape), resident((rows, width)),
            resident(vec.shape), resident(w_attn.shape), resident(w_up.shape), resident(w_down.shape),
        ],
        out_specs=specs + [
            per_step(slab), result((16, width)),
            pl.BlockSpec(memory_space=pl.ANY), pl.BlockSpec(memory_space=pl.ANY),
        ],
        out_shape=shapes + [
            struct(slab, BF16), struct((16, width), F32),
            struct((*whole, *w_up.shape), BF16), struct((*whole, *w_down.shape), BF16),
        ],
        scratch_shapes=[
            pltpu.VMEM((*whole, *vec.shape), F32), pltpu.VMEM((*whole, *w_attn.shape), BF16),
            pltpu.VMEM((groups, 8, 3 * width // groups), F32),
            pltpu.SemaphoreType.DMA((5, SLOTS)), pltpu.SemaphoreType.DMA((5, SLOTS)),
            pltpu.SemaphoreType.DMA((5,)),
        ],
        compiler_params=pltpu.CompilerParams(
            dimension_semantics=("arbitrary",), vmem_limit_bytes=VMEM_LIMIT, collective_id=0,
            has_side_effects=True,
        ),
        name="attend",
    )(lengths, table, tokens, vec, w_attn, w_up, w_down)


def run_ffn(length, residual, cotangent, vectors, w_up, w_down):
    rows, width = residual.shape
    groups = w_up.shape[0]
    units = w_up.shape[2]
    slab = pl.BlockSpec((1, width, units), lambda p, t: (t, 0, 0))
    grad = pl.BlockSpec((1, width, units), lambda p, t: (p * t, 0, 0))
    return pl.pallas_call(
        ffn_kernel,
        grid=(2, groups),
        in_specs=[
            pl.BlockSpec(memory_space=pltpu.SMEM),
            resident((rows, width)),
            resident((rows, width)),
            resident(vectors.shape),
            slab, slab,
        ],
        out_specs=[
            result((rows, width)), result((rows, width)), result((rows, width)), result((16, width)),
            grad, grad,
        ],
        out_shape=[
            struct((rows, width), F32), struct((rows, width), F32), struct((rows, width), BF16),
            struct((16, width), F32),
            struct(w_up.shape, BF16), struct(w_up.shape, BF16),
        ],
        scratch_shapes=[
            pltpu.VMEM((rows, width), F32), pltpu.VMEM((rows, width), BF16),
            pltpu.VMEM((rows, width), F32), pltpu.VMEM((rows, width), BF16),
            pltpu.VMEM((groups, rows, units), BF16), pltpu.VMEM((groups, rows, units), F32),
            pltpu.VMEM((rows, units), BF16),
        ],
        compiler_params=params(2),
        name="ffn",
    )(length, residual, cotangent, vectors, w_up, w_down)


def back_scratch(rows, width, cols):
    heads = cols // HEAD
    return [
        pltpu.VMEM((heads, rows, WIDE), BF16), pltpu.VMEM((heads, rows, WIDE), BF16),
        pltpu.VMEM((rows, WIDE), F32), pltpu.VMEM((heads, rows, WIDE), BF16),
        pltpu.VMEM((rows, 3 * cols), BF16),
    ]


def run_attend_back(tokens, w_attn, grad_attn, grad_first, q, k, v, mixed, lse):
    rows, width = tokens.shape
    groups = w_attn.shape[0]
    cols = width // groups
    return pl.pallas_call(
        attend_back_kernel,
        grid=(groups,),
        in_specs=[
            resident((rows, width)), per_step(w_attn.shape),
            resident((rows, width)), resident((rows, width)),
            per_step(q.shape), per_step(k.shape), per_step(v.shape),
            per_step(mixed.shape), per_step(lse.shape),
        ],
        out_specs=[result((rows, width)), per_step(w_attn.shape), per_step((groups, 8, cols))],
        out_shape=[
            struct((rows, width), F32), struct(w_attn.shape, BF16), struct((groups, 8, cols), F32),
        ],
        scratch_shapes=back_scratch(rows, width, cols),
        compiler_params=params(1),
        name="attend_back",
    )(tokens, w_attn, grad_attn, grad_first, q, k, v, mixed, lse)


def run_attend_back_collect(
    tokens, w_attn, grad_attn, grad_first, q, k, v, mixed, lse, small, grad_up, grad_down
):
    rows, width = tokens.shape
    groups = w_attn.shape[0]
    cols = width // groups
    table = segment_tables()

    def back(shape):
        return pl.BlockSpec((1, *shape[1:]), lambda t: (groups - 1 - t, 0, 0))

    def buffers(block, dtype, last):
        chip = (DEPTH, 2, *block)
        return [
            pltpu.VMEM((2, *chip), dtype),
            pltpu.VMEM(chip if last == "x" else (2, DEPTH, *block), dtype),
            pltpu.VMEM((DEPTH, *block), dtype), pltpu.VMEM((DEPTH - 1, *block), dtype),
        ]

    part = (width // (2 * DEPTH), width)
    half, third = (part[0] // 2, width), part[0] // 3
    pair = (2, DEPTH, 2)
    dots = (16, 128)
    return pl.pallas_call(
        attend_back_collect_kernel,
        grid=(groups,),
        in_specs=[
            resident(table.shape), resident((rows, width)), back(w_attn.shape),
            resident((rows, width)), pl.BlockSpec(memory_space=pl.ANY),
            back(q.shape), back(k.shape), back(v.shape), back(mixed.shape), back(lse.shape),
            resident(small.shape),
            pl.BlockSpec(memory_space=pl.ANY), pl.BlockSpec(memory_space=pl.ANY),
        ],
        out_specs=[result((rows, width)), result(part), result(part), result(part), result(dots)],
        out_shape=[
            struct((rows, width), F32), struct(part, F32), struct(part, F32), struct(part, F32),
            struct(dots, F32),
        ],
        scratch_shapes=[
            *back_scratch(rows, width, cols),
            pltpu.VMEM((1, 8, cols), F32), pltpu.VMEM((groups, 8, cols), F32),
            pltpu.VMEM((groups, DEPTH, 2, *part), BF16), *buffers(part, BF16, "x")[:2],
            pltpu.VMEM((DEPTH, 2 * third, width), BF16), pltpu.VMEM((DEPTH - 1, 2 * third, width), BF16),
            pltpu.VMEM((DEPTH - 1, 2, third, width), BF16), pltpu.VMEM((third, width), BF16),
            pltpu.VMEM((*pair, *part), BF16), *buffers(part, BF16, "x"),
            pltpu.VMEM((*pair, *half), BF16), *buffers(half, BF16, "y"),
            pltpu.VMEM((*pair, *half), BF16), pltpu.VMEM((*pair, *half), BF16),
            pltpu.VMEM((DEPTH - 1, 2, 2, *half), BF16), pltpu.VMEM((2, *half), BF16), pltpu.VMEM(half, BF16),
            pltpu.VMEM((2, *pair, *dots), F32), pltpu.VMEM((*pair, *dots), F32), *buffers(dots, F32, "x"),
            pltpu.SemaphoreType.DMA((6, 8)), pltpu.SemaphoreType.DMA((6, 8)),
            pltpu.SemaphoreType.DMA((5, 2)),
        ],
        compiler_params=pltpu.CompilerParams(
            dimension_semantics=("arbitrary",), vmem_limit_bytes=VMEM_LIMIT, collective_id=1,
            has_side_effects=True,
        ),
        name="attend_back",
    )(table, tokens, w_attn, grad_attn, grad_first, q, k, v, mixed, lse, small, grad_up, grad_down)


def shards(
    tokens, lengths, w_query, w_key, w_value, w_out, w_up, w_down,
    query_bias, value_bias, out_bias, attn_gain, attn_shift, up_bias, down_bias, ffn_gain, ffn_shift,
    cotangent,
):
    rows, width = tokens.shape
    groups = lax.axis_size("tensor")
    spans = lax.axis_size("dp")
    seq_count = lengths.shape[0]
    assert rows * groups == seq_count * rows and seq_count == groups
    rank = lax.axis_index("tensor")
    both = ("dp", "tensor")

    cols = width // groups
    units = w_up.shape[1]
    count = query_bias.shape[0]
    vectors = (query_bias, value_bias, out_bias, attn_gain, attn_shift, down_bias, ffn_gain, ffn_shift)
    flat = jnp.concatenate([*vectors, up_bias])
    own_attn = jnp.concatenate([w_query, w_key, w_value, w_out.T], axis=1)

    near = (spans, groups, width, units) == (8, 4, 768, 768)
    if near:
        vec = jnp.pad(jnp.stack(vectors), ((0, 8), (0, 128 - count)))
        vec = vec.at[8, : up_bias.shape[0]].set(up_bias)
        residual, q, k, v, mixed, lse, w_attn, full, w_in, w_back = run_attend_spread(
            lengths, tokens, vec, own_attn, w_up, w_down.T
        )
        w_in, w_back = w_in.reshape(groups, width, units), w_back.reshape(groups, width, units)
    else:
        pack = jnp.concatenate([own_attn, w_up, w_down.T], axis=1)
        whole = lax.all_gather(pack, both, axis=0, tiled=True)
        whole = whole.reshape(spans, groups, *pack.shape).swapaxes(0, 1)
        whole = whole.reshape(groups, width, pack.shape[1])
        w_attn, w_in, w_back = jnp.split(whole, [4 * cols, 4 * cols + units], axis=2)
        gathered = lax.all_gather(flat, both, axis=0, tiled=True).reshape(spans * groups, -1)
        full = gathered[:, : 8 * count].reshape(-1, 8, count).swapaxes(0, 1).reshape(8, width)
        full = jnp.concatenate([full, gathered[:, 8 * count :].reshape(groups, units)])
        full = jnp.pad(full, ((0, 16 - full.shape[0]), (0, 0)))
        qb, vb = full[0].reshape(groups, 1, cols), full[1].reshape(groups, 1, cols)
        bias = jnp.pad(jnp.concatenate([qb, jnp.zeros_like(qb), vb], axis=2), ((0, 0), (0, 7), (0, 0)))
        residual, q, k, v, mixed, lse = run_attend(
            lax.dynamic_slice_in_dim(lengths, rank, 1), tokens, w_attn, bias, full[2:3]
        )
    output, grad_first, grad_attn, small, grad_in, grad_back = run_ffn(
        lengths, residual, cotangent, full, w_in, w_back
    )
    if near:
        split = (2, 2, DEPTH, 2, width // (2 * DEPTH), units)
        grad_tokens, own_a, own_u, own_d, dots = run_attend_back_collect(
            tokens, w_attn, grad_attn, grad_first, q, k, v, mixed, lse, small,
            grad_in.reshape(split), grad_back.reshape(split),
        )
        tiny8 = dots[:8, :count]
        return (
            output, grad_tokens,
            own_a[:, :cols], own_a[:, cols : 2 * cols], own_a[:, 2 * cols : 3 * cols], own_a[:, 3 * cols :].T,
            own_u, own_d.T,
            tiny8[0], tiny8[1], tiny8[2], tiny8[3], tiny8[4], dots[8, : up_bias.shape[0]],
            tiny8[5], tiny8[6], tiny8[7],
        )
    grad_tokens, grad_attn_w, bias_grad = run_attend_back(
        tokens, w_attn, grad_attn, grad_first, q, k, v, mixed, lse
    )

    every = jnp.concatenate([grad_attn_w, grad_in, grad_back], axis=2)
    every = every.reshape(groups, spans, width // spans, -1).swapaxes(0, 1)
    every = every.reshape(spans * groups * (width // spans), -1)
    owned = lax.psum_scatter(every, both, scatter_dimension=0, tiled=True).astype(F32)

    rows8 = jnp.concatenate(
        [bias_grad[:, 0].reshape(1, width), bias_grad[:, 1].reshape(1, width), small[:6]]
    )
    parts = jnp.concatenate(
        [
            rows8.reshape(8, spans * groups, count).swapaxes(0, 1).reshape(spans * groups, 8 * count),
            small[8 : 8 + groups].reshape(spans * groups, -1),
        ],
        axis=1,
    )
    tiny = lax.psum_scatter(parts.reshape(-1), both, scatter_dimension=0, tiled=True)
    tiny8 = tiny[: 8 * count].reshape(8, count)
    return (
        output, grad_tokens,
        owned[:, :cols], owned[:, cols : 2 * cols], owned[:, 2 * cols : 3 * cols],
        owned[:, 3 * cols : 4 * cols].T,
        owned[:, 4 * cols : 4 * cols + units], owned[:, 4 * cols + units :].T,
        tiny8[0], tiny8[1], tiny8[2], tiny8[3], tiny8[4], tiny[8 * count :], tiny8[5], tiny8[6], tiny8[7],
    )


def solution(mesh):
    rows, vector, matrix, flipped = (
        P(("dp", "tensor"), None), P(("dp", "tensor")), P("dp", "tensor"), P("tensor", "dp"),
    )
    return jax.shard_map(
        shards,
        mesh=mesh,
        in_specs=(rows, P("dp"), matrix, matrix, matrix, flipped, matrix, flipped, *(vector,) * 9, rows),
        out_specs=(rows, rows, matrix, matrix, matrix, flipped, matrix, flipped, *(vector,) * 9),
        check_vma=False,
    )
```
